8 devices in a mesh: dp: 1 (over z), tp: 2 (over y), role: 4 (over x, core).
Axes of the slice: x: 2, y: 2, z: 1, core: 2. Of those that a mesh axis runs over, the one named last changes fastest.
Arguments:
- hidden: bfloat16 [2, 64, 2048], P(None, 'dp')
- segment_ids: int32 [64], P('dp')
- loss_mask: int32 [64], P('dp')
- target: int32 [64], P('dp')
- norm_gains: float32 [2, 3, 2048], replicated
- w_query: bfloat16 [4096, 2048], P(('role', 'tp'))
- b_query: bfloat16 [64, 64], P(('role', 'tp'))
- w_key: bfloat16 [512, 2048], P('role')
- b_key: bfloat16 [8, 64], P('role')
- w_value: bfloat16 [512, 2048], P('role')
- b_value: bfloat16 [8, 64], P('role')
- w_out: bfloat16 [4096, 2048], P(('role', 'tp'))
- w_gate: bfloat16 [11264, 2048], P(('role', 'tp'))
- w_up: bfloat16 [11264, 2048], P(('role', 'tp'))
- w_down: bfloat16 [11264, 2048], P(('role', 'tp'))
- w_head: bfloat16 [64000, 2048], P(('role', 'tp'))
Outputs:
- output 1: float32 [64], P('dp')
- output 2: float32 [64], P('dp')
All inputs are finite; a program needn't handle non-finite values.
Results may differ from the reference program's by a relative error of at most 0.00370071.
Values sent between devices are 32-bit elements.
A program may use at most 1 GiB of HBM per device.

```python
import jax
import jax.numpy as jnp
from jax import lax

TOKENS = 64
D = 2048
HEADS = 32
KV_HEADS = 4
HEAD = 64
FF = 5632
VOCAB = 32000
ROW_BLOCK = 32

EPS = 1e-6
ROPE_BASE = 1000000.0
TEMPERATURE = 0.7


def draw_pair(rng_key, shape, scale):
    base_key, diff_key = jax.random.split(rng_key)
    base_vals = jax.random.normal(base_key, shape, jnp.float32)
    diff_vals = jax.random.normal(diff_key, shape, jnp.float32)
    return jnp.concatenate([base_vals, 0.98 * base_vals + 0.2 * diff_vals], axis=0) * scale


def draw_segments(rng_key):
    mean_len = max(TOKENS // 4, 8)
    tok_index = jnp.arange(TOKENS)
    is_start = jax.random.randint(rng_key, (TOKENS,), 0, mean_len) == 0
    is_start = jnp.where(tok_index == 0, False, is_start)
    is_start = jnp.where(tok_index == TOKENS // 2, True, is_start)
    return jnp.cumsum(is_start.astype(jnp.int32)).astype(jnp.int32)


def setup_inputs(seed: int = 0, part: int = 0) -> dict:
    weight_keys = jax.random.split(jax.random.key(seed), 12)
    hid_keys = jax.random.split(jax.random.fold_in(jax.random.key(seed + 1), part), 2)
    int_keys = jax.random.split(jax.random.fold_in(jax.random.key(seed + 2), part), 3)
    base_hid = jax.random.normal(hid_keys[0], (TOKENS, D), jnp.float32)
    diff_hid = jax.random.normal(hid_keys[1], (TOKENS, D), jnp.float32)
    gain_base = jnp.array([1.0, 1.0, 2.0], jnp.float32).reshape(1, 3, 1)
    q_rows = HEADS * HEAD
    kv_rows = KV_HEADS * HEAD
    return {
        "hidden": jnp.stack([base_hid, 0.95 * base_hid + 0.3 * diff_hid]).astype(jnp.bfloat16),
        "segment_ids": draw_segments(int_keys[0]),
        "loss_mask": (jax.random.randint(int_keys[1], (TOKENS,), 0, 8) > 0).astype(jnp.int32),
        "target": jax.random.randint(int_keys[2], (TOKENS,), 0, VOCAB).astype(jnp.int32),
        "norm_gains": draw_pair(weight_keys[0], (1, 3, D), 0.2) + gain_base,
        "w_query": draw_pair(weight_keys[1], (q_rows, D), D ** -0.5).astype(jnp.bfloat16),
        "b_query": draw_pair(weight_keys[2], (HEADS, HEAD), 0.5).astype(jnp.bfloat16),
        "w_key": draw_pair(weight_keys[3], (kv_rows, D), D ** -0.5).astype(jnp.bfloat16),
        "b_key": draw_pair(weight_keys[4], (KV_HEADS, HEAD), 0.5).astype(jnp.bfloat16),
        "w_value": draw_pair(weight_keys[5], (kv_rows, D), D ** -0.5).astype(jnp.bfloat16),
        "b_value": draw_pair(weight_keys[6], (KV_HEADS, HEAD), 0.5).astype(jnp.bfloat16),
        "w_out": draw_pair(weight_keys[7], (q_rows, D), 2.5 * q_rows ** -0.5).astype(jnp.bfloat16),
        "w_gate": draw_pair(weight_keys[8], (FF, D), D ** -0.5).astype(jnp.bfloat16),
        "w_up": draw_pair(weight_keys[9], (FF, D), D ** -0.5).astype(jnp.bfloat16),
        "w_down": draw_pair(weight_keys[10], (FF, D), 1.5 * FF ** -0.5).astype(jnp.bfloat16),
        "w_head": draw_pair(weight_keys[11], (VOCAB, D), D ** -0.5).astype(jnp.bfloat16),
    }


def rms_norm(values, gain):
    vals_f32 = values.astype(jnp.float32)
    inv_rms = lax.rsqrt(jnp.mean(vals_f32 * vals_f32, axis=-1, keepdims=True) + EPS)
    return (vals_f32 * inv_rms * gain).astype(jnp.bfloat16)


def segment_positions(segment_ids):
    tok_index = jnp.arange(segment_ids.shape[-1])
    prev_ids = jnp.concatenate([segment_ids[..., :1] - 1, segment_ids[..., :-1]], axis=-1)
    seg_start = lax.cummax(jnp.where(segment_ids != prev_ids, tok_index, 0), axis=segment_ids.ndim - 1)
    return tok_index - seg_start


def rotary(values, positions):
    half_dim = values.shape[-1] // 2
    inv_freq = ROPE_BASE ** (-2.0 * jnp.arange(half_dim).astype(jnp.float32) / values.shape[-1])
    angles = positions.astype(jnp.float32)[..., None] * inv_freq
    cos_part = jnp.cos(angles)[..., None, :]
    sin_part = jnp.sin(angles)[..., None, :]
    first_half = values[..., :half_dim]
    second_half = values[..., half_dim:]
    return jnp.concatenate([first_half * cos_part - second_half * sin_part, second_half * cos_part + first_half * sin_part], axis=-1)


def model_layer(x_in, segment_ids, gain3, w_query, b_query, w_key, b_key, w_value, b_value, w_out, w_gate, w_up, w_down):
    positions = segment_positions(segment_ids)
    tok_index = jnp.arange(TOKENS)
    allowed = (segment_ids[:, None] == segment_ids[None, :]) & (tok_index[:, None] >= tok_index[None, :])
    normed = rms_norm(x_in, gain3[0])
    q_proj = jnp.dot(normed, w_query.T, preferred_element_type=jnp.float32).reshape(TOKENS, HEADS, HEAD) + b_query.astype(jnp.float32)
    k_proj = jnp.dot(normed, w_key.T, preferred_element_type=jnp.float32).reshape(TOKENS, KV_HEADS, HEAD) + b_key.astype(jnp.float32)
    v_proj = (jnp.dot(normed, w_value.T, preferred_element_type=jnp.float32).reshape(TOKENS, KV_HEADS, HEAD) + b_value.astype(jnp.float32)).astype(jnp.bfloat16)
    q_rot = rotary(q_proj, positions).astype(jnp.bfloat16)
    k_rot = rotary(k_proj, positions).astype(jnp.bfloat16)
    q_grouped = jnp.moveaxis(q_rot.reshape(TOKENS, KV_HEADS, HEADS // KV_HEADS, HEAD), 1, 0)

    def one_group(group_args):
        q_group, k_group, v_group = group_args
        scores = jnp.einsum("tgd,sd->gts", q_group.astype(jnp.float32), k_group.astype(jnp.float32)) * HEAD ** -0.5
        scores = jnp.where(allowed[None], scores, -1e30)
        attn_probs = jax.nn.softmax(scores, axis=-1).astype(jnp.bfloat16)
        return jnp.einsum("gts,sd->tgd", attn_probs.astype(jnp.float32), v_group.astype(jnp.float32)).astype(jnp.bfloat16)

    attn = lax.map(one_group, (q_grouped, jnp.moveaxis(k_rot, 1, 0), jnp.moveaxis(v_proj, 1, 0)))
    attn = jnp.moveaxis(attn, 0, 1).reshape(TOKENS, HEADS * HEAD)
    resid = (x_in.astype(jnp.float32) + jnp.dot(attn, w_out, preferred_element_type=jnp.float32)).astype(jnp.bfloat16)
    normed_mlp = rms_norm(resid, gain3[1])
    gate_proj = jnp.dot(normed_mlp, w_gate.T, preferred_element_type=jnp.float32)
    up_proj = jnp.dot(normed_mlp, w_up.T, preferred_element_type=jnp.float32)
    act_vals = (jax.nn.silu(gate_proj) * up_proj).astype(jnp.bfloat16)
    layer_out = (resid.astype(jnp.float32) + jnp.dot(act_vals, w_down, preferred_element_type=jnp.float32)).astype(jnp.bfloat16)
    return rms_norm(layer_out, gain3[2])


def reference(hidden, segment_ids, loss_mask, target, norm_gains, w_query, b_query, w_key, b_key, w_value, b_value, w_out, w_gate, w_up, w_down, w_head):
    q_rows = HEADS * HEAD
    kv_rows = KV_HEADS * HEAD
    finals = []
    for model_idx in range(2):
        q_lo = model_idx * q_rows
        kv_lo = model_idx * kv_rows
        ff_lo = model_idx * FF
        finals.append(model_layer(
            hidden[model_idx], segment_ids, norm_gains[model_idx],
            w_query[q_lo:q_lo + q_rows], b_query[model_idx * HEADS:(model_idx + 1) * HEADS],
            w_key[kv_lo:kv_lo + kv_rows], b_key[model_idx * KV_HEADS:(model_idx + 1) * KV_HEADS],
            w_value[kv_lo:kv_lo + kv_rows], b_value[model_idx * KV_HEADS:(model_idx + 1) * KV_HEADS],
            w_out[q_lo:q_lo + q_rows], w_gate[ff_lo:ff_lo + FF], w_up[ff_lo:ff_lo + FF], w_down[ff_lo:ff_lo + FF]))
    head_pol = w_head[:VOCAB]
    head_ref = w_head[VOCAB:]
    num_blocks = TOKENS // ROW_BLOCK
    vocab_ids = jnp.arange(VOCAB)

    def head_block(block_args):
        pol_rows, ref_rows, tgt_rows = block_args
        pol_lp = jax.nn.log_softmax(jnp.dot(pol_rows, head_pol.T, preferred_element_type=jnp.float32) / TEMPERATURE, axis=-1)
        ref_lp = jax.nn.log_softmax(jnp.dot(ref_rows, head_ref.T, preferred_element_type=jnp.float32) / TEMPERATURE, axis=-1)
        kl_rows = jnp.sum(jnp.exp(pol_lp) * (pol_lp - ref_lp), axis=-1)
        tgt_lp = jnp.sum(jnp.where(vocab_ids[None, :] == tgt_rows[:, None], pol_lp, 0.0), axis=-1)
        return kl_rows, tgt_lp

    kl_div, target_logp = lax.map(head_block, (finals[0].reshape(num_blocks, ROW_BLOCK, D), finals[1].reshape(num_blocks, ROW_BLOCK, D), target.reshape(num_blocks, ROW_BLOCK)))
    mask_vals = loss_mask.astype(jnp.float32)
    return kl_div.reshape(TOKENS) * mask_vals, target_logp.reshape(TOKENS) * mask_vals
```

```python
import functools
import math

import jax
import jax.numpy as jnp
from jax import lax
from jax.experimental import pallas as pl
from jax.experimental.pallas import tpu as pltpu
from jax.sharding import PartitionSpec as P

EPS = 1e-6
ROPE_BASE = 1000000.0
TEMPERATURE = 0.7
NEG = -1e30
GROUPS = 2
CHUNK = 512
LAG = 3
F32 = jnp.float32
BF16 = jnp.bfloat16
MESH = pl.DeviceIdType.MESH


def dot_t(rows, weight):
    return lax.dot_general(rows, weight, (((1,), (1,)), ((), ())), preferred_element_type=F32)


def dot_n(rows, weight):
    return lax.dot_general(rows, weight, (((1,), (0,)), ((), ())), preferred_element_type=F32)


def normed(vals, gain):
    inv_rms = lax.rsqrt(jnp.mean(vals * vals, axis=-1, keepdims=True) + EPS)
    return (vals * inv_rms * gain).astype(BF16)


def kernel(cfg, hidden, gains, w_query, w_key, w_value, w_out, w_gate, w_up, w_down, w_head,
           seg_ref, mask_ref, tgt_ref, bq_ref, bk_ref, bv_ref, out_ref,
           xb, gn, wqkv, wo, wg, wu, wd, wh, qs, os_, part, rbuf, sbuf, ybuf, resid, full,
           zsend, zkeep, zrecv, m_own, s_own, m_kl, s_kl, t_acc, dup, pack,
           in_sem, head_sem, d_send, d_recv, y_send, y_recv, b_send, b_recv, z_send, z_recv, p_send, p_recv):
    tokens, dim, head_dim, q_heads, vocab = cfg
    n = tokens // GROUPS
    own = n // 2
    halves = ((vocab // CHUNK + 2) // 2) * CHUNK
    steps = halves // CHUNK
    tp = lax.axis_index("tp")
    role = lax.axis_index("role")
    core = role % 2
    half = role // 2
    here = role * 2 + tp
    shard = core * 2 + tp
    d_peer = {"role": half * 2 + 1 - core}
    y_peer = {"tp": 1 - tp}
    x_peer = {"role": (1 - half) * 2 + core}
    send_half = 1 - half

    barrier = pltpu.get_barrier_semaphore()
    for hop in range(1, 8):
        other = (here + hop) % 8
        pl.semaphore_signal(barrier, inc=1, device_id={"tp": other % 2, "role": other // 2}, device_id_type=MESH)

    first = []
    kv_rows = pl.ds(pl.multiple_of(tp * head_dim, head_dim), head_dim)
    q_rows = q_heads * head_dim
    moves = [(hidden.at[half], xb), (gains.at[half], gn), (w_query, wqkv.at[pl.ds(0, q_rows)])]
    for slot in range(2):
        moves.append((w_key.at[kv_rows], wqkv.at[pl.ds(q_rows + slot * head_dim, head_dim)]))
        moves.append((w_value.at[kv_rows], wqkv.at[pl.ds(q_rows + (2 + slot) * head_dim, head_dim)]))
    moves += [(w_out, wo), (w_gate, wg), (w_up, wu), (w_down, wd)]
    for idx, (src, dst) in enumerate(moves):
        first.append(pltpu.make_async_copy(src, dst, in_sem.at[idx]))
    for copy in first:
        copy.start()

    def chunk_start(part_half, step):
        nominal = part_half * halves + step * CHUNK
        start = jnp.minimum(nominal, vocab - CHUNK)
        return start, nominal - start

    def head_copy(part_half, step):
        start, _ = chunk_start(part_half, step)
        slot = part_half * steps + step
        return pltpu.make_async_copy(w_head.at[pl.ds(pl.multiple_of(start, 64), CHUNK)], wh.at[slot], head_sem.at[slot])

    @pl.loop(0, steps)
    def _(step):
        head_copy(send_half, step).start()
        head_copy(1 - send_half, step).start()

    ti = lax.broadcasted_iota(jnp.int32, (tokens, tokens), 0)
    tj = lax.broadcasted_iota(jnp.int32, (tokens, tokens), 1)
    eye = ti == tj
    seg_row = seg_ref[...].astype(F32)
    seg_col = jnp.sum(jnp.where(eye, seg_row, 0.0), axis=1, keepdims=True)
    same = seg_col == seg_row
    allowed = same & (ti >= tj)
    seg_first = jnp.min(jnp.where(same, tj.astype(F32), 1e9), axis=1, keepdims=True)
    pos = lax.broadcasted_iota(jnp.int32, (tokens, 1), 0).astype(F32) - seg_first
    wide = 2 * head_dim
    lane = lax.broadcasted_iota(jnp.int32, (1, wide), 1)
    half_dim = head_dim // 2
    freq = jnp.exp((lane % half_dim).astype(F32) * (-2.0 * math.log(ROPE_BASE) / head_dim))
    angles = pos * freq
    cos_t = jnp.cos(angles)
    sin_t = jnp.sin(angles)
    low = (lane % head_dim) < half_dim
    sin_t = jnp.where(low, -sin_t, sin_t)
    even = lane < head_dim
    tgt_col = jnp.sum(jnp.where(eye, tgt_ref[...].astype(F32), 0.0), axis=1, keepdims=True)

    dup[...] = jnp.zeros_like(dup)
    dup[0:q_heads, 0:head_dim] = bq_ref[...].astype(F32)
    dup[q_heads:q_heads + 2, 0:head_dim] = bk_ref[...].astype(F32)
    dup[q_heads + 2:q_heads + 4, 0:head_dim] = bv_ref[...].astype(F32)
    bias = dup[...]
    bias = bias + pltpu.roll(bias, head_dim, 1)
    bias_k = jnp.where(tp == 0, bias[q_heads:q_heads + 1], bias[q_heads + 1:q_heads + 2])
    bias_v = jnp.where(tp == 0, bias[q_heads + 2:q_heads + 3], bias[q_heads + 3:q_heads + 4])

    def rotate(vals):
        turned = jnp.where(low, pltpu.roll(vals, wide - half_dim, 1), pltpu.roll(vals, half_dim, 1))
        return vals * cos_t + turned * sin_t

    first[0].wait()
    first[1].wait()
    xf = xb[...].astype(F32)
    a_in = normed(xf, gn[0:1, :])
    for copy in first[2:7]:
        copy.wait()
    qkv = dot_t(a_in, wqkv[...])
    k_rot = rotate(qkv[:, q_rows:q_rows + wide] + bias_k).astype(BF16)
    v_two = (qkv[:, q_rows + wide:q_rows + 2 * wide] + bias_v).astype(BF16)
    for pair in range(q_heads // 2):
        bias_q = jnp.where(even, bias[2 * pair:2 * pair + 1], bias[2 * pair + 1:2 * pair + 2])
        q_rot = rotate(qkv[:, pair * wide:(pair + 1) * wide] + bias_q) * head_dim ** -0.5
        qs[2 * pair * tokens:(2 * pair + 1) * tokens, :] = jnp.where(even, q_rot, 0.0).astype(BF16)
        qs[(2 * pair + 1) * tokens:(2 * pair + 2) * tokens, :] = jnp.where(even, 0.0, q_rot).astype(BF16)
    scores = dot_t(qs[...], k_rot).reshape(q_heads, tokens, tokens)
    scores = jnp.where(allowed[None], scores, NEG)
    expd = jnp.exp(scores - jnp.max(scores, axis=-1, keepdims=True))
    probs = (expd / jnp.sum(expd, axis=-1, keepdims=True)).astype(BF16).reshape(q_heads * tokens, tokens)
    heads_out = dot_n(probs, v_two)
    for pair in range(q_heads // 2):
        lo = heads_out[2 * pair * tokens:(2 * pair + 1) * tokens]
        hi = heads_out[(2 * pair + 1) * tokens:(2 * pair + 2) * tokens]
        os_[:, pair * wide:(pair + 1) * wide] = jnp.where(even, lo, hi).astype(BF16)
    first[7].wait()
    part[0] = dot_n(os_[...], wo[...])

    def own_rows(grp, which):
        return pl.ds(pl.multiple_of(grp * n + which * own, 8), own)

    def d_copy(red, grp):
        return pltpu.make_async_remote_copy(
            part.at[red, own_rows(grp, 1 - core)], rbuf.at[red, grp], d_send.at[red, grp], d_recv.at[red, grp],
            device_id=d_peer, device_id_type=MESH)

    def y_copy(red, grp):
        return pltpu.make_async_remote_copy(
            sbuf.at[red, grp], ybuf.at[red, grp], y_send.at[red, grp], y_recv.at[red, grp],
            device_id=y_peer, device_id_type=MESH)

    def b_copy(red, grp):
        rows = pl.ds(pl.multiple_of(core * own, 8), own)
        return pltpu.make_async_remote_copy(
            full.at[red, grp, rows], full.at[red, grp, rows], b_send.at[red, grp], b_recv.at[red, grp],
            device_id=d_peer, device_id_type=MESH)

    def chip_sum(red, grp):
        d_copy(red, grp).wait_recv()
        sbuf[red, grp] = part[red, own_rows(grp, core)] + rbuf[red, grp]
        y_copy(red, grp).start()

    def finish(red, grp):
        y_copy(red, grp).wait_recv()
        total = sbuf[red, grp] + ybuf[red, grp]
        if red == 0:
            base = xb[own_rows(grp, core), :].astype(F32)
        else:
            base = resid[grp]
        rows = (base + total).astype(BF16).astype(F32)
        if red == 0:
            resid[grp] = rows
        full[red, grp, pl.ds(pl.multiple_of(core * own, 8), own)] = normed(rows, gn[red + 1:red + 2, :]).astype(F32)
        b_copy(red, grp).start()

    def gathered(red, grp):
        b_copy(red, grp).wait_recv()
        return full[red, grp].astype(BF16)

    def mlp(grp, b_in):
        if grp == 0:
            for copy in first[8:11]:
                copy.wait()
        gate = dot_t(b_in, wg[...])
        up = dot_t(b_in, wu[...])
        act = (gate * (1.0 / (1.0 + jnp.exp(-gate))) * up).astype(BF16)
        part[1, grp * n:(grp + 1) * n] = dot_n(act, wd[...])
        d_copy(1, grp).start()

    pl.semaphore_wait(barrier, 7)
    for grp in range(GROUPS):
        d_copy(0, grp).start()
    for grp in range(GROUPS):
        chip_sum(0, grp)
    finish(0, 0)
    for grp in range(GROUPS):
        mlp(grp, gathered(0, grp))
        if grp + 1 < GROUPS:
            finish(0, grp + 1)
        chip_sum(1, grp)
    finish(1, 0)

    for stat in (s_own, s_kl, t_acc):
        stat[...] = jnp.zeros_like(stat)
    m_own[...] = jnp.full_like(m_own, NEG)
    m_kl[...] = jnp.full_like(m_kl, NEG)
    lanes = lax.broadcasted_iota(jnp.int32, (1, CHUNK), 1)
    tiles = CHUNK // 128

    def z_copy(grp, step):
        return pltpu.make_async_remote_copy(
            zsend.at[grp, step], zrecv.at[grp, step], z_send.at[grp, step], z_recv.at[grp, step],
            device_id=x_peer, device_id_type=MESH)

    def logits(grp, rows, part_half, step):
        start, repeated = chunk_start(part_half, step)
        z = dot_t(rows, wh[part_half * steps + step]) * (1.0 / TEMPERATURE)
        fresh = lanes >= repeated
        z = jnp.where(fresh, z, NEG)
        ids = (lanes + (shard * vocab + start)).astype(F32)
        hit = jnp.where((ids == tgt_col[grp * n:(grp + 1) * n]) & fresh, z, 0.0)
        pieces = [z[:, 128 * t:128 * (t + 1)] for t in range(tiles)]
        m_old = m_own[grp]
        m_new = functools.reduce(jnp.maximum, pieces, m_old)
        total = s_own[grp] * jnp.exp(m_old - m_new)
        for piece in pieces:
            total = total + jnp.exp(piece - m_new)
        m_own[grp] = m_new
        s_own[grp] = total
        t_acc[grp] = t_acc[grp] + functools.reduce(jnp.add, [hit[:, 128 * t:128 * (t + 1)] for t in range(tiles)])
        return z

    def kl_step(grp, step):
        z_copy(grp, step).wait_recv()
        mine, theirs = zkeep[grp, step], zrecv[grp, step]
        diff = mine - theirs
        policy = half == 0
        top = jnp.where(policy, mine, theirs)
        diff = jnp.where(policy, diff, -diff)
        pieces = [top[:, 128 * t:128 * (t + 1)] for t in range(tiles)]
        m_old = m_kl[grp]
        m_new = functools.reduce(jnp.maximum, pieces, m_old)
        total = s_kl[grp] * jnp.exp(m_old - m_new)
        for t, piece in enumerate(pieces):
            total = total + jnp.exp(piece - m_new) * diff[:, 128 * t:128 * (t + 1)]
        m_kl[grp] = m_new
        s_kl[grp] = total

    def head_steps(grp, rows, begin, end):
        @pl.loop(begin, end)
        def _(step):
            if grp == 0:
                head_copy(send_half, step).wait()
            zsend[grp, step] = logits(grp, rows, send_half, step)
            z_copy(grp, step).start()
            if grp == 0:
                head_copy(1 - send_half, step).wait()
            zkeep[grp, step] = logits(grp, rows, 1 - send_half, step)
            if grp > 0:
                @pl.when(step < LAG)
                def _():
                    kl_step(grp - 1, steps - LAG + step)

            @pl.when(step >= LAG)
            def _():
                kl_step(grp, step - LAG)

    middle = steps // 2
    for grp in range(GROUPS):
        rows = gathered(1, grp)
        head_steps(grp, rows, 0, middle)
        if grp + 1 < GROUPS:
            finish(1, grp + 1)
        head_steps(grp, rows, middle, steps)

    def to_row(col):
        return jnp.sum(jnp.where(eye, col, 0.0), axis=0, keepdims=True)

    def stat_rows(m_ref, s_ref):
        m_all = m_ref[...].reshape(tokens, 128)
        m_col = jnp.max(m_all, axis=1, keepdims=True)
        s_col = jnp.sum(s_ref[...].reshape(tokens, 128) * jnp.exp(m_all - m_col), axis=1, keepdims=True)
        return to_row(m_col), to_row(s_col)

    pack[here, 0:1, 0:tokens], pack[here, 1:2, 0:tokens] = stat_rows(m_own, s_own)
    pack[here, 4:5, 0:tokens] = to_row(jnp.sum(t_acc[...].reshape(tokens, 128), axis=1, keepdims=True))
    for step in range(steps - LAG, steps):
        kl_step(GROUPS - 1, step)
    pack[here, 2:3, 0:tokens], pack[here, 3:4, 0:tokens] = stat_rows(m_kl, s_kl)

    def p_copy(hop):
        other = (here + hop) % 8
        return pltpu.make_async_remote_copy(
            pack.at[here], pack.at[here], p_send.at[hop - 1], p_recv.at[hop - 1],
            device_id={"tp": other % 2, "role": other // 2}, device_id_type=MESH)

    for hop in range(1, 8):
        p_copy(hop).start()
    for red in range(2):
        for grp in range(GROUPS):
            d_copy(red, grp).wait_send()
            y_copy(red, grp).wait_send()
            b_copy(red, grp).wait_send()

    @pl.loop(0, GROUPS * steps)
    def _(idx):
        z_copy(idx // steps, idx % steps).wait_send()

    for hop in range(1, 8):
        p_copy(hop).wait_recv()

    def lse(devices):
        tops = [pack[dev, 0:1, 0:tokens] for dev in devices]
        top = functools.reduce(jnp.maximum, tops)
        total = functools.reduce(jnp.add, [pack[dev, 1:2, 0:tokens] * jnp.exp(t - top) for dev, t in zip(devices, tops)])
        return top + jnp.log(total)

    lse_pol = lse(range(4))
    lse_ref = lse(range(4, 8))
    cross = functools.reduce(jnp.add, [pack[dev, 3:4, 0:tokens] * jnp.exp(pack[dev, 2:3, 0:tokens] - lse_pol) for dev in range(8)])
    tgt_z = functools.reduce(jnp.add, [pack[dev, 4:5, 0:tokens] for dev in range(4)])
    mask_vals = mask_ref[...].astype(F32)
    out_ref[0:1, :] = (cross - lse_pol + lse_ref) * mask_vals
    out_ref[1:2, :] = (tgt_z - lse_pol) * mask_vals
    for hop in range(1, 8):
        p_copy(hop).wait_send()


def solution(mesh):
    by_shard = P(("role", "tp"), None)
    by_role = P("role", None)

    def per_device(hidden, segment_ids, loss_mask, target, norm_gains, w_query, b_query, w_key, b_key, w_value, b_value, w_out, w_gate, w_up, w_down, w_head):
        tokens, dim = hidden.shape[1:]
        q_heads, head_dim = b_query.shape
        ff = w_gate.shape[0]
        vocab = w_head.shape[0]
        n = tokens // GROUPS
        own = n // 2
        halves = ((vocab // CHUNK + 2) // 2) * CHUNK
        steps = halves // CHUNK
        any_spec = pl.BlockSpec(memory_space=pl.ANY)
        vmem_spec = pl.BlockSpec(memory_space=pltpu.VMEM)
        wide = 2 * head_dim
        out = pl.pallas_call(
            functools.partial(kernel, (tokens, dim, head_dim, q_heads, vocab)),
            out_shape=jax.ShapeDtypeStruct((2, tokens), F32),
            in_specs=[any_spec] * 10 + [vmem_spec] * 6,
            out_specs=vmem_spec,
            scratch_shapes=[
                pltpu.VMEM((tokens, dim), BF16),
                pltpu.VMEM((3, dim), F32),
                pltpu.VMEM((q_heads * head_dim + 2 * wide, dim), BF16),
                pltpu.VMEM((q_heads * head_dim, dim), BF16),
                pltpu.VMEM((ff, dim), BF16),
                pltpu.VMEM((ff, dim), BF16),
                pltpu.VMEM((ff, dim), BF16),
                pltpu.VMEM((2 * steps, CHUNK, dim), BF16),
                pltpu.VMEM((q_heads * tokens, wide), BF16),
                pltpu.VMEM((tokens, q_heads * head_dim), BF16),
                pltpu.VMEM((2, tokens, dim), F32),
                pltpu.VMEM((2, GROUPS, own, dim), F32),
                pltpu.VMEM((2, GROUPS, own, dim), F32),
                pltpu.VMEM((2, GROUPS, own, dim), F32),
                pltpu.VMEM((GROUPS, own, dim), F32),
                pltpu.VMEM((2, GROUPS, n, dim), F32),
                pltpu.VMEM((GROUPS, steps, n, CHUNK), F32),
                pltpu.VMEM((GROUPS, steps, n, CHUNK), F32),
                pltpu.VMEM((GROUPS, steps, n, CHUNK), F32),
                pltpu.VMEM((GROUPS, n, 128), F32),
                pltpu.VMEM((GROUPS, n, 128), F32),
                pltpu.VMEM((GROUPS, n, 128), F32),
                pltpu.VMEM((GROUPS, n, 128), F32),
                pltpu.VMEM((GROUPS, n, 128), F32),
                pltpu.VMEM((16, 128), F32),
                pltpu.VMEM((8, 8, 128), F32),
                pltpu.SemaphoreType.DMA((11,)),
                pltpu.SemaphoreType.DMA((2 * steps,)),
                pltpu.SemaphoreType.DMA((2, GROUPS)),
                pltpu.SemaphoreType.DMA((2, GROUPS)),
                pltpu.SemaphoreType.DMA((2, GROUPS)),
                pltpu.SemaphoreType.DMA((2, GROUPS)),
                pltpu.SemaphoreType.DMA((2, GROUPS)),
                pltpu.SemaphoreType.DMA((2, GROUPS)),
                pltpu.SemaphoreType.DMA((GROUPS, steps)),
                pltpu.SemaphoreType.DMA((GROUPS, steps)),
                pltpu.SemaphoreType.DMA((7,)),
                pltpu.SemaphoreType.DMA((7,)),
            ],
            compiler_params=pltpu.CompilerParams(
                collective_id=0, has_side_effects=True, vmem_limit_bytes=67043328),
            name="layer_head_kl",
        )(hidden, norm_gains, w_query, w_key, w_value, w_out, w_gate, w_up, w_down, w_head,
          segment_ids.reshape(1, tokens), loss_mask.reshape(1, tokens), target.reshape(1, tokens), b_query, b_key, b_value)
        return out[0], out[1]

    in_specs = (P(None, "dp", None), P("dp"), P("dp"), P("dp"), P(None, None, None), by_shard, by_shard, by_role, by_role, by_role, by_role, by_shard, by_shard, by_shard, by_shard, by_shard)
    return jax.shard_map(per_device, mesh=mesh, in_specs=in_specs, out_specs=(P("dp"), P("dp")), check_vma=False)
```

```python
import contextlib
import functools
import math

import jax
import jax.numpy as jnp
from jax import lax
from jax.experimental import pallas as pl
from jax.experimental.pallas import tpu as pltpu
from jax.sharding import PartitionSpec as P

EPS = 1e-6
ROPE_BASE = 1000000.0
TEMPERATURE = 0.7
NEG = -1e30
SIZES = (32, 32)
CHUNK = 512
LAG = 5
F32 = jnp.float32
BF16 = jnp.bfloat16
MESH = pl.DeviceIdType.MESH


def scope(name):
    return contextlib.nullcontext()


def dot_t(rows, weight):
    return lax.dot_general(rows, weight, (((1,), (1,)), ((), ())), preferred_element_type=F32)


def dot_n(rows, weight):
    return lax.dot_general(rows, weight, (((1,), (0,)), ((), ())), preferred_element_type=F32)


def normed(vals, gain):
    inv_rms = lax.rsqrt(jnp.mean(vals * vals, axis=-1, keepdims=True) + EPS)
    return (vals * inv_rms * gain).astype(BF16)


def kernel(cfg, hidden, gains, w_query, w_key, w_value, w_out, w_gate, w_up, w_down, w_head,
           seg_in, mask_in, tgt_in, bq_in, bk_in, bv_in, out_ref,
           xb, gn, seg_ref, mask_ref, tgt_ref, bq_ref, bk_ref, bv_ref, wqkv, wo, wg, wu, wd, wh, xcol, qs, os_, part, rbuf, ybuf, full,
           zsend, zkeep, zrecv, m_own, s_own, m_kl, s_kl, t_acc, dup, pack,
           in_sem, head_sem, d_send, d_recv, y_send, y_recv, b_send, b_recv, z_send, z_recv, p_send, p_recv):
    tokens, dim, head_dim, q_heads, vocab = cfg
    offs = [sum(SIZES[:grp]) for grp in range(len(SIZES))]
    groups = len(SIZES)
    cols = dim // 2
    halves = ((vocab // CHUNK + 2) // 2) * CHUNK
    steps = halves // CHUNK
    tp = lax.axis_index("tp")
    role = lax.axis_index("role")
    core = role % 2
    half = role // 2
    here = role * 2 + tp
    shard = core * 2 + tp
    d_peer = {"role": half * 2 + 1 - core}
    y_peer = {"tp": 1 - tp}
    x_peer = {"role": (1 - half) * 2 + core}
    send_half = 1 - half
    q_rows = q_heads * head_dim
    wide = 2 * head_dim

    kv_rows = pl.ds(pl.multiple_of(tp * head_dim, head_dim), head_dim)
    theirs_cols = pl.ds(pl.multiple_of((1 - core) * cols, cols), cols)
    mine_cols = pl.ds(pl.multiple_of(core * cols, cols), cols)
    moves = [(hidden.at[half], xb), (gains, gn), (seg_in, seg_ref), (mask_in, mask_ref), (tgt_in, tgt_ref),
             (bq_in, bq_ref), (bk_in, bk_ref), (bv_in, bv_ref)]
    n_small = len(moves)
    for piece in range(4):
        rows = pl.ds(piece * q_rows // 4, q_rows // 4)
        moves.append((w_query.at[rows], wqkv.at[rows]))
    for slot in range(2):
        moves.append((w_key.at[kv_rows], wqkv.at[pl.ds(q_rows + slot * head_dim, head_dim)]))
        moves.append((w_value.at[kv_rows], wqkv.at[pl.ds(q_rows + (2 + slot) * head_dim, head_dim)]))
    n_qkv = len(moves)
    moves += [(w_out.at[:, theirs_cols], wo.at[0]), (w_out.at[:, mine_cols], wo.at[1])]
    n_out = len(moves)
    moves += [(w_gate, wg), (w_up, wu), (w_down.at[:, theirs_cols], wd.at[0]), (w_down.at[:, mine_cols], wd.at[1])]
    loads = [pltpu.make_async_copy(src, dst, in_sem.at[idx]) for idx, (src, dst) in enumerate(moves)]
    for copy in loads[:n_out]:
        copy.start()

    barrier = pltpu.get_barrier_semaphore()
    for hop in range(1, 8):
        other = (here + hop) % 8
        pl.semaphore_signal(barrier, inc=1, device_id={"tp": other % 2, "role": other // 2}, device_id_type=MESH)

    def chunk_start(part_half, step):
        nominal = part_half * halves + step * CHUNK
        start = jnp.minimum(nominal, vocab - CHUNK)
        return start, nominal - start

    def head_copy(keep, step):
        start, _ = chunk_start((1 - send_half) if keep else send_half, step)
        return pltpu.make_async_copy(w_head.at[pl.ds(pl.multiple_of(start, 64), CHUNK)],
                                     wh.at[step, pl.ds(keep * CHUNK, CHUNK)], head_sem.at[keep, step])

    ti = lax.broadcasted_iota(jnp.int32, (tokens, tokens), 0)
    tj = lax.broadcasted_iota(jnp.int32, (tokens, tokens), 1)
    eye = ti == tj
    lane = lax.broadcasted_iota(jnp.int32, (1, wide), 1)
    half_dim = head_dim // 2
    freq = jnp.exp((lane % half_dim).astype(F32) * (-2.0 * math.log(ROPE_BASE) / head_dim))
    low = (lane % head_dim) < half_dim
    even = lane < head_dim

    def gain_row(which):
        return jnp.where(half == 0, gn[which, 0:1, :], gn[which, 1:2, :])

    with scope("wait_x"):
        for copy in loads[:n_small]:
            copy.wait()
    with scope("norm_x"):
        seg_row = seg_ref[...].astype(F32)
        seg_col = jnp.sum(jnp.where(eye, seg_row, 0.0), axis=1, keepdims=True)
        same = seg_col == seg_row
        allowed = same & (ti >= tj)
        seg_first = jnp.min(jnp.where(same, tj.astype(F32), 1e9), axis=1, keepdims=True)
        pos = lax.broadcasted_iota(jnp.int32, (tokens, 1), 0).astype(F32) - seg_first
        angles = pos * freq
        cos_t = jnp.cos(angles)
        sin_t = jnp.sin(angles)
        sin_t = jnp.where(low, -sin_t, sin_t)
        tgt_col = jnp.sum(jnp.where(eye, tgt_ref[...].astype(F32), 0.0), axis=1, keepdims=True)
        dup[...] = jnp.zeros_like(dup)
        dup[0:q_heads, 0:head_dim] = bq_ref[...].astype(F32)
        dup[q_heads:q_heads + 2, 0:head_dim] = bk_ref[...].astype(F32)
        dup[q_heads + 2:q_heads + 4, 0:head_dim] = bv_ref[...].astype(F32)
        bias = dup[...]
        bias = bias + pltpu.roll(bias, head_dim, 1)
        bias_k = jnp.where(tp == 0, bias[q_heads:q_heads + 1], bias[q_heads + 1:q_heads + 2])
        bias_v = jnp.where(tp == 0, bias[q_heads + 2:q_heads + 3], bias[q_heads + 3:q_heads + 4])
        xf = xb[...].astype(F32)
        xcol[0] = xf[:, :cols]
        xcol[1] = xf[:, cols:]
        a_in = normed(xf, gain_row(0))

    def rotate(vals):
        turned = jnp.where(low, pltpu.roll(vals, wide - half_dim, 1), pltpu.roll(vals, half_dim, 1))
        return vals * cos_t + turned * sin_t

    with scope("wait_qkv"):
        for copy in loads[n_small:n_qkv]:
            copy.wait()
    for copy in loads[n_out:]:
        copy.start()

    @pl.loop(0, steps)
    def _(step):
        head_copy(0, step).start()
        head_copy(1, step).start()

    with scope("qkv"):
        qkv = dot_t(a_in, wqkv[...])
        k_rot = rotate(qkv[:, q_rows:q_rows + wide] + bias_k).astype(BF16)
        v_two = (qkv[:, q_rows + wide:q_rows + 2 * wide] + bias_v).astype(BF16)
        for pair in range(q_heads // 2):
            bias_q = jnp.where(even, bias[2 * pair:2 * pair + 1], bias[2 * pair + 1:2 * pair + 2])
            q_rot = rotate(qkv[:, pair * wide:(pair + 1) * wide] + bias_q) * head_dim ** -0.5
            qs[2 * pair * tokens:(2 * pair + 1) * tokens, :] = jnp.where(even, q_rot, 0.0).astype(BF16)
            qs[(2 * pair + 1) * tokens:(2 * pair + 2) * tokens, :] = jnp.where(even, 0.0, q_rot).astype(BF16)
    with scope("attn"):
        scores = dot_t(qs[...], k_rot).reshape(q_heads, tokens, tokens)
        scores = jnp.where(allowed[None], scores, NEG)
        expd = jnp.exp(scores - jnp.max(scores, axis=-1, keepdims=True))
        probs = (expd / jnp.sum(expd, axis=-1, keepdims=True)).astype(BF16).reshape(q_heads * tokens, tokens)
        heads_out = dot_n(probs, v_two)
        for pair in range(q_heads // 2):
            lo = heads_out[2 * pair * tokens:(2 * pair + 1) * tokens]
            hi = heads_out[(2 * pair + 1) * tokens:(2 * pair + 2) * tokens]
            os_[:, pair * wide:(pair + 1) * wide] = jnp.where(even, lo, hi).astype(BF16)

    def rows_of(grp):
        return pl.ds(offs[grp], SIZES[grp])

    def d_copy(red, grp):
        return pltpu.make_async_remote_copy(
            part.at[red, 0, rows_of(grp)], rbuf.at[red, rows_of(grp)], d_send.at[red, grp], d_recv.at[red, grp],
            device_id=d_peer, device_id_type=MESH)

    def y_copy(red, grp):
        return pltpu.make_async_remote_copy(
            part.at[red, 1, rows_of(grp)], ybuf.at[red, rows_of(grp)], y_send.at[red, grp], y_recv.at[red, grp],
            device_id=y_peer, device_id_type=MESH)

    def b_copy(red, grp):
        return pltpu.make_async_remote_copy(
            full.at[red, core, rows_of(grp)], full.at[red, core, rows_of(grp)], b_send.at[red, grp], b_recv.at[red, grp],
            device_id=d_peer, device_id_type=MESH)

    def chip_sum(red, grp):
        rows = rows_of(grp)
        with scope(f"wait_d{red}{grp}"):
            d_copy(red, grp).wait_recv()
        part[red, 1, rows] = part[red, 1, rows] + rbuf[red, rows]
        y_copy(red, grp).start()

    def finish(red, grp):
        rows = rows_of(grp)
        with scope(f"wait_y{red}{grp}"):
            y_copy(red, grp).wait_recv()
        base = xcol[core, rows] if red == 0 else full[0, core, rows]
        full[red, core, rows] = (base + (part[red, 1, rows] + ybuf[red, rows])).astype(BF16).astype(F32)
        b_copy(red, grp).start()

    def gathered(red, grp):
        rows = rows_of(grp)
        with scope(f"wait_b{red}{grp}"):
            b_copy(red, grp).wait_recv()
        left, right = full[red, 0, rows], full[red, 1, rows]
        total = jnp.sum(left * left, axis=-1, keepdims=True) + jnp.sum(right * right, axis=-1, keepdims=True)
        inv_rms = lax.rsqrt(total * (1.0 / dim) + EPS)
        gain = gain_row(red + 1)
        return jnp.concatenate([(left * inv_rms * gain[:, :cols]).astype(BF16),
                                (right * inv_rms * gain[:, cols:]).astype(BF16)], axis=1)

    def mlp(grp, b_in):
        rows = rows_of(grp)
        if grp == 0:
            for copy in loads[n_out:]:
                copy.wait()
        with scope(f"mlp{grp}"):
            gate = dot_t(b_in, wg[...])
            up = dot_t(b_in, wu[...])
            act = (gate * (1.0 / (1.0 + jnp.exp(-gate))) * up).astype(BF16)
            part[1, 0, rows] = dot_n(act, wd[0])
        d_copy(1, grp).start()
        with scope(f"down{grp}"):
            part[1, 1, rows] = dot_n(act, wd[1])

    for copy in loads[n_qkv:n_out]:
        copy.wait()
    with scope("oproj"):
        part[0, 0] = dot_n(os_[...], wo[0])
    with scope("entry"):
        pl.semaphore_wait(barrier, 7)
    for grp in range(groups):
        d_copy(0, grp).start()
    with scope("oproj"):
        part[0, 1] = dot_n(os_[...], wo[1])
    for grp in range(groups):
        chip_sum(0, grp)
    finish(0, 0)
    for grp in range(groups):
        mlp(grp, gathered(0, grp))
        if grp + 1 < groups:
            finish(0, grp + 1)
        if grp == groups - 1:
            finish(1, 0)
        chip_sum(1, grp)

    for stat in (s_own, s_kl, t_acc):
        stat[...] = jnp.zeros_like(stat)
    m_own[...] = jnp.full_like(m_own, NEG)
    m_kl[...] = jnp.full_like(m_kl, NEG)
    lanes = lax.broadcasted_iota(jnp.int32, (1, CHUNK), 1)
    tiles = CHUNK // 128

    def split(vals):
        return [vals[:, 128 * t:128 * (t + 1)] for t in range(tiles)]

    def z_copy(grp, step):
        return pltpu.make_async_remote_copy(
            zsend.at[step, rows_of(grp)], zrecv.at[step, rows_of(grp)], z_send.at[grp, step], z_recv.at[grp, step],
            device_id=x_peer, device_id_type=MESH)

    def scaled(z, keep, step):
        _, repeated = chunk_start((1 - send_half) if keep else send_half, step)
        return jnp.where(lanes >= repeated, z * (1.0 / TEMPERATURE), NEG)

    def own_step(grp, step):
        rows = rows_of(grp)
        m_old, total, hits = m_own[rows], s_own[rows], t_acc[rows]
        goal = tgt_col[offs[grp]:offs[grp] + SIZES[grp]]
        parts = []
        for keep, src in ((0, zsend), (1, zkeep)):
            start, repeated = chunk_start((1 - send_half) if keep else send_half, step)
            z = src[step, rows]
            ids = (lanes + (shard * vocab + start)).astype(F32)
            for hit in split(jnp.where((ids == goal) & (lanes >= repeated), z, 0.0)):
                hits = hits + hit
            parts += split(z)
        m_new = functools.reduce(jnp.maximum, parts, m_old)
        total = total * jnp.exp(m_old - m_new)
        for piece in parts:
            total = total + jnp.exp(piece - m_new)
        m_own[rows] = m_new
        s_own[rows] = total
        t_acc[rows] = hits

    def kl_wait(grp, step):
        with scope(f"wait_z{grp}"):
            z_copy(grp, step).wait_recv()

    def kl_step(grp, step):
        rows = rows_of(grp)
        mine, theirs = zkeep[step, rows], zrecv[step, rows]
        policy = half == 0
        tops = split(jnp.where(policy, mine, theirs))
        diffs = split(jnp.where(policy, mine - theirs, theirs - mine))
        m_old = m_kl[rows]
        m_new = functools.reduce(jnp.maximum, tops, m_old)
        total = s_kl[rows] * jnp.exp(m_old - m_new)
        for top, diff in zip(tops, diffs):
            total = total + jnp.exp(top - m_new) * diff
        m_kl[rows] = m_new
        s_kl[rows] = total

    def head_step(grp, h_in, step, behind, kl_of):
        rows = rows_of(grp)
        if grp == 0:
            with scope("wait_w"):
                head_copy(0, step).wait()
                head_copy(1, step).wait()
        if kl_of is not None:
            kl_wait(*kl_of)
        with scope(f"step{grp}"):
            z = dot_t(h_in, wh[step])
            zsend[step, rows] = scaled(z[:, :CHUNK], 0, step)
            zkeep[step, rows] = scaled(z[:, CHUNK:], 1, step)
            if behind is not None:
                own_step(*behind)
            if kl_of is not None:
                kl_step(*kl_of)
        z_copy(grp, step).start()

    def first_step(grp, h_in):
        rows = rows_of(grp)
        head_copy(0, 0).wait()
        with scope("first"):
            zsend[0, rows] = scaled(dot_t(h_in, wh[0, 0:CHUNK]), 0, 0)
        z_copy(grp, 0).start()
        head_copy(1, 0).wait()
        with scope("first"):
            zkeep[0, rows] = scaled(dot_t(h_in, wh[0, CHUNK:2 * CHUNK]), 1, 0)

    for grp in range(groups):
        h_in = gathered(1, grp)
        if grp == 0:
            first_step(grp, h_in)

            @pl.loop(1, LAG)
            def _(step):
                head_step(grp, h_in, step, (grp, step - 1), None)
        else:
            head_step(grp, h_in, 0, (grp - 1, steps - 1), (grp - 1, steps - LAG))

            @pl.loop(1, LAG)
            def _(step):
                head_step(grp, h_in, step, (grp, step - 1), (grp - 1, steps - LAG + step))

        if grp + 1 < groups:
            finish(1, grp + 1)

        @pl.loop(LAG, steps)
        def _(step):
            head_step(grp, h_in, step, (grp, step - 1), (grp, step - LAG))

    last = groups - 1
    own_step(last, steps - 1)

    def to_row(col):
        return jnp.sum(jnp.where(eye, col, 0.0), axis=0, keepdims=True)

    def stat_rows(m_ref, s_ref):
        m_all = m_ref[...]
        m_col = jnp.max(m_all, axis=1, keepdims=True)
        s_col = jnp.sum(s_ref[...] * jnp.exp(m_all - m_col), axis=1, keepdims=True)
        return to_row(m_col), to_row(s_col)

    pack[here, 0:1, 0:tokens], pack[here, 1:2, 0:tokens] = stat_rows(m_own, s_own)
    pack[here, 4:5, 0:tokens] = to_row(jnp.sum(t_acc[...], axis=1, keepdims=True))
    for red in range(2):
        for grp in range(groups):
            d_copy(red, grp).wait_send()
            y_copy(red, grp).wait_send()
            b_copy(red, grp).wait_send()
    for step in range(steps - LAG, steps):
        kl_wait(last, step)
        kl_step(last, step)
    pack[here, 2:3, 0:tokens], pack[here, 3:4, 0:tokens] = stat_rows(m_kl, s_kl)

    def p_copy(hop):
        other = (here + hop) % 8
        return pltpu.make_async_remote_copy(
            pack.at[here], pack.at[here], p_send.at[hop - 1], p_recv.at[hop - 1],
            device_id={"tp": other % 2, "role": other // 2}, device_id_type=MESH)

    for hop in range(1, 8):
        p_copy(hop).start()
    for grp in range(groups):
        @pl.loop(0, steps)
        def _(step):
            z_copy(grp, step).wait_send()

    with scope("wait_p"):
        for hop in range(1, 8):
            p_copy(hop).wait_recv()

    with scope("final"):
        def lse(devices):
            tops = [pack[dev, 0:1, 0:tokens] for dev in devices]
            top = functools.reduce(jnp.maximum, tops)
            total = functools.reduce(jnp.add, [pack[dev, 1:2, 0:tokens] * jnp.exp(t - top) for dev, t in zip(devices, tops)])
            return top + jnp.log(total)

        lse_pol = lse(range(4))
        lse_ref = lse(range(4, 8))
        cross = functools.reduce(jnp.add, [pack[dev, 3:4, 0:tokens] * jnp.exp(pack[dev, 2:3, 0:tokens] - lse_pol) for dev in range(8)])
        tgt_z = functools.reduce(jnp.add, [pack[dev, 4:5, 0:tokens] for dev in range(4)])
        mask_vals = mask_ref[...].astype(F32)
        out_ref[0:1, :] = (cross - lse_pol + lse_ref) * mask_vals
        out_ref[1:2, :] = (tgt_z - lse_pol) * mask_vals
    with scope("wait_ps"):
        for hop in range(1, 8):
            p_copy(hop).wait_send()


def solution(mesh):
    by_shard = P(("role", "tp"), None)
    by_role = P("role", None)

    def per_device(hidden, segment_ids, loss_mask, target, norm_gains, w_query, b_query, w_key, b_key, w_value, b_value, w_out, w_gate, w_up, w_down, w_head):
        tokens, dim = hidden.shape[1:]
        q_heads, head_dim = b_query.shape
        ff = w_gate.shape[0]
        vocab = w_head.shape[0]
        groups = len(SIZES)
        cols = dim // 2
        q_rows = q_heads * head_dim
        halves = ((vocab // CHUNK + 2) // 2) * CHUNK
        steps = halves // CHUNK
        wide = 2 * head_dim
        sem = pltpu.SemaphoreType.DMA
        out = pl.pallas_call(
            functools.partial(kernel, (tokens, dim, head_dim, q_heads, vocab)),
            out_shape=jax.ShapeDtypeStruct((2, tokens), F32),
            in_specs=[pl.BlockSpec(memory_space=pl.ANY)] * 16,
            out_specs=pl.BlockSpec(memory_space=pltpu.VMEM),
            scratch_shapes=[
                pltpu.VMEM((tokens, dim), BF16),
                pltpu.VMEM((3, 2, dim), F32),
                pltpu.VMEM((1, tokens), jnp.int32),
                pltpu.VMEM((1, tokens), jnp.int32),
                pltpu.VMEM((1, tokens), jnp.int32),
                pltpu.VMEM(b_query.shape, BF16),
                pltpu.VMEM(b_key.shape, BF16),
                pltpu.VMEM(b_value.shape, BF16),
                pltpu.VMEM((q_rows + 2 * wide, dim), BF16),
                pltpu.VMEM((2, q_rows, cols), BF16),
                pltpu.VMEM((ff, dim), BF16),
                pltpu.VMEM((ff, dim), BF16),
                pltpu.VMEM((2, ff, cols), BF16),
                pltpu.VMEM((steps, 2 * CHUNK, dim), BF16),
                pltpu.VMEM((2, tokens, cols), F32),
                pltpu.VMEM((q_heads * tokens, wide), BF16),
                pltpu.VMEM((tokens, q_rows), BF16),
                pltpu.VMEM((2, 2, tokens, cols), F32),
                pltpu.VMEM((2, tokens, cols), F32),
                pltpu.VMEM((2, tokens, cols), F32),
                pltpu.VMEM((2, 2, tokens, cols), F32),
                pltpu.VMEM((steps, tokens, CHUNK), F32),
                pltpu.VMEM((steps, tokens, CHUNK), F32),
                pltpu.VMEM((steps, tokens, CHUNK), F32),
                pltpu.VMEM((tokens, 128), F32),
                pltpu.VMEM((tokens, 128), F32),
                pltpu.VMEM((tokens, 128), F32),
                pltpu.VMEM((tokens, 128), F32),
                pltpu.VMEM((tokens, 128), F32),
                pltpu.VMEM((16, 128), F32),
                pltpu.VMEM((8, 8, 128), F32),
                sem((22,)), sem((2, steps)),
                sem((2, groups)), sem((2, groups)), sem((2, groups)), sem((2, groups)), sem((2, groups)), sem((2, groups)),
                sem((groups, steps)), sem((groups, steps)), sem((7,)), sem((7,)),
            ],
            compiler_params=pltpu.CompilerParams(
                collective_id=0, has_side_effects=True, vmem_limit_bytes=67043328),
            name="layer_head_kl",
        )(hidden, jnp.transpose(norm_gains, (1, 0, 2)), w_query, w_key, w_value, w_out, w_gate, w_up, w_down, w_head,
          segment_ids.reshape(1, tokens), loss_mask.reshape(1, tokens), target.reshape(1, tokens), b_query, b_key, b_value)
        return out[0], out[1]

    in_specs = (P(None, "dp", None), P("dp"), P("dp"), P("dp"), P(None, None, None), by_shard, by_shard, by_role, by_role, by_role, by_role, by_shard, by_shard, by_shard, by_shard, by_shard)
    return jax.shard_map(per_device, mesh=mesh, in_specs=in_specs, out_specs=(P("dp"), P("dp")), check_vma=False)
```

```python
import contextlib
import functools
import math

import jax
import jax.numpy as jnp
from jax import lax
from jax.experimental import pallas as pl
from jax.experimental.pallas import tpu as pltpu
from jax.sharding import PartitionSpec as P

EPS = 1e-6
ROPE_BASE = 1000000.0
TEMPERATURE = 0.7
NEG = -1e30
SIZES = (24, 40)
AHEAD = 4
LATE = 6
TILE = 256
CHUNK = 512
LAG = 5
F32 = jnp.float32
BF16 = jnp.bfloat16
MESH = pl.DeviceIdType.MESH


def scope(name):
    return contextlib.nullcontext()


def dot_t(rows, weight):
    return lax.dot_general(rows, weight, (((1,), (1,)), ((), ())), preferred_element_type=F32)


def dot_n(rows, weight):
    return lax.dot_general(rows, weight, (((1,), (0,)), ((), ())), preferred_element_type=F32)


def normed(vals, gain):
    inv_rms = lax.rsqrt(jnp.mean(vals * vals, axis=-1, keepdims=True) + EPS)
    return (vals * inv_rms * gain).astype(BF16)


def kernel(cfg, hidden, gains, w_query, w_key, w_value, w_out, w_gate, w_up, w_down, w_head,
           seg_in, mask_in, tgt_in, bq_in, bk_in, bv_in, out_ref,
           xb, gn, seg_ref, mask_ref, tgt_ref, bq_ref, bk_ref, bv_ref, wqkv, wo, wgu, wd, wh, xcol, qs, os_, part, rbuf, ybuf, full,
           gate_up, zsend, zkeep, zrecv, m_own, s_own, m_kl, s_kl, t_acc, dup, pack,
           in_sem, head_sem, d_send, d_recv, y_send, y_recv, b_send, b_recv, z_send, z_recv, p_send, p_recv):
    tokens, dim, head_dim, q_heads, vocab = cfg
    offs = [sum(SIZES[:grp]) for grp in range(len(SIZES))]
    groups = len(SIZES)
    cols = dim // 2
    ff = w_gate.shape[0]
    halves = ((vocab // CHUNK + 2) // 2) * CHUNK
    steps = halves // CHUNK
    tp = lax.axis_index("tp")
    role = lax.axis_index("role")
    core = role % 2
    half = role // 2
    here = role * 2 + tp
    shard = core * 2 + tp
    d_peer = {"role": half * 2 + 1 - core}
    y_peer = {"tp": 1 - tp}
    x_peer = {"role": (1 - half) * 2 + core}
    send_half = 1 - half
    q_rows = q_heads * head_dim
    wide = 2 * head_dim

    kv_rows = pl.ds(pl.multiple_of(tp * head_dim, head_dim), head_dim)
    theirs_cols = pl.ds(pl.multiple_of((1 - core) * cols, cols), cols)
    mine_cols = pl.ds(pl.multiple_of(core * cols, cols), cols)
    moves = [(hidden.at[half], xb), (gains, gn), (seg_in, seg_ref), (mask_in, mask_ref), (tgt_in, tgt_ref),
             (bq_in, bq_ref), (bk_in, bk_ref), (bv_in, bv_ref)]
    n_small = len(moves)
    for piece in range(4):
        rows = pl.ds(piece * q_rows // 4, q_rows // 4)
        moves.append((w_query.at[rows], wqkv.at[rows]))
    for slot in range(2):
        moves.append((w_key.at[kv_rows], wqkv.at[pl.ds(q_rows + slot * head_dim, head_dim)]))
        moves.append((w_value.at[kv_rows], wqkv.at[pl.ds(q_rows + (2 + slot) * head_dim, head_dim)]))
    n_qkv = len(moves)
    moves += [(w_out.at[:, theirs_cols], wo.at[0]), (w_out.at[:, mine_cols], wo.at[1])]
    n_out = len(moves)
    moves += [(w_gate, wgu.at[pl.ds(0, ff)]), (w_up, wgu.at[pl.ds(ff, ff)])]
    n_gu = len(moves)
    moves += [(w_down.at[:, theirs_cols], wd.at[0]), (w_down.at[:, mine_cols], wd.at[1])]
    loads = [pltpu.make_async_copy(src, dst, in_sem.at[idx]) for idx, (src, dst) in enumerate(moves)]
    for copy in loads[:n_qkv]:
        copy.start()

    barrier = pltpu.get_barrier_semaphore()
    for hop in range(1, 8):
        other = (here + hop) % 8
        pl.semaphore_signal(barrier, inc=1, device_id={"tp": other % 2, "role": other // 2}, device_id_type=MESH)

    def chunk_start(part_half, step):
        nominal = part_half * halves + step * CHUNK
        start = jnp.minimum(nominal, vocab - CHUNK)
        return start, nominal - start

    def head_copy(keep, step):
        start, _ = chunk_start((1 - send_half) if keep else send_half, step)
        return pltpu.make_async_copy(w_head.at[pl.ds(pl.multiple_of(start, 64), CHUNK)],
                                     wh.at[step, pl.ds(keep * CHUNK, CHUNK)], head_sem.at[keep, step])

    ti = lax.broadcasted_iota(jnp.int32, (tokens, tokens), 0)
    tj = lax.broadcasted_iota(jnp.int32, (tokens, tokens), 1)
    eye = ti == tj
    lane = lax.broadcasted_iota(jnp.int32, (1, wide), 1)
    half_dim = head_dim // 2
    freq = jnp.exp((lane % half_dim).astype(F32) * (-2.0 * math.log(ROPE_BASE) / head_dim))
    low = (lane % head_dim) < half_dim
    even = lane < head_dim

    def gain_row(which):
        return jnp.where(half == 0, gn[which, 0:1, :], gn[which, 1:2, :])

    with scope("wait_x"):
        for copy in loads[:n_small]:
            copy.wait()
    with scope("norm_x"):
        seg_row = seg_ref[...].astype(F32)
        seg_col = jnp.sum(jnp.where(eye, seg_row, 0.0), axis=1, keepdims=True)
        same = seg_col == seg_row
        allowed = same & (ti >= tj)
        seg_first = jnp.min(jnp.where(same, tj.astype(F32), 1e9), axis=1, keepdims=True)
        pos = lax.broadcasted_iota(jnp.int32, (tokens, 1), 0).astype(F32) - seg_first
        angles = pos * freq
        cos_t = jnp.cos(angles)
        sin_t = jnp.sin(angles)
        sin_t = jnp.where(low, -sin_t, sin_t)
        tgt_col = jnp.sum(jnp.where(eye, tgt_ref[...].astype(F32), 0.0), axis=1, keepdims=True)
        dup[...] = jnp.zeros_like(dup)
        dup[0:q_heads, 0:head_dim] = bq_ref[...].astype(F32)
        dup[q_heads:q_heads + 2, 0:head_dim] = bk_ref[...].astype(F32)
        dup[q_heads + 2:q_heads + 4, 0:head_dim] = bv_ref[...].astype(F32)
        bias = dup[...]
        bias = bias + pltpu.roll(bias, head_dim, 1)
        bias_k = jnp.where(tp == 0, bias[q_heads:q_heads + 1], bias[q_heads + 1:q_heads + 2])
        bias_v = jnp.where(tp == 0, bias[q_heads + 2:q_heads + 3], bias[q_heads + 3:q_heads + 4])
        xf = xb[...].astype(F32)
        xcol[0] = xf[:, :cols]
        xcol[1] = xf[:, cols:]
        a_in = normed(xf, gain_row(0))

    def rotate(vals):
        turned = jnp.where(low, pltpu.roll(vals, wide - half_dim, 1), pltpu.roll(vals, half_dim, 1))
        return vals * cos_t + turned * sin_t

    with scope("wait_qkv"):
        for copy in loads[n_small:n_qkv]:
            copy.wait()
    for copy in loads[n_qkv:]:
        copy.start()

    @pl.loop(0, steps)
    def _(step):
        head_copy(0, step).start()
        head_copy(1, step).start()

    with scope("qkv"):
        qkv = dot_t(a_in, wqkv[...])
        k_rot = rotate(qkv[:, q_rows:q_rows + wide] + bias_k).astype(BF16)
        v_two = (qkv[:, q_rows + wide:q_rows + 2 * wide] + bias_v).astype(BF16)
        for pair in range(q_heads // 2):
            bias_q = jnp.where(even, bias[2 * pair:2 * pair + 1], bias[2 * pair + 1:2 * pair + 2])
            q_rot = rotate(qkv[:, pair * wide:(pair + 1) * wide] + bias_q) * head_dim ** -0.5
            qs[2 * pair * tokens:(2 * pair + 1) * tokens, :] = jnp.where(even, q_rot, 0.0).astype(BF16)
            qs[(2 * pair + 1) * tokens:(2 * pair + 2) * tokens, :] = jnp.where(even, 0.0, q_rot).astype(BF16)
    with scope("attn"):
        scores = dot_t(qs[...], k_rot).reshape(q_heads, tokens, tokens)
        scores = jnp.where(allowed[None], scores, NEG)
        expd = jnp.exp(scores - jnp.max(scores, axis=-1, keepdims=True))
        probs = (expd / jnp.sum(expd, axis=-1, keepdims=True)).astype(BF16).reshape(q_heads * tokens, tokens)
        heads_out = dot_n(probs, v_two)
        for pair in range(q_heads // 2):
            lo = heads_out[2 * pair * tokens:(2 * pair + 1) * tokens]
            hi = heads_out[(2 * pair + 1) * tokens:(2 * pair + 2) * tokens]
            os_[:, pair * wide:(pair + 1) * wide] = jnp.where(even, lo, hi).astype(BF16)

    def rows_of(grp):
        return pl.ds(offs[grp], SIZES[grp])

    def d_copy(red, grp):
        return pltpu.make_async_remote_copy(
            part.at[red, 0, rows_of(grp)], rbuf.at[red, rows_of(grp)], d_send.at[red, grp], d_recv.at[red, grp],
            device_id=d_peer, device_id_type=MESH)

    def y_copy(red, grp):
        return pltpu.make_async_remote_copy(
            part.at[red, 1, rows_of(grp)], ybuf.at[red, rows_of(grp)], y_send.at[red, grp], y_recv.at[red, grp],
            device_id=y_peer, device_id_type=MESH)

    def b_copy(red, grp):
        return pltpu.make_async_remote_copy(
            full.at[red, core, rows_of(grp)], full.at[red, core, rows_of(grp)], b_send.at[red, grp], b_recv.at[red, grp],
            device_id=d_peer, device_id_type=MESH)

    def chip_sum(red, grp):
        rows = rows_of(grp)
        with scope(f"wait_d{red}{grp}"):
            d_copy(red, grp).wait_recv()
        part[red, 1, rows] = part[red, 1, rows] + rbuf[red, rows]
        y_copy(red, grp).start()

    def finish(red, grp):
        rows = rows_of(grp)
        with scope(f"wait_y{red}{grp}"):
            y_copy(red, grp).wait_recv()
        base = xcol[core, rows] if red == 0 else full[0, core, rows]
        full[red, core, rows] = (base + (part[red, 1, rows] + ybuf[red, rows])).astype(BF16).astype(F32)
        b_copy(red, grp).start()

    def b_wait(red, grp):
        with scope(f"wait_b{red}{grp}"):
            b_copy(red, grp).wait_recv()

    def normed_rows(red, off, size):
        rows = pl.ds(off, size)
        left, right = full[red, 0, rows], full[red, 1, rows]
        total = jnp.sum(left * left, axis=-1, keepdims=True) + jnp.sum(right * right, axis=-1, keepdims=True)
        inv_rms = lax.rsqrt(total * (1.0 / dim) + EPS)
        gain = gain_row(red + 1)
        return jnp.concatenate([(left * inv_rms * gain[:, :cols]).astype(BF16),
                                (right * inv_rms * gain[:, cols:]).astype(BF16)], axis=1)

    def gathered(red, grp):
        b_wait(red, grp)
        return normed_rows(red, offs[grp], SIZES[grp])

    def turn_tiles(ref, rows):
        for k in range(dim // TILE):
            ref[rows, k * TILE:(k + 1) * TILE] = ref[rows, k * TILE:(k + 1) * TILE].T

    def turn(first, last):
        with scope("turn"):
            @pl.loop(first, last)
            def _(blk):
                turn_tiles(wgu, pl.ds(pl.multiple_of(blk * TILE, TILE), TILE))

    def turn_head(step):
        for row in range(0, CHUNK, TILE):
            turn_tiles(wh.at[step], pl.ds(row, TILE))

    def turned_dot(vals, ref, row):
        return functools.reduce(jnp.add, [dot_n(vals[:, k * TILE:(k + 1) * TILE], ref[row:row + TILE, k * TILE:(k + 1) * TILE])
                                          for k in range(dim // TILE)])

    def mlp(grp, b_in):
        rows = rows_of(grp)
        if grp == 0:
            for copy in loads[n_gu:]:
                copy.wait()
        if grp == groups - 1:
            for step in range(AHEAD):
                head_copy(0, step).wait()
        with scope(f"mlp{grp}"):
            if grp == groups - 1:
                for step in range(AHEAD):
                    turn_head(step)
            for row in range(0, 2 * ff, TILE):
                gate_up[rows, row:row + TILE] = turned_dot(b_in, wgu, row)
            gate, up = gate_up[rows, 0:ff], gate_up[rows, ff:2 * ff]
            act = (gate * (1.0 / (1.0 + jnp.exp(-gate))) * up).astype(BF16)
            part[1, 0, rows] = dot_n(act, wd[0])
        d_copy(1, grp).start()
        with scope(f"down{grp}"):
            part[1, 1, rows] = dot_n(act, wd[1])

    for copy in loads[n_qkv:n_out]:
        copy.wait()
    with scope("oproj"):
        part[0, 0] = dot_n(os_[...], wo[0])
    with scope("entry"):
        pl.semaphore_wait(barrier, 7)
    for grp in range(groups):
        d_copy(0, grp).start()
    with scope("oproj"):
        part[0, 1] = dot_n(os_[...], wo[1])
    blocks = 2 * ff // TILE
    early = ff // TILE
    for grp in range(groups):
        chip_sum(0, grp)
    loads[n_out].wait()
    turn(0, early)
    loads[n_out + 1].wait()
    turn(early, blocks)
    finish(0, 0)
    for grp in range(groups):
        mlp(grp, gathered(0, grp))
        if grp + 1 < groups:
            finish(0, grp + 1)
        if grp == groups - 1:
            finish(1, 0)
        chip_sum(1, grp)

    for stat in (s_own, s_kl, t_acc):
        stat[...] = jnp.zeros_like(stat)
    m_own[...] = jnp.full_like(m_own, NEG)
    m_kl[...] = jnp.full_like(m_kl, NEG)
    lanes = lax.broadcasted_iota(jnp.int32, (1, CHUNK), 1)
    tiles = CHUNK // 128

    def split(vals):
        return [vals[:, 128 * t:128 * (t + 1)] for t in range(tiles)]

    entries = [(step, offs[grp], SIZES[grp]) for grp in range(groups) for step in range(steps)]

    def z_copy(entry):
        step, off, size = entries[entry]
        rows = pl.ds(off, size)
        return pltpu.make_async_remote_copy(
            zsend.at[step, rows], zrecv.at[step, rows], z_send.at[entry], z_recv.at[entry],
            device_id=x_peer, device_id_type=MESH)

    def scaled(z, keep, step):
        _, repeated = chunk_start((1 - send_half) if keep else send_half, step)
        return jnp.where(lanes >= repeated, z * (1.0 / TEMPERATURE), NEG)

    def own_step(entry):
        step, off, size = entries[entry]
        rows = pl.ds(off, size)
        m_old, total, hits = m_own[rows], s_own[rows], t_acc[rows]
        goal = tgt_col[off:off + size]
        parts = []
        for keep, src in ((0, zsend), (1, zkeep)):
            start, repeated = chunk_start((1 - send_half) if keep else send_half, step)
            z = src[step, rows]
            ids = (lanes + (shard * vocab + start)).astype(F32)
            for hit in split(jnp.where((ids == goal) & (lanes >= repeated), z, 0.0)):
                hits = hits + hit
            parts += split(z)
        m_new = functools.reduce(jnp.maximum, parts, m_old)
        total = total * jnp.exp(m_old - m_new)
        for piece in parts:
            total = total + jnp.exp(piece - m_new)
        m_own[rows] = m_new
        s_own[rows] = total
        t_acc[rows] = hits

    def kl_wait(entry):
        with scope(f"wait_z{entry}"):
            z_copy(entry).wait_recv()

    def kl_step(entry):
        step, off, size = entries[entry]
        rows = pl.ds(off, size)
        mine, theirs = zkeep[step, rows], zrecv[step, rows]
        policy = half == 0
        tops = split(jnp.where(policy, mine, theirs))
        diffs = split(jnp.where(policy, mine - theirs, theirs - mine))
        m_old = m_kl[rows]
        m_new = functools.reduce(jnp.maximum, tops, m_old)
        total = s_kl[rows] * jnp.exp(m_old - m_new)
        for top, diff in zip(tops, diffs):
            total = total + jnp.exp(top - m_new) * diff
        m_kl[rows] = m_new
        s_kl[rows] = total

    def head_entry(entry, h_in):
        step, off, size = entries[entry]
        rows = pl.ds(off, size)
        if entry == step:
            with scope("wait_w"):
                head_copy(1, step).wait()
                if step + AHEAD < steps:
                    head_copy(0, step + AHEAD).wait()
        if entry >= LAG:
            kl_wait(entry - LAG)
        with scope(f"entry{entry}"):
            z = jnp.concatenate([turned_dot(h_in, wh.at[step], row) for row in range(0, CHUNK, TILE)], axis=1)
            zsend[step, rows] = scaled(z, 0, step)
            if entry == 0:
                z_copy(entry).start()
            zkeep[step, rows] = scaled(dot_t(h_in, wh[step, CHUNK:2 * CHUNK]), 1, step)
            if entry == step and step + AHEAD < steps:
                turn_head(step + AHEAD)
            if entry > 0:
                own_step(entry - 1)
            if entry >= LAG:
                kl_step(entry - LAG)
        if entry > 0:
            z_copy(entry).start()

    b_wait(1, 0)
    h_in = normed_rows(1, 0, SIZES[0])
    for entry in range(steps):
        if entry == LATE:
            finish(1, 1)
        head_entry(entry, h_in)
    b_wait(1, 1)
    h_in = normed_rows(1, SIZES[0], SIZES[1])
    for entry in range(steps, 2 * steps):
        head_entry(entry, h_in)

    own_step(len(entries) - 1)

    def to_row(col):
        return jnp.sum(jnp.where(eye, col, 0.0), axis=0, keepdims=True)

    def stat_rows(m_ref, s_ref):
        m_all = m_ref[...]
        m_col = jnp.max(m_all, axis=1, keepdims=True)
        s_col = jnp.sum(s_ref[...] * jnp.exp(m_all - m_col), axis=1, keepdims=True)
        return to_row(m_col), to_row(s_col)

    pack[here, 0:1, 0:tokens], pack[here, 1:2, 0:tokens] = stat_rows(m_own, s_own)
    pack[here, 4:5, 0:tokens] = to_row(jnp.sum(t_acc[...], axis=1, keepdims=True))
    for red in range(2):
        for grp in range(groups):
            d_copy(red, grp).wait_send()
            y_copy(red, grp).wait_send()
            b_copy(red, grp).wait_send()
    for entry in range(len(entries) - LAG, len(entries)):
        kl_wait(entry)
        kl_step(entry)
    pack[here, 2:3, 0:tokens], pack[here, 3:4, 0:tokens] = stat_rows(m_kl, s_kl)

    def p_copy(hop):
        other = (here + hop) % 8
        return pltpu.make_async_remote_copy(
            pack.at[here], pack.at[here], p_send.at[hop - 1], p_recv.at[hop - 1],
            device_id={"tp": other % 2, "role": other // 2}, device_id_type=MESH)

    for hop in range(1, 8):
        p_copy(hop).start()
    for entry in range(len(entries)):
        z_copy(entry).wait_send()

    with scope("wait_p"):
        for hop in range(1, 8):
            p_copy(hop).wait_recv()

    with scope("final"):
        def lse(devices):
            tops = [pack[dev, 0:1, 0:tokens] for dev in devices]
            top = functools.reduce(jnp.maximum, tops)
            total = functools.reduce(jnp.add, [pack[dev, 1:2, 0:tokens] * jnp.exp(t - top) for dev, t in zip(devices, tops)])
            return top + jnp.log(total)

        lse_pol = lse(range(4))
        lse_ref = lse(range(4, 8))
        cross = functools.reduce(jnp.add, [pack[dev, 3:4, 0:tokens] * jnp.exp(pack[dev, 2:3, 0:tokens] - lse_pol) for dev in range(8)])
        tgt_z = functools.reduce(jnp.add, [pack[dev, 4:5, 0:tokens] for dev in range(4)])
        mask_vals = mask_ref[...].astype(F32)
        out_ref[0:1, :] = (cross - lse_pol + lse_ref) * mask_vals
        out_ref[1:2, :] = (tgt_z - lse_pol) * mask_vals
    with scope("wait_ps"):
        for hop in range(1, 8):
            p_copy(hop).wait_send()


def solution(mesh):
    by_shard = P(("role", "tp"), None)
    by_role = P("role", None)

    def per_device(hidden, segment_ids, loss_mask, target, norm_gains, w_query, b_query, w_key, b_key, w_value, b_value, w_out, w_gate, w_up, w_down, w_head):
        tokens, dim = hidden.shape[1:]
        q_heads, head_dim = b_query.shape
        ff = w_gate.shape[0]
        vocab = w_head.shape[0]
        groups = len(SIZES)
        cols = dim // 2
        q_rows = q_heads * head_dim
        halves = ((vocab // CHUNK + 2) // 2) * CHUNK
        steps = halves // CHUNK
        wide = 2 * head_dim
        sem = pltpu.SemaphoreType.DMA
        out = pl.pallas_call(
            functools.partial(kernel, (tokens, dim, head_dim, q_heads, vocab)),
            out_shape=jax.ShapeDtypeStruct((2, tokens), F32),
            in_specs=[pl.BlockSpec(memory_space=pl.ANY)] * 16,
            out_specs=pl.BlockSpec(memory_space=pltpu.VMEM),
            scratch_shapes=[
                pltpu.VMEM((tokens, dim), BF16),
                pltpu.VMEM((3, 2, dim), F32),
                pltpu.VMEM((1, tokens), jnp.int32),
                pltpu.VMEM((1, tokens), jnp.int32),
                pltpu.VMEM((1, tokens), jnp.int32),
                pltpu.VMEM(b_query.shape, BF16),
                pltpu.VMEM(b_key.shape, BF16),
                pltpu.VMEM(b_value.shape, BF16),
                pltpu.VMEM((q_rows + 2 * wide, dim), BF16),
                pltpu.VMEM((2, q_rows, cols), BF16),
                pltpu.VMEM((2 * ff, dim), BF16),
                pltpu.VMEM((2, ff, cols), BF16),
                pltpu.VMEM((steps, 2 * CHUNK, dim), BF16),
                pltpu.VMEM((2, tokens, cols), F32),
                pltpu.VMEM((q_heads * tokens, wide), BF16),
                pltpu.VMEM((tokens, q_rows), BF16),
                pltpu.VMEM((2, 2, tokens, cols), F32),
                pltpu.VMEM((2, tokens, cols), F32),
                pltpu.VMEM((2, tokens, cols), F32),
                pltpu.VMEM((2, 2, tokens, cols), F32),
                pltpu.VMEM((tokens, 2 * ff), F32),
                pltpu.VMEM((steps, tokens, CHUNK), F32),
                pltpu.VMEM((steps, tokens, CHUNK), F32),
                pltpu.VMEM((steps, tokens, CHUNK), F32),
                pltpu.VMEM((tokens, 128), F32),
                pltpu.VMEM((tokens, 128), F32),
                pltpu.VMEM((tokens, 128), F32),
                pltpu.VMEM((tokens, 128), F32),
                pltpu.VMEM((tokens, 128), F32),
                pltpu.VMEM((16, 128), F32),
                pltpu.VMEM((8, 8, 128), F32),
                sem((22,)), sem((2, steps)),
                sem((2, groups)), sem((2, groups)), sem((2, groups)), sem((2, groups)), sem((2, groups)), sem((2, groups)),
                sem((groups * steps,)), sem((groups * steps,)), sem((7,)), sem((7,)),
            ],
            compiler_params=pltpu.CompilerParams(
                collective_id=0, has_side_effects=True, vmem_limit_bytes=67043328),
            name="layer_head_kl",
        )(hidden, jnp.transpose(norm_gains, (1, 0, 2)), w_query, w_key, w_value, w_out, w_gate, w_up, w_down, w_head,
          segment_ids.reshape(1, tokens), loss_mask.reshape(1, tokens), target.reshape(1, tokens), b_query, b_key, b_value)
        return out[0], out[1]

    in_specs = (P(None, "dp", None), P("dp"), P("dp"), P("dp"), P(None, None, None), by_shard, by_shard, by_role, by_role, by_role, by_role, by_shard, by_shard, by_shard, by_shard, by_shard)
    return jax.shard_map(per_device, mesh=mesh, in_specs=in_specs, out_specs=(P("dp"), P("dp")), check_vma=False)
```

```python
import contextlib
import functools
import math

import jax
import jax.numpy as jnp
from jax import lax
from jax.experimental import pallas as pl
from jax.experimental.pallas import tpu as pltpu
from jax.sharding import PartitionSpec as P

EPS = 1e-6
ROPE_BASE = 1000000.0
TEMPERATURE = 0.7
NEG = -1e30
SIZES = (24, 40)
AHEAD = 4
SPARE = 2
LATE = 6
TILE = 256
CHUNK = 512
LAG = 5
F32 = jnp.float32
BF16 = jnp.bfloat16
MESH = pl.DeviceIdType.MESH


def scope(name):
    return contextlib.nullcontext()


def dot_t(rows, weight):
    return lax.dot_general(rows, weight, (((1,), (1,)), ((), ())), preferred_element_type=F32)


def dot_n(rows, weight):
    return lax.dot_general(rows, weight, (((1,), (0,)), ((), ())), preferred_element_type=F32)


def normed(vals, gain):
    inv_rms = lax.rsqrt(jnp.mean(vals * vals, axis=-1, keepdims=True) + EPS)
    return (vals * inv_rms * gain).astype(BF16)


def kernel(cfg, hidden, gains, w_query, w_key, w_value, w_out, w_gate, w_up, w_down, w_head,
           seg_in, mask_in, tgt_in, bq_in, bk_in, bv_in, out_ref,
           xb, gn, seg_ref, mask_ref, tgt_ref, bq_ref, bk_ref, bv_ref, wqkv, wo, wgu, wd, wh, xcol, qs, os_, part, rbuf, ybuf, full,
           gate_up, zsend, zkeep, zrecv, m_own, s_own, m_kl, s_kl, t_acc, dup, pack, pack_kl,
           in_sem, head_sem, d_send, d_recv, y_send, y_recv, b_send, b_recv, z_send, z_recv, p_send, p_recv):
    tokens, dim, head_dim, q_heads, vocab = cfg
    offs = [sum(SIZES[:grp]) for grp in range(len(SIZES))]
    groups = len(SIZES)
    cols = dim // 2
    ff = w_gate.shape[0]
    halves = ((vocab // CHUNK + 2) // 2) * CHUNK
    steps = halves // CHUNK
    tp = lax.axis_index("tp")
    role = lax.axis_index("role")
    core = role % 2
    half = role // 2
    here = role * 2 + tp
    shard = core * 2 + tp
    d_peer = {"role": half * 2 + 1 - core}
    y_peer = {"tp": 1 - tp}
    x_peer = {"role": (1 - half) * 2 + core}
    send_half = 1 - half
    q_rows = q_heads * head_dim
    wide = 2 * head_dim

    kv_rows = pl.ds(pl.multiple_of(tp * head_dim, head_dim), head_dim)
    theirs_cols = pl.ds(pl.multiple_of((1 - core) * cols, cols), cols)
    mine_cols = pl.ds(pl.multiple_of(core * cols, cols), cols)
    moves = [(hidden.at[half], xb), (gains, gn), (seg_in, seg_ref), (mask_in, mask_ref), (tgt_in, tgt_ref),
             (bq_in, bq_ref), (bk_in, bk_ref), (bv_in, bv_ref)]
    n_small = len(moves)
    for slot in range(2):
        moves.append((w_key.at[kv_rows], wqkv.at[pl.ds(slot * head_dim, head_dim)]))
        moves.append((w_value.at[kv_rows], wqkv.at[pl.ds((2 + slot) * head_dim, head_dim)]))
    for piece in range(2):
        moves.append((w_query.at[pl.ds(piece * q_rows // 2, q_rows // 2)],
                      wqkv.at[pl.ds(2 * wide + piece * q_rows // 2, q_rows // 2)]))
    n_qkv = len(moves)
    moves += [(w_out.at[:, theirs_cols], wo.at[0]), (w_out.at[:, mine_cols], wo.at[1])]
    n_out = len(moves)
    moves += [(w_gate, wgu.at[pl.ds(0, ff)]), (w_up, wgu.at[pl.ds(ff, ff)])]
    n_gu = len(moves)
    moves += [(w_down.at[:, theirs_cols], wd.at[0]), (w_down.at[:, mine_cols], wd.at[1])]
    loads = [pltpu.make_async_copy(src, dst, in_sem.at[idx]) for idx, (src, dst) in enumerate(moves)]
    for copy in loads[:n_qkv]:
        copy.start()

    barrier = pltpu.get_barrier_semaphore()
    for hop in range(1, 8):
        other = (here + hop) % 8
        pl.semaphore_signal(barrier, inc=1, device_id={"tp": other % 2, "role": other // 2}, device_id_type=MESH)

    def chunk_start(part_half, step):
        nominal = part_half * halves + step * CHUNK
        start = jnp.minimum(nominal, vocab - CHUNK)
        return start, nominal - start

    def head_copy(keep, step):
        start, _ = chunk_start((1 - send_half) if keep else send_half, step)
        return pltpu.make_async_copy(w_head.at[pl.ds(pl.multiple_of(start, 64), CHUNK)],
                                     wh.at[step, pl.ds(keep * CHUNK, CHUNK)], head_sem.at[keep, step])

    ti = lax.broadcasted_iota(jnp.int32, (tokens, tokens), 0)
    tj = lax.broadcasted_iota(jnp.int32, (tokens, tokens), 1)
    eye = ti == tj
    lane = lax.broadcasted_iota(jnp.int32, (1, wide), 1)
    half_dim = head_dim // 2
    freq = jnp.exp((lane % half_dim).astype(F32) * (-2.0 * math.log(ROPE_BASE) / head_dim))
    low = (lane % head_dim) < half_dim
    even = lane < head_dim

    def gain_row(which):
        return jnp.where(half == 0, gn[which, 0:1, :], gn[which, 1:2, :])

    with scope("wait_x"):
        for copy in loads[:n_small]:
            copy.wait()
    with scope("norm_x"):
        seg_row = seg_ref[...].astype(F32)
        seg_col = jnp.sum(jnp.where(eye, seg_row, 0.0), axis=1, keepdims=True)
        same = seg_col == seg_row
        allowed = same & (ti >= tj)
        seg_first = jnp.min(jnp.where(same, tj.astype(F32), 1e9), axis=1, keepdims=True)
        pos = lax.broadcasted_iota(jnp.int32, (tokens, 1), 0).astype(F32) - seg_first
        angles = pos * freq
        cos_t = jnp.cos(angles)
        sin_t = jnp.sin(angles)
        sin_t = jnp.where(low, -sin_t, sin_t)
        tgt_col = jnp.sum(jnp.where(eye, tgt_ref[...].astype(F32), 0.0), axis=1, keepdims=True)
        dup[...] = jnp.zeros_like(dup)
        dup[0:q_heads, 0:head_dim] = bq_ref[...].astype(F32)
        dup[q_heads:q_heads + 2, 0:head_dim] = bk_ref[...].astype(F32)
        dup[q_heads + 2:q_heads + 4, 0:head_dim] = bv_ref[...].astype(F32)
        bias = dup[...]
        bias = bias + pltpu.roll(bias, head_dim, 1)
        bias_k = jnp.where(tp == 0, bias[q_heads:q_heads + 1], bias[q_heads + 1:q_heads + 2])
        bias_v = jnp.where(tp == 0, bias[q_heads + 2:q_heads + 3], bias[q_heads + 3:q_heads + 4])
        xf = xb[...].astype(F32)
        xcol[0] = xf[:, :cols]
        xcol[1] = xf[:, cols:]
        a_in = normed(xf, gain_row(0))

    def rotate(vals):
        turned = jnp.where(low, pltpu.roll(vals, wide - half_dim, 1), pltpu.roll(vals, half_dim, 1))
        return vals * cos_t + turned * sin_t

    with scope("wait_kv"):
        for copy in loads[n_small:n_small + 5]:
            copy.wait()
    for copy in loads[n_qkv:]:
        copy.start()

    @pl.loop(0, steps)
    def _(step):
        head_copy(0, step).start()
        head_copy(1, step).start()

    def put_q(first_pair, vals):
        for idx in range(q_heads // 4):
            pair = first_pair + idx
            bias_q = jnp.where(even, bias[2 * pair:2 * pair + 1], bias[2 * pair + 1:2 * pair + 2])
            q_rot = rotate(vals[:, idx * wide:(idx + 1) * wide] + bias_q) * head_dim ** -0.5
            qs[2 * pair * tokens:(2 * pair + 1) * tokens, :] = jnp.where(even, q_rot, 0.0).astype(BF16)
            qs[(2 * pair + 1) * tokens:(2 * pair + 2) * tokens, :] = jnp.where(even, 0.0, q_rot).astype(BF16)

    cut = 2 * wide + q_rows // 2
    with scope("qkv"):
        kvq = dot_t(a_in, wqkv[0:cut])
        loads[n_small + 5].wait()
        rest = dot_t(a_in, wqkv[cut:cut + q_rows // 2])
        k_rot = rotate(kvq[:, :wide] + bias_k).astype(BF16)
        v_two = (kvq[:, wide:2 * wide] + bias_v).astype(BF16)
        put_q(0, kvq[:, 2 * wide:])
        put_q(q_heads // 4, rest)
    with scope("attn"):
        scores = dot_t(qs[...], k_rot).reshape(q_heads, tokens, tokens)
        scores = jnp.where(allowed[None], scores, NEG)
        expd = jnp.exp(scores - jnp.max(scores, axis=-1, keepdims=True))
        probs = (expd / jnp.sum(expd, axis=-1, keepdims=True)).astype(BF16).reshape(q_heads * tokens, tokens)
        heads_out = dot_n(probs, v_two)
        for pair in range(q_heads // 2):
            lo = heads_out[2 * pair * tokens:(2 * pair + 1) * tokens]
            hi = heads_out[(2 * pair + 1) * tokens:(2 * pair + 2) * tokens]
            os_[:, pair * wide:(pair + 1) * wide] = jnp.where(even, lo, hi).astype(BF16)

    def rows_of(grp):
        return pl.ds(offs[grp], SIZES[grp])

    def d_copy(red, grp):
        return pltpu.make_async_remote_copy(
            part.at[red, 0, rows_of(grp)], rbuf.at[red, rows_of(grp)], d_send, d_recv.at[red, grp],
            device_id=d_peer, device_id_type=MESH)

    def y_copy(red, grp):
        return pltpu.make_async_remote_copy(
            part.at[red, 1, rows_of(grp)], ybuf.at[red, rows_of(grp)], y_send, y_recv.at[red, grp],
            device_id=y_peer, device_id_type=MESH)

    def b_copy(red, grp):
        return pltpu.make_async_remote_copy(
            full.at[red, core, rows_of(grp)], full.at[red, core, rows_of(grp)], b_send, b_recv.at[red, grp],
            device_id=d_peer, device_id_type=MESH)

    def chip_sum(red, grp):
        rows = rows_of(grp)
        with scope(f"wait_d{red}{grp}"):
            d_copy(red, grp).wait_recv()
        part[red, 1, rows] = part[red, 1, rows] + rbuf[red, rows]
        y_copy(red, grp).start()

    def finish(red, grp):
        rows = rows_of(grp)
        with scope(f"wait_y{red}{grp}"):
            y_copy(red, grp).wait_recv()
        base = xcol[core, rows] if red == 0 else full[0, core, rows]
        full[red, core, rows] = (base + (part[red, 1, rows] + ybuf[red, rows])).astype(BF16).astype(F32)
        b_copy(red, grp).start()

    def b_wait(red, grp):
        with scope(f"wait_b{red}{grp}"):
            b_copy(red, grp).wait_recv()

    def normed_rows(red, off, size):
        rows = pl.ds(off, size)
        left, right = full[red, 0, rows], full[red, 1, rows]
        total = jnp.sum(left * left, axis=-1, keepdims=True) + jnp.sum(right * right, axis=-1, keepdims=True)
        inv_rms = lax.rsqrt(total * (1.0 / dim) + EPS)
        gain = gain_row(red + 1)
        return jnp.concatenate([(left * inv_rms * gain[:, :cols]).astype(BF16),
                                (right * inv_rms * gain[:, cols:]).astype(BF16)], axis=1)

    def gathered(red, grp):
        b_wait(red, grp)
        return normed_rows(red, offs[grp], SIZES[grp])

    def turn_tiles(ref, rows):
        for k in range(dim // TILE):
            ref[rows, k * TILE:(k + 1) * TILE] = ref[rows, k * TILE:(k + 1) * TILE].T

    def turn(first, last):
        with scope("turn"):
            @pl.loop(first, last)
            def _(blk):
                turn_tiles(wgu, pl.ds(pl.multiple_of(blk * TILE, TILE), TILE))

    def turn_head(step):
        for row in range(0, CHUNK, TILE):
            turn_tiles(wh.at[step], pl.ds(row, TILE))

    def turned_dot(vals, ref, row):
        return functools.reduce(jnp.add, [dot_n(vals[:, k * TILE:(k + 1) * TILE], ref[row:row + TILE, k * TILE:(k + 1) * TILE])
                                          for k in range(dim // TILE)])

    def mlp(grp, b_in):
        rows = rows_of(grp)
        if grp == 0:
            for copy in loads[n_gu:]:
                copy.wait()
        if grp == groups - 1:
            for step in range(AHEAD):
                head_copy(0, step).wait()
        with scope(f"mlp{grp}"):
            if grp == groups - 1:
                for step in range(AHEAD):
                    turn_head(step)
            for row in range(0, 2 * ff, TILE):
                gate_up[rows, row:row + TILE] = turned_dot(b_in, wgu, row)
            gate, up = gate_up[rows, 0:ff], gate_up[rows, ff:2 * ff]
            act = (gate * (1.0 / (1.0 + jnp.exp(-gate))) * up).astype(BF16)
            part[1, 0, rows] = dot_n(act, wd[0])
        d_copy(1, grp).start()
        with scope(f"down{grp}"):
            part[1, 1, rows] = dot_n(act, wd[1])

    for copy in loads[n_qkv:n_out]:
        copy.wait()
    with scope("oproj"):
        part[0, 0] = dot_n(os_[...], wo[0])
    with scope("entry"):
        pl.semaphore_wait(barrier, 7)
    for grp in range(groups):
        d_copy(0, grp).start()
    with scope("oproj"):
        part[0, 1] = dot_n(os_[...], wo[1])
    blocks = 2 * ff // TILE
    early = ff // TILE
    for grp in range(groups):
        chip_sum(0, grp)
    loads[n_out].wait()
    turn(0, early)
    loads[n_out + 1].wait()
    turn(early, blocks - SPARE)
    finish(0, 0)
    turn(blocks - SPARE, blocks)
    for grp in range(groups):
        mlp(grp, gathered(0, grp))
        if grp + 1 < groups:
            finish(0, grp + 1)
        if grp == groups - 1:
            finish(1, 0)
        chip_sum(1, grp)

    for stat in (s_own, s_kl, t_acc):
        stat[...] = jnp.zeros_like(stat)
    m_own[...] = jnp.full_like(m_own, NEG)
    m_kl[...] = jnp.full_like(m_kl, NEG)
    lanes = lax.broadcasted_iota(jnp.int32, (1, CHUNK), 1)
    tiles = CHUNK // 128

    def split(vals):
        return [vals[:, 128 * t:128 * (t + 1)] for t in range(tiles)]

    entries = [(step, offs[grp], SIZES[grp]) for grp in range(groups) for step in range(steps)]

    def z_copy(entry):
        step, off, size = entries[entry]
        rows = pl.ds(off, size)
        return pltpu.make_async_remote_copy(
            zsend.at[step, rows], zrecv.at[step, rows], z_send, z_recv.at[entry],
            device_id=x_peer, device_id_type=MESH)

    def scaled(z, keep, step):
        _, repeated = chunk_start((1 - send_half) if keep else send_half, step)
        return jnp.where(lanes >= repeated, z * (1.0 / TEMPERATURE), NEG)

    def own_step(entry):
        step, off, size = entries[entry]
        rows = pl.ds(off, size)
        m_old, total, hits = m_own[rows], s_own[rows], t_acc[rows]
        goal = tgt_col[off:off + size]
        parts = []
        for keep, src in ((0, zsend), (1, zkeep)):
            start, repeated = chunk_start((1 - send_half) if keep else send_half, step)
            z = src[step, rows]
            ids = (lanes + (shard * vocab + start)).astype(F32)
            for hit in split(jnp.where((ids == goal) & (lanes >= repeated), z, 0.0)):
                hits = hits + hit
            parts += split(z)
        m_new = functools.reduce(jnp.maximum, parts, m_old)
        total = total * jnp.exp(m_old - m_new)
        for piece in parts:
            total = total + jnp.exp(piece - m_new)
        m_own[rows] = m_new
        s_own[rows] = total
        t_acc[rows] = hits

    def kl_wait(entry):
        with scope(f"wait_z{entry}"):
            z_copy(entry).wait_recv()

    def kl_step(entry):
        step, off, size = entries[entry]
        rows = pl.ds(off, size)
        mine, theirs = zkeep[step, rows], zrecv[step, rows]
        policy = half == 0
        tops = split(jnp.where(policy, mine, theirs))
        diffs = split(jnp.where(policy, mine - theirs, theirs - mine))
        m_old = m_kl[rows]
        m_new = functools.reduce(jnp.maximum, tops, m_old)
        total = s_kl[rows] * jnp.exp(m_old - m_new)
        for top, diff in zip(tops, diffs):
            total = total + jnp.exp(top - m_new) * diff
        m_kl[rows] = m_new
        s_kl[rows] = total

    def head_entry(entry, h_in):
        step, off, size = entries[entry]
        rows = pl.ds(off, size)
        if entry == step:
            with scope("wait_w"):
                head_copy(1, step).wait()
                if step + AHEAD < steps:
                    head_copy(0, step + AHEAD).wait()
        if entry >= LAG:
            kl_wait(entry - LAG)
        with scope(f"entry{entry}"):
            z = jnp.concatenate([turned_dot(h_in, wh.at[step], row) for row in range(0, CHUNK, TILE)], axis=1)
            zsend[step, rows] = scaled(z, 0, step)
            if entry == 0:
                z_copy(entry).start()
            zkeep[step, rows] = scaled(dot_t(h_in, wh[step, CHUNK:2 * CHUNK]), 1, step)
            if entry == step and step + AHEAD < steps:
                turn_head(step + AHEAD)
            if entry > 0:
                own_step(entry - 1)
            if entry >= LAG:
                kl_step(entry - LAG)
        if entry > 0:
            z_copy(entry).start()

    b_wait(1, 0)
    h_in = normed_rows(1, 0, SIZES[0])
    for entry in range(steps):
        if entry == LATE:
            finish(1, 1)
        head_entry(entry, h_in)
    b_wait(1, 1)
    h_in = normed_rows(1, SIZES[0], SIZES[1])
    for entry in range(steps, 2 * steps):
        head_entry(entry, h_in)

    own_step(len(entries) - 1)

    def to_row(col):
        return jnp.sum(jnp.where(eye, col, 0.0), axis=0, keepdims=True)

    def stat_rows(m_ref, s_ref):
        m_all = m_ref[...]
        m_col = jnp.max(m_all, axis=1, keepdims=True)
        s_col = jnp.sum(s_ref[...] * jnp.exp(m_all - m_col), axis=1, keepdims=True)
        return to_row(m_col), to_row(s_col)

    packs = (pack, pack_kl)

    def p_copy(which, hop):
        other = (here + hop) % 8
        return pltpu.make_async_remote_copy(
            packs[which].at[here], packs[which].at[here], p_send.at[which], p_recv.at[which],
            device_id={"tp": other % 2, "role": other // 2}, device_id_type=MESH)

    def p_all(which):
        seven = packs[which].at[pl.ds(0, 7)]
        return pltpu.make_async_remote_copy(
            seven, seven, p_send.at[which], p_recv.at[which], device_id=x_peer, device_id_type=MESH)

    pack[here, 0:1, 0:tokens], pack[here, 1:2, 0:tokens] = stat_rows(m_own, s_own)
    pack[here, 2:3, 0:tokens] = to_row(jnp.sum(t_acc[...], axis=1, keepdims=True))
    for hop in range(1, 8):
        p_copy(0, hop).start()
    for send in (d_send, y_send, b_send):
        pltpu.make_async_remote_copy(rbuf, rbuf, send, d_recv.at[0, 0], device_id=d_peer, device_id_type=MESH).wait_send()
    for entry in range(len(entries) - LAG, len(entries)):
        kl_wait(entry)
        kl_step(entry)
    pack_kl[here, 0:1, 0:tokens], pack_kl[here, 1:2, 0:tokens] = stat_rows(m_kl, s_kl)
    for hop in range(1, 8):
        p_copy(1, hop).start()
    pltpu.make_async_remote_copy(zsend, zsend, z_send, z_recv.at[0], device_id=x_peer, device_id_type=MESH).wait_send()
    p_all(0).wait_send()
    with scope("wait_p0"):
        p_all(0).wait_recv()
    with scope("wait_p"):
        p_all(1).wait_recv()

    with scope("final"):
        def lse(devices):
            tops = [pack[dev, 0:1, 0:tokens] for dev in devices]
            top = functools.reduce(jnp.maximum, tops)
            total = functools.reduce(jnp.add, [pack[dev, 1:2, 0:tokens] * jnp.exp(t - top) for dev, t in zip(devices, tops)])
            return top + jnp.log(total)

        lse_pol = lse(range(4))
        lse_ref = lse(range(4, 8))
        cross = functools.reduce(jnp.add, [pack_kl[dev, 1:2, 0:tokens] * jnp.exp(pack_kl[dev, 0:1, 0:tokens] - lse_pol) for dev in range(8)])
        tgt_z = functools.reduce(jnp.add, [pack[dev, 2:3, 0:tokens] for dev in range(4)])
        mask_vals = mask_ref[...].astype(F32)
        out_ref[0:1, :] = (cross - lse_pol + lse_ref) * mask_vals
        out_ref[1:2, :] = (tgt_z - lse_pol) * mask_vals
    p_all(1).wait_send()


def solution(mesh):
    by_shard = P(("role", "tp"), None)
    by_role = P("role", None)

    def per_device(hidden, segment_ids, loss_mask, target, norm_gains, w_query, b_query, w_key, b_key, w_value, b_value, w_out, w_gate, w_up, w_down, w_head):
        tokens, dim = hidden.shape[1:]
        q_heads, head_dim = b_query.shape
        ff = w_gate.shape[0]
        vocab = w_head.shape[0]
        groups = len(SIZES)
        cols = dim // 2
        q_rows = q_heads * head_dim
        halves = ((vocab // CHUNK + 2) // 2) * CHUNK
        steps = halves // CHUNK
        wide = 2 * head_dim
        sem = pltpu.SemaphoreType.DMA
        out = pl.pallas_call(
            functools.partial(kernel, (tokens, dim, head_dim, q_heads, vocab)),
            out_shape=pltpu.VMEM((2, tokens), F32),
            in_specs=[pl.BlockSpec(memory_space=pl.ANY)] * 16,
            out_specs=pl.BlockSpec(memory_space=pltpu.VMEM),
            scratch_shapes=[
                pltpu.VMEM((tokens, dim), BF16),
                pltpu.VMEM((3, 2, dim), F32),
                pltpu.VMEM((1, tokens), jnp.int32),
                pltpu.VMEM((1, tokens), jnp.int32),
                pltpu.VMEM((1, tokens), jnp.int32),
                pltpu.VMEM(b_query.shape, BF16),
                pltpu.VMEM(b_key.shape, BF16),
                pltpu.VMEM(b_value.shape, BF16),
                pltpu.VMEM((q_rows + 2 * wide, dim), BF16),
                pltpu.VMEM((2, q_rows, cols), BF16),
                pltpu.VMEM((2 * ff, dim), BF16),
                pltpu.VMEM((2, ff, cols), BF16),
                pltpu.VMEM((steps, 2 * CHUNK, dim), BF16),
                pltpu.VMEM((2, tokens, cols), F32),
                pltpu.VMEM((q_heads * tokens, wide), BF16),
                pltpu.VMEM((tokens, q_rows), BF16),
                pltpu.VMEM((2, 2, tokens, cols), F32),
                pltpu.VMEM((2, tokens, cols), F32),
                pltpu.VMEM((2, tokens, cols), F32),
                pltpu.VMEM((2, 2, tokens, cols), F32),
                pltpu.VMEM((tokens, 2 * ff), F32),
                pltpu.VMEM((steps, tokens, CHUNK), F32),
                pltpu.VMEM((steps, tokens, CHUNK), F32),
                pltpu.VMEM((steps, tokens, CHUNK), F32),
                pltpu.VMEM((tokens, 128), F32),
                pltpu.VMEM((tokens, 128), F32),
                pltpu.VMEM((tokens, 128), F32),
                pltpu.VMEM((tokens, 128), F32),
                pltpu.VMEM((tokens, 128), F32),
                pltpu.VMEM((16, 128), F32),
                pltpu.VMEM((8, 4, 128), F32),
                pltpu.VMEM((8, 2, 128), F32),
                sem((20,)), sem((2, steps)),
                sem(()), sem((2, groups)), sem(()), sem((2, groups)), sem(()), sem((2, groups)),
                sem(()), sem((groups * steps,)), sem((2,)), sem((2,)),
            ],
            compiler_params=pltpu.CompilerParams(
                collective_id=0, has_side_effects=True, vmem_limit_bytes=64500000),
            name="layer_head_kl",
        )(hidden, jnp.transpose(norm_gains, (1, 0, 2)), w_query, w_key, w_value, w_out, w_gate, w_up, w_down, w_head,
          segment_ids.reshape(1, tokens), loss_mask.reshape(1, tokens), target.reshape(1, tokens), b_query, b_key, b_value)
        return out[0], out[1]

    in_specs = (P(None, "dp", None), P("dp"), P("dp"), P("dp"), P(None, None, None), by_shard, by_shard, by_role, by_role, by_role, by_role, by_shard, by_shard, by_shard, by_shard, by_shard)
    return jax.shard_map(per_device, mesh=mesh, in_specs=in_specs, out_specs=(P("dp"), P("dp")), check_vma=False)
```

```python
import contextlib
import functools
import math

import jax
import jax.numpy as jnp
from jax import lax
from jax.experimental import pallas as pl
from jax.experimental.pallas import tpu as pltpu
from jax.sharding import PartitionSpec as P

EPS = 1e-6
ROPE_BASE = 1000000.0
TEMPERATURE = 0.7
NEG = -1e30
SIZES = (24, 40)
AHEAD = 4
SPARE = 2
TILE = 256
CHUNK = 512
F32 = jnp.float32
BF16 = jnp.bfloat16
MESH = pl.DeviceIdType.MESH


def scope(name):
    return contextlib.nullcontext()


def dot_t(rows, weight):
    return lax.dot_general(rows, weight, (((1,), (1,)), ((), ())), preferred_element_type=F32)


def dot_n(rows, weight):
    return lax.dot_general(rows, weight, (((1,), (0,)), ((), ())), preferred_element_type=F32)


def normed(vals, gain):
    inv_rms = lax.rsqrt(jnp.mean(vals * vals, axis=-1, keepdims=True) + EPS)
    return (vals * inv_rms * gain).astype(BF16)


def kernel(cfg, hidden, gains, w_query, w_key, w_value, w_out, w_gate, w_up, w_down, w_head,
           seg_in, mask_in, tgt_in, bq_in, bk_in, bv_in, out_ref,
           xb, gn, seg_ref, mask_ref, tgt_ref, bq_ref, bk_ref, bv_ref, wqkv, wo, wgu, wd, wh, xcol, qs, os_, part, rbuf, ybuf, full,
           gate_up, zsend, zkeep, zrecv, m_own, s_own, m_kl, s_kl, t_acc, dup, pack, pack_kl,
           in_sem, head_sem, d_send, d_recv, y_send, y_recv, b_send, b_recv, z_send, z_recv, p_send, p_recv):
    tokens, dim, head_dim, q_heads, vocab = cfg
    offs = [sum(SIZES[:grp]) for grp in range(len(SIZES))]
    groups = len(SIZES)
    cols = dim // 2
    ff = w_gate.shape[0]
    halves = ((vocab // CHUNK + 2) // 2) * CHUNK
    steps = halves // CHUNK
    tp = lax.axis_index("tp")
    role = lax.axis_index("role")
    core = role % 2
    half = role // 2
    here = role * 2 + tp
    shard = core * 2 + tp
    d_peer = {"role": half * 2 + 1 - core}
    y_peer = {"tp": 1 - tp}
    x_peer = {"role": (1 - half) * 2 + core}
    send_half = 1 - half
    q_rows = q_heads * head_dim
    wide = 2 * head_dim

    kv_rows = pl.ds(pl.multiple_of(tp * head_dim, head_dim), head_dim)
    theirs_cols = pl.ds(pl.multiple_of((1 - core) * cols, cols), cols)
    mine_cols = pl.ds(pl.multiple_of(core * cols, cols), cols)
    moves = [(hidden.at[half], xb), (gains, gn), (seg_in, seg_ref), (mask_in, mask_ref), (tgt_in, tgt_ref),
             (bq_in, bq_ref), (bk_in, bk_ref), (bv_in, bv_ref)]
    n_small = len(moves)
    for slot in range(2):
        moves.append((w_key.at[kv_rows], wqkv.at[pl.ds(slot * head_dim, head_dim)]))
        moves.append((w_value.at[kv_rows], wqkv.at[pl.ds((2 + slot) * head_dim, head_dim)]))
    for piece in range(2):
        moves.append((w_query.at[pl.ds(piece * q_rows // 2, q_rows // 2)],
                      wqkv.at[pl.ds(2 * wide + piece * q_rows // 2, q_rows // 2)]))
    n_qkv = len(moves)
    moves += [(w_out.at[:, theirs_cols], wo.at[0]), (w_out.at[:, mine_cols], wo.at[1])]
    n_out = len(moves)
    moves += [(w_gate, wgu.at[pl.ds(0, ff)]), (w_up, wgu.at[pl.ds(ff, ff)])]
    n_gu = len(moves)
    moves += [(w_down.at[:, theirs_cols], wd.at[0]), (w_down.at[:, mine_cols], wd.at[1])]
    bounds = [n_small, n_small + 5, n_qkv, n_out, n_out + 1, n_gu]
    loads = [pltpu.make_async_copy(src, dst, in_sem.at[sum(idx >= bound for bound in bounds)])
             for idx, (src, dst) in enumerate(moves)]
    for copy in loads[:n_qkv]:
        copy.start()

    barrier = pltpu.get_barrier_semaphore()
    for hop in range(1, 8):
        other = (here + hop) % 8
        pl.semaphore_signal(barrier, inc=1, device_id={"tp": other % 2, "role": other // 2}, device_id_type=MESH)

    def chunk_start(part_half, step):
        nominal = part_half * halves + step * CHUNK
        start = jnp.minimum(nominal, vocab - CHUNK)
        return start, nominal - start

    def head_copy(keep, step):
        start, _ = chunk_start((1 - send_half) if keep else send_half, step)
        return pltpu.make_async_copy(w_head.at[pl.ds(pl.multiple_of(start, 64), CHUNK)],
                                     wh.at[step, pl.ds(keep * CHUNK, CHUNK)], head_sem.at[step])

    ti = lax.broadcasted_iota(jnp.int32, (tokens, tokens), 0)
    tj = lax.broadcasted_iota(jnp.int32, (tokens, tokens), 1)
    eye = ti == tj
    lane = lax.broadcasted_iota(jnp.int32, (1, wide), 1)
    half_dim = head_dim // 2
    freq = jnp.exp((lane % half_dim).astype(F32) * (-2.0 * math.log(ROPE_BASE) / head_dim))
    low = (lane % head_dim) < half_dim
    even = lane < head_dim

    def gain_row(which):
        return jnp.where(half == 0, gn[which, 0:1, :], gn[which, 1:2, :])

    with scope("wait_x"):
        for copy in loads[:n_small]:
            copy.wait()
    with scope("norm_x"):
        seg_row = seg_ref[...].astype(F32)
        seg_col = jnp.sum(jnp.where(eye, seg_row, 0.0), axis=1, keepdims=True)
        same = seg_col == seg_row
        allowed = same & (ti >= tj)
        seg_first = jnp.min(jnp.where(same, tj.astype(F32), 1e9), axis=1, keepdims=True)
        pos = lax.broadcasted_iota(jnp.int32, (tokens, 1), 0).astype(F32) - seg_first
        angles = pos * freq
        cos_t = jnp.cos(angles)
        sin_t = jnp.sin(angles)
        sin_t = jnp.where(low, -sin_t, sin_t)
        tgt_col = jnp.sum(jnp.where(eye, tgt_ref[...].astype(F32), 0.0), axis=1, keepdims=True)
        dup[...] = jnp.zeros_like(dup)
        dup[0:q_heads, 0:head_dim] = bq_ref[...].astype(F32)
        dup[q_heads:q_heads + 2, 0:head_dim] = bk_ref[...].astype(F32)
        dup[q_heads + 2:q_heads + 4, 0:head_dim] = bv_ref[...].astype(F32)
        bias = dup[...]
        bias = bias + pltpu.roll(bias, head_dim, 1)
        bias_k = jnp.where(tp == 0, bias[q_heads:q_heads + 1], bias[q_heads + 1:q_heads + 2])
        bias_v = jnp.where(tp == 0, bias[q_heads + 2:q_heads + 3], bias[q_heads + 3:q_heads + 4])
        xf = xb[...].astype(F32)
        xcol[0] = xf[:, :cols]
        xcol[1] = xf[:, cols:]
        a_in = normed(xf, gain_row(0))

    def rotate(vals):
        turned = jnp.where(low, pltpu.roll(vals, wide - half_dim, 1), pltpu.roll(vals, half_dim, 1))
        return vals * cos_t + turned * sin_t

    with scope("wait_kv"):
        for copy in loads[n_small:n_small + 5]:
            copy.wait()
    for copy in loads[n_qkv:]:
        copy.start()

    @pl.loop(0, steps)
    def _(step):
        head_copy(0, step).start()
        head_copy(1, step).start()

    def put_q(first_pair, vals):
        for idx in range(q_heads // 4):
            pair = first_pair + idx
            bias_q = jnp.where(even, bias[2 * pair:2 * pair + 1], bias[2 * pair + 1:2 * pair + 2])
            q_rot = rotate(vals[:, idx * wide:(idx + 1) * wide] + bias_q) * head_dim ** -0.5
            qs[2 * pair * tokens:(2 * pair + 1) * tokens, :] = jnp.where(even, q_rot, 0.0).astype(BF16)
            qs[(2 * pair + 1) * tokens:(2 * pair + 2) * tokens, :] = jnp.where(even, 0.0, q_rot).astype(BF16)

    cut = 2 * wide + q_rows // 2
    with scope("qkv"):
        kvq = dot_t(a_in, wqkv[0:cut])
        loads[n_small + 5].wait()
        rest = dot_t(a_in, wqkv[cut:cut + q_rows // 2])
        k_rot = rotate(kvq[:, :wide] + bias_k).astype(BF16)
        v_two = (kvq[:, wide:2 * wide] + bias_v).astype(BF16)
        put_q(0, kvq[:, 2 * wide:])
        put_q(q_heads // 4, rest)
    with scope("attn"):
        scores = dot_t(qs[...], k_rot).reshape(q_heads, tokens, tokens)
        scores = jnp.where(allowed[None], scores, NEG)
        expd = jnp.exp(scores - jnp.max(scores, axis=-1, keepdims=True))
        probs = (expd / jnp.sum(expd, axis=-1, keepdims=True)).astype(BF16).reshape(q_heads * tokens, tokens)
        heads_out = dot_n(probs, v_two)
        for pair in range(q_heads // 2):
            lo = heads_out[2 * pair * tokens:(2 * pair + 1) * tokens]
            hi = heads_out[(2 * pair + 1) * tokens:(2 * pair + 2) * tokens]
            os_[:, pair * wide:(pair + 1) * wide] = jnp.where(even, lo, hi).astype(BF16)

    def rows_of(grp):
        return pl.ds(offs[grp], SIZES[grp])

    def d_copy(red, grp):
        return pltpu.make_async_remote_copy(
            part.at[red, 0, rows_of(grp)], rbuf.at[red, rows_of(grp)], d_send, d_recv.at[red, grp],
            device_id=d_peer, device_id_type=MESH)

    def y_copy(red, grp):
        return pltpu.make_async_remote_copy(
            part.at[red, 1, rows_of(grp)], ybuf.at[red, rows_of(grp)], y_send, y_recv.at[red, grp],
            device_id=y_peer, device_id_type=MESH)

    def b_copy(red, grp):
        return pltpu.make_async_remote_copy(
            full.at[red, core, rows_of(grp)], full.at[red, core, rows_of(grp)], b_send, b_recv.at[red, grp],
            device_id=d_peer, device_id_type=MESH)

    def chip_sum(red, grp):
        rows = rows_of(grp)
        with scope(f"wait_d{red}{grp}"):
            d_copy(red, grp).wait_recv()
        part[red, 1, rows] = part[red, 1, rows] + rbuf[red, rows]
        y_copy(red, grp).start()

    def finish(red, grp):
        rows = rows_of(grp)
        with scope(f"wait_y{red}{grp}"):
            y_copy(red, grp).wait_recv()
        base = xcol[core, rows] if red == 0 else full[0, core, rows]
        full[red, core, rows] = (base + (part[red, 1, rows] + ybuf[red, rows])).astype(BF16).astype(F32)
        b_copy(red, grp).start()

    def b_wait(red, grp):
        with scope(f"wait_b{red}{grp}"):
            b_copy(red, grp).wait_recv()

    def normed_rows(red, off, size):
        rows = pl.ds(off, size)
        left, right = full[red, 0, rows], full[red, 1, rows]
        total = jnp.sum(left * left, axis=-1, keepdims=True) + jnp.sum(right * right, axis=-1, keepdims=True)
        inv_rms = lax.rsqrt(total * (1.0 / dim) + EPS)
        gain = gain_row(red + 1)
        return jnp.concatenate([(left * inv_rms * gain[:, :cols]).astype(BF16),
                                (right * inv_rms * gain[:, cols:]).astype(BF16)], axis=1)

    def gathered(red, grp):
        b_wait(red, grp)
        return normed_rows(red, offs[grp], SIZES[grp])

    def turn_tiles(ref, rows):
        for k in range(dim // TILE):
            ref[rows, k * TILE:(k + 1) * TILE] = ref[rows, k * TILE:(k + 1) * TILE].T

    def turn(first, last):
        with scope("turn"):
            @pl.loop(first, last)
            def _(blk):
                turn_tiles(wgu, pl.ds(pl.multiple_of(blk * TILE, TILE), TILE))

    def turn_head(step):
        for row in range(0, CHUNK, TILE):
            turn_tiles(wh.at[step], pl.ds(row, TILE))

    def turned_dot(vals, ref, row):
        return functools.reduce(jnp.add, [dot_n(vals[:, k * TILE:(k + 1) * TILE], ref[row:row + TILE, k * TILE:(k + 1) * TILE])
                                          for k in range(dim // TILE)])

    def mlp(grp, b_in):
        rows = rows_of(grp)
        if grp == 0:
            for copy in loads[n_gu:]:
                copy.wait()
        if grp == groups - 1:
            for step in range(AHEAD):
                head_copy(0, step).wait()
                head_copy(1, step).wait()
        with scope(f"mlp{grp}"):
            if grp == groups - 1:
                for step in range(AHEAD):
                    turn_head(step)
            for row in range(0, 2 * ff, TILE):
                gate_up[rows, row:row + TILE] = turned_dot(b_in, wgu, row)
            gate, up = gate_up[rows, 0:ff], gate_up[rows, ff:2 * ff]
            act = (gate * (1.0 / (1.0 + jnp.exp(-gate))) * up).astype(BF16)
            part[1, 0, rows] = dot_n(act, wd[0])
        d_copy(1, grp).start()
        with scope(f"down{grp}"):
            part[1, 1, rows] = dot_n(act, wd[1])

    for copy in loads[n_qkv:n_out]:
        copy.wait()
    with scope("oproj"):
        part[0, 0] = dot_n(os_[...], wo[0])
    with scope("entry"):
        pl.semaphore_wait(barrier, 7)
    for grp in range(groups):
        d_copy(0, grp).start()
    with scope("oproj"):
        part[0, 1] = dot_n(os_[...], wo[1])
    blocks = 2 * ff // TILE
    early = ff // TILE
    for grp in range(groups):
        chip_sum(0, grp)
    loads[n_out].wait()
    turn(0, early)
    loads[n_out + 1].wait()
    turn(early, blocks - SPARE)
    finish(0, 0)
    turn(blocks - SPARE, blocks)
    for grp in range(groups):
        mlp(grp, gathered(0, grp))
        if grp + 1 < groups:
            finish(0, grp + 1)
        if grp == groups - 1:
            finish(1, 0)
        chip_sum(1, grp)

    for stat in (s_own, s_kl, t_acc):
        stat[...] = jnp.zeros_like(stat)
    m_own[...] = jnp.full_like(m_own, NEG)
    m_kl[...] = jnp.full_like(m_kl, NEG)
    lanes = lax.broadcasted_iota(jnp.int32, (1, CHUNK), 1)
    tiles = CHUNK // 128

    def split(vals):
        return [vals[:, 128 * t:128 * (t + 1)] for t in range(tiles)]

    everyone = pl.ds(0, tokens)

    def z_copy(grp, step):
        return pltpu.make_async_remote_copy(
            zsend.at[step, rows_of(grp)], zrecv.at[step, rows_of(grp)], z_send, z_recv.at[(1 + step) if grp else 0],
            device_id=x_peer, device_id_type=MESH)

    def scaled(z, keep, step):
        _, repeated = chunk_start((1 - send_half) if keep else send_half, step)
        return jnp.where(lanes >= repeated, z * (1.0 / TEMPERATURE), NEG)

    def own_step(step):
        m_old, total, hits = m_own[...], s_own[...], t_acc[...]
        parts = []
        for keep, src in ((0, zsend), (1, zkeep)):
            start, repeated = chunk_start((1 - send_half) if keep else send_half, step)
            z = src[step]
            ids = (lanes + (shard * vocab + start)).astype(F32)
            for hit in split(jnp.where((ids == tgt_col) & (lanes >= repeated), z, 0.0)):
                hits = hits + hit
            parts += split(z)
        m_new = functools.reduce(jnp.maximum, parts, m_old)
        total = total * jnp.exp(m_old - m_new)
        for piece in parts:
            total = total + jnp.exp(piece - m_new)
        m_own[...] = m_new
        s_own[...] = total
        t_acc[...] = hits

    def kl_step(step):
        with scope(f"wait_z{step}"):
            z_copy(groups - 1, step).wait_recv()
        mine, theirs = zkeep[step], zrecv[step]
        policy = half == 0
        tops = split(jnp.where(policy, mine, theirs))
        diffs = split(jnp.where(policy, mine - theirs, theirs - mine))
        m_old = m_kl[...]
        m_new = functools.reduce(jnp.maximum, tops, m_old)
        total = s_kl[...] * jnp.exp(m_old - m_new)
        for top, diff in zip(tops, diffs):
            total = total + jnp.exp(top - m_new) * diff
        m_kl[...] = m_new
        s_kl[...] = total

    for grp in range(groups):
        h_in = gathered(1, grp)
        for step in range(steps):
            if grp == 0 and step + AHEAD < steps:
                with scope("wait_w"):
                    head_copy(0, step + AHEAD).wait()
                    head_copy(1, step + AHEAD).wait()
            with scope(f"send{grp}"):
                z = jnp.concatenate([turned_dot(h_in, wh.at[step], row) for row in range(0, CHUNK, TILE)], axis=1)
                zsend[step, rows_of(grp)] = scaled(z, 0, step)
                if grp == 0 and step + AHEAD < steps:
                    turn_head(step + AHEAD)
            z_copy(grp, step).start()
        if grp + 1 < groups:
            finish(1, grp + 1)
    h_in = normed_rows(1, 0, tokens)
    for step in range(steps):
        with scope("keep"):
            zkeep[step] = scaled(dot_t(h_in, wh[step, CHUNK:2 * CHUNK]), 1, step)
            if step > 0:
                own_step(step - 1)
    own_step(steps - 1)


    def to_row(col):
        return jnp.sum(jnp.where(eye, col, 0.0), axis=0, keepdims=True)

    def stat_rows(m_ref, s_ref):
        m_all = m_ref[...]
        m_col = jnp.max(m_all, axis=1, keepdims=True)
        s_col = jnp.sum(s_ref[...] * jnp.exp(m_all - m_col), axis=1, keepdims=True)
        return to_row(m_col), to_row(s_col)

    packs = (pack, pack_kl)

    def p_copy(which, hop):
        other = (here + hop) % 8
        return pltpu.make_async_remote_copy(
            packs[which].at[here], packs[which].at[here], p_send.at[which], p_recv.at[which],
            device_id={"tp": other % 2, "role": other // 2}, device_id_type=MESH)

    def p_all(which):
        seven = packs[which].at[pl.ds(0, 7)]
        return pltpu.make_async_remote_copy(
            seven, seven, p_send.at[which], p_recv.at[which], device_id=x_peer, device_id_type=MESH)

    pack[here, 0:1, 0:tokens], pack[here, 1:2, 0:tokens] = stat_rows(m_own, s_own)
    pack[here, 2:3, 0:tokens] = to_row(jnp.sum(t_acc[...], axis=1, keepdims=True))
    for hop in range(1, 8):
        p_copy(0, hop).start()
    for send in (d_send, y_send, b_send):
        pltpu.make_async_remote_copy(rbuf, rbuf, send, d_recv.at[0, 0], device_id=d_peer, device_id_type=MESH).wait_send()
    early = zrecv.at[pl.ds(0, steps), rows_of(0)]
    pltpu.make_async_remote_copy(early, early, z_send, z_recv.at[0], device_id=x_peer, device_id_type=MESH).wait_recv()
    for step in range(steps):
        kl_step(step)
    pack_kl[here, 0:1, 0:tokens], pack_kl[here, 1:2, 0:tokens] = stat_rows(m_kl, s_kl)
    for hop in range(1, 8):
        p_copy(1, hop).start()
    pltpu.make_async_remote_copy(zsend, zsend, z_send, z_recv.at[0], device_id=x_peer, device_id_type=MESH).wait_send()
    p_all(0).wait_send()
    with scope("wait_p0"):
        p_all(0).wait_recv()
    with scope("wait_p"):
        p_all(1).wait_recv()

    with scope("final"):
        def lse(devices):
            tops = [pack[dev, 0:1, 0:tokens] for dev in devices]
            top = functools.reduce(jnp.maximum, tops)
            total = functools.reduce(jnp.add, [pack[dev, 1:2, 0:tokens] * jnp.exp(t - top) for dev, t in zip(devices, tops)])
            return top + jnp.log(total)

        lse_pol = lse(range(4))
        lse_ref = lse(range(4, 8))
        cross = functools.reduce(jnp.add, [pack_kl[dev, 1:2, 0:tokens] * jnp.exp(pack_kl[dev, 0:1, 0:tokens] - lse_pol) for dev in range(8)])
        tgt_z = functools.reduce(jnp.add, [pack[dev, 2:3, 0:tokens] for dev in range(4)])
        mask_vals = mask_ref[...].astype(F32)
        out_ref[0:1, :] = (cross - lse_pol + lse_ref) * mask_vals
        out_ref[1:2, :] = (tgt_z - lse_pol) * mask_vals
    p_all(1).wait_send()


def solution(mesh):
    by_shard = P(("role", "tp"), None)
    by_role = P("role", None)

    def per_device(hidden, segment_ids, loss_mask, target, norm_gains, w_query, b_query, w_key, b_key, w_value, b_value, w_out, w_gate, w_up, w_down, w_head):
        tokens, dim = hidden.shape[1:]
        q_heads, head_dim = b_query.shape
        ff = w_gate.shape[0]
        vocab = w_head.shape[0]
        groups = len(SIZES)
        cols = dim // 2
        q_rows = q_heads * head_dim
        halves = ((vocab // CHUNK + 2) // 2) * CHUNK
        steps = halves // CHUNK
        wide = 2 * head_dim
        sem = pltpu.SemaphoreType.DMA
        out = pl.pallas_call(
            functools.partial(kernel, (tokens, dim, head_dim, q_heads, vocab)),
            out_shape=pltpu.VMEM((2, tokens), F32),
            in_specs=[pl.BlockSpec(memory_space=pl.ANY)] * 16,
            out_specs=pl.BlockSpec(memory_space=pltpu.VMEM),
            scratch_shapes=[
                pltpu.VMEM((tokens, dim), BF16),
                pltpu.VMEM((3, 2, dim), F32),
                pltpu.VMEM((1, tokens), jnp.int32),
                pltpu.VMEM((1, tokens), jnp.int32),
                pltpu.VMEM((1, tokens), jnp.int32),
                pltpu.VMEM(b_query.shape, BF16),
                pltpu.VMEM(b_key.shape, BF16),
                pltpu.VMEM(b_value.shape, BF16),
                pltpu.VMEM((q_rows + 2 * wide, dim), BF16),
                pltpu.VMEM((2, q_rows, cols), BF16),
                pltpu.VMEM((2 * ff, dim), BF16),
                pltpu.VMEM((2, ff, cols), BF16),
                pltpu.VMEM((steps, 2 * CHUNK, dim), BF16),
                pltpu.VMEM((2, tokens, cols), F32),
                pltpu.VMEM((q_heads * tokens, wide), BF16),
                pltpu.VMEM((tokens, q_rows), BF16),
                pltpu.VMEM((2, 2, tokens, cols), F32),
                pltpu.VMEM((2, tokens, cols), F32),
                pltpu.VMEM((2, tokens, cols), F32),
                pltpu.VMEM((2, 2, tokens, cols), F32),
                pltpu.VMEM((tokens, 2 * ff), F32),
                pltpu.VMEM((steps, tokens, CHUNK), F32),
                pltpu.VMEM((steps, tokens, CHUNK), F32),
                pltpu.VMEM((steps, tokens, CHUNK), F32),
                pltpu.VMEM((tokens, 128), F32),
                pltpu.VMEM((tokens, 128), F32),
                pltpu.VMEM((tokens, 128), F32),
                pltpu.VMEM((tokens, 128), F32),
                pltpu.VMEM((tokens, 128), F32),
                pltpu.VMEM((16, 128), F32),
                pltpu.VMEM((8, 4, 128), F32),
                pltpu.VMEM((8, 2, 128), F32),
                sem((7,)), sem((steps,)),
                sem(()), sem((2, groups)), sem(()), sem((2, groups)), sem(()), sem((2, groups)),
                sem(()), sem((1 + steps,)), sem((2,)), sem((2,)),
            ],
            compiler_params=pltpu.CompilerParams(
                collective_id=0, has_side_effects=True, vmem_limit_bytes=64500000),
            name="layer_head_kl",
        )(hidden, jnp.transpose(norm_gains, (1, 0, 2)), w_query, w_key, w_value, w_out, w_gate, w_up, w_down, w_head,
          segment_ids.reshape(1, tokens), loss_mask.reshape(1, tokens), target.reshape(1, tokens), b_query, b_key, b_value)
        return out[0], out[1]

    in_specs = (P(None, "dp", None), P("dp"), P("dp"), P("dp"), P(None, None, None), by_shard, by_shard, by_role, by_role, by_role, by_role, by_shard, by_shard, by_shard, by_shard, by_shard)
    return jax.shard_map(per_device, mesh=mesh, in_specs=in_specs, out_specs=(P("dp"), P("dp")), check_vma=False)
```

```python
import contextlib
import functools
import math

import jax
import jax.numpy as jnp
from jax import lax
from jax.experimental import pallas as pl
from jax.experimental.pallas import tpu as pltpu
from jax.sharding import PartitionSpec as P

EPS = 1e-6
ROPE_BASE = 1000000.0
TEMPERATURE = 0.7
NEG = -1e30
SIZES = (24, 40)
AHEAD = 4
DIRECT = 256
SPARE = 2
TILE = 256
CHUNK = 512
F32 = jnp.float32
BF16 = jnp.bfloat16
MESH = pl.DeviceIdType.MESH


def scope(name):
    return contextlib.nullcontext()


def dot_t(rows, weight):
    return lax.dot_general(rows, weight, (((1,), (1,)), ((), ())), preferred_element_type=F32)


def dot_n(rows, weight):
    return lax.dot_general(rows, weight, (((1,), (0,)), ((), ())), preferred_element_type=F32)


def normed(vals, gain):
    inv_rms = lax.rsqrt(jnp.mean(vals * vals, axis=-1, keepdims=True) + EPS)
    return (vals * inv_rms * gain).astype(BF16)


def kernel(cfg, hidden, gains, w_query, w_key, w_value, w_out, w_gate, w_up, w_down, w_head,
           seg_in, mask_in, tgt_in, bq_in, bk_in, bv_in, out_ref,
           xb, gn, seg_ref, mask_ref, tgt_ref, bq_ref, bk_ref, bv_ref, wqkv, wo, wgu, wd, wh, xcol, qs, os_, part, rbuf, ybuf, dbuf, full,
           gate_up, zsend, zkeep, zrecv, m_own, s_own, m_kl, s_kl, t_acc, dup, pack, pack_kl,
           in_sem, head_sem, d_send, d_recv, y_send, y_recv, c_send, c_recv, b_send, b_recv, z_send, z_recv, p_send, p_recv):
    tokens, dim, head_dim, q_heads, vocab = cfg
    offs = [sum(SIZES[:grp]) for grp in range(len(SIZES))]
    groups = len(SIZES)
    cols = dim // 2
    ff = w_gate.shape[0]
    halves = ((vocab // CHUNK + 2) // 2) * CHUNK
    steps = halves // CHUNK
    tp = lax.axis_index("tp")
    role = lax.axis_index("role")
    core = role % 2
    half = role // 2
    here = role * 2 + tp
    shard = core * 2 + tp
    d_peer = {"role": half * 2 + 1 - core}
    y_peer = {"tp": 1 - tp}
    c_peer = {"tp": 1 - tp, "role": half * 2 + 1 - core}
    x_peer = {"role": (1 - half) * 2 + core}
    send_half = 1 - half
    q_rows = q_heads * head_dim
    wide = 2 * head_dim

    kv_rows = pl.ds(pl.multiple_of(tp * head_dim, head_dim), head_dim)
    theirs_cols = pl.ds(pl.multiple_of((1 - core) * cols, cols), cols)
    mine_cols = pl.ds(pl.multiple_of(core * cols, cols), cols)
    moves = [(hidden.at[half], xb), (gains, gn), (seg_in, seg_ref), (mask_in, mask_ref), (tgt_in, tgt_ref),
             (bq_in, bq_ref), (bk_in, bk_ref), (bv_in, bv_ref)]
    n_small = len(moves)
    for slot in range(2):
        moves.append((w_key.at[kv_rows], wqkv.at[pl.ds(slot * head_dim, head_dim)]))
        moves.append((w_value.at[kv_rows], wqkv.at[pl.ds((2 + slot) * head_dim, head_dim)]))
    for piece in range(2):
        moves.append((w_query.at[pl.ds(piece * q_rows // 2, q_rows // 2)],
                      wqkv.at[pl.ds(2 * wide + piece * q_rows // 2, q_rows // 2)]))
    n_qkv = len(moves)
    moves += [(w_out.at[:, theirs_cols], wo.at[0]), (w_out.at[:, mine_cols], wo.at[1])]
    n_out = len(moves)
    moves += [(w_gate, wgu.at[pl.ds(0, ff)]), (w_up, wgu.at[pl.ds(ff, ff)])]
    n_gu = len(moves)
    moves += [(w_down.at[:, theirs_cols], wd.at[0]), (w_down.at[:, mine_cols], wd.at[1])]
    bounds = [n_small, n_small + 5, n_qkv, n_out, n_out + 1, n_gu]
    loads = [pltpu.make_async_copy(src, dst, in_sem.at[sum(idx >= bound for bound in bounds)])
             for idx, (src, dst) in enumerate(moves)]
    for copy in loads[:n_qkv]:
        copy.start()

    barrier = pltpu.get_barrier_semaphore()
    for hop in range(1, 8):
        other = (here + hop) % 8
        pl.semaphore_signal(barrier, inc=1, device_id={"tp": other % 2, "role": other // 2}, device_id_type=MESH)

    def chunk_start(part_half, step):
        nominal = part_half * halves + step * CHUNK
        start = jnp.minimum(nominal, vocab - CHUNK)
        return start, nominal - start

    def head_copy(keep, step):
        start, _ = chunk_start((1 - send_half) if keep else send_half, step)
        return pltpu.make_async_copy(w_head.at[pl.ds(pl.multiple_of(start, 64), CHUNK)],
                                     wh.at[step, pl.ds(keep * CHUNK, CHUNK)], head_sem.at[step])

    ti = lax.broadcasted_iota(jnp.int32, (tokens, tokens), 0)
    tj = lax.broadcasted_iota(jnp.int32, (tokens, tokens), 1)
    eye = ti == tj
    lane = lax.broadcasted_iota(jnp.int32, (1, wide), 1)
    half_dim = head_dim // 2
    freq = jnp.exp((lane % half_dim).astype(F32) * (-2.0 * math.log(ROPE_BASE) / head_dim))
    low = (lane % head_dim) < half_dim
    even = lane < head_dim

    def gain_row(which):
        return jnp.where(half == 0, gn[which, 0:1, :], gn[which, 1:2, :])

    with scope("wait_x"):
        for copy in loads[:n_small]:
            copy.wait()
    with scope("norm_x"):
        seg_row = seg_ref[...].astype(F32)
        seg_col = jnp.sum(jnp.where(eye, seg_row, 0.0), axis=1, keepdims=True)
        same = seg_col == seg_row
        allowed = same & (ti >= tj)
        seg_first = jnp.min(jnp.where(same, tj.astype(F32), 1e9), axis=1, keepdims=True)
        pos = lax.broadcasted_iota(jnp.int32, (tokens, 1), 0).astype(F32) - seg_first
        angles = pos * freq
        cos_t = jnp.cos(angles)
        sin_t = jnp.sin(angles)
        sin_t = jnp.where(low, -sin_t, sin_t)
        tgt_col = jnp.sum(jnp.where(eye, tgt_ref[...].astype(F32), 0.0), axis=1, keepdims=True)
        dup[...] = jnp.zeros_like(dup)
        dup[0:q_heads, 0:head_dim] = bq_ref[...].astype(F32)
        dup[q_heads:q_heads + 2, 0:head_dim] = bk_ref[...].astype(F32)
        dup[q_heads + 2:q_heads + 4, 0:head_dim] = bv_ref[...].astype(F32)
        bias = dup[...]
        bias = bias + pltpu.roll(bias, head_dim, 1)
        bias_k = jnp.where(tp == 0, bias[q_heads:q_heads + 1], bias[q_heads + 1:q_heads + 2])
        bias_v = jnp.where(tp == 0, bias[q_heads + 2:q_heads + 3], bias[q_heads + 3:q_heads + 4])
        xf = xb[...].astype(F32)
        xcol[0] = xf[:, :cols]
        xcol[1] = xf[:, cols:]
        a_in = normed(xf, gain_row(0))

    def rotate(vals):
        turned = jnp.where(low, pltpu.roll(vals, wide - half_dim, 1), pltpu.roll(vals, half_dim, 1))
        return vals * cos_t + turned * sin_t

    with scope("wait_kv"):
        for copy in loads[n_small:n_small + 5]:
            copy.wait()
    for copy in loads[n_qkv:]:
        copy.start()

    @pl.loop(0, steps)
    def _(step):
        head_copy(0, step).start()
        head_copy(1, step).start()

    def put_q(first_pair, vals):
        for idx in range(q_heads // 4):
            pair = first_pair + idx
            bias_q = jnp.where(even, bias[2 * pair:2 * pair + 1], bias[2 * pair + 1:2 * pair + 2])
            q_rot = rotate(vals[:, idx * wide:(idx + 1) * wide] + bias_q) * head_dim ** -0.5
            qs[2 * pair * tokens:(2 * pair + 1) * tokens, :] = jnp.where(even, q_rot, 0.0).astype(BF16)
            qs[(2 * pair + 1) * tokens:(2 * pair + 2) * tokens, :] = jnp.where(even, 0.0, q_rot).astype(BF16)

    cut = 2 * wide + q_rows // 2
    with scope("qkv"):
        kvq = dot_t(a_in, wqkv[0:cut])
        loads[n_small + 5].wait()
        rest = dot_t(a_in, wqkv[cut:cut + q_rows // 2])
        k_rot = rotate(kvq[:, :wide] + bias_k).astype(BF16)
        v_two = (kvq[:, wide:2 * wide] + bias_v).astype(BF16)
        put_q(0, kvq[:, 2 * wide:])
        put_q(q_heads // 4, rest)
    with scope("attn"):
        scores = dot_t(qs[...], k_rot).reshape(q_heads, tokens, tokens)
        scores = jnp.where(allowed[None], scores, NEG)
        expd = jnp.exp(scores - jnp.max(scores, axis=-1, keepdims=True))
        probs = (expd / jnp.sum(expd, axis=-1, keepdims=True)).astype(BF16).reshape(q_heads * tokens, tokens)
        heads_out = dot_n(probs, v_two)
        for pair in range(q_heads // 2):
            lo = heads_out[2 * pair * tokens:(2 * pair + 1) * tokens]
            hi = heads_out[(2 * pair + 1) * tokens:(2 * pair + 2) * tokens]
            os_[:, pair * wide:(pair + 1) * wide] = jnp.where(even, lo, hi).astype(BF16)

    def rows_of(grp):
        return pl.ds(offs[grp], SIZES[grp])

    def d_copy(red, grp):
        return pltpu.make_async_remote_copy(
            part.at[red, 0, rows_of(grp)], rbuf.at[red, rows_of(grp)], d_send, d_recv.at[red, grp],
            device_id=d_peer, device_id_type=MESH)

    def summed(grp):
        return pl.ds(DIRECT, cols - DIRECT) if grp == 0 else pl.ds(0, cols)

    def y_copy(red, grp):
        place = (red, rows_of(grp), summed(grp))
        return pltpu.make_async_remote_copy(
            rbuf.at[place], ybuf.at[place], y_send.at[grp], y_recv.at[red, grp],
            device_id=y_peer, device_id_type=MESH)

    def c_copy(red, mine):
        return pltpu.make_async_remote_copy(
            part.at[red, mine, rows_of(0), pl.ds(0, DIRECT)], dbuf.at[red, 1 - mine], c_send, c_recv.at[red],
            device_id=y_peer if mine else c_peer, device_id_type=MESH)

    def b_copy(red, grp):
        return pltpu.make_async_remote_copy(
            full.at[red, core, rows_of(grp)], full.at[red, core, rows_of(grp)], b_send, b_recv.at[red, grp],
            device_id=d_peer, device_id_type=MESH)

    def chip_sum(red, grp):
        rows = rows_of(grp)
        with scope(f"wait_d{red}{grp}"):
            d_copy(red, grp).wait_recv()
        rbuf[red, rows] = part[red, 1, rows] + rbuf[red, rows]
        y_copy(red, grp).start()

    def finish(red, grp):
        rows = rows_of(grp)
        with scope(f"wait_y{red}{grp}"):
            y_copy(red, grp).wait_recv()
        base = xcol if red == 0 else full.at[0]
        place = (rows, summed(grp))
        full[(red, core) + place] = (base[(core,) + place] + (rbuf[(red,) + place] + ybuf[(red,) + place])).astype(BF16).astype(F32)
        if grp == 0:
            pltpu.make_async_remote_copy(dbuf.at[red], dbuf.at[red], c_send, c_recv.at[red],
                                         device_id=y_peer, device_id_type=MESH).wait_recv()
            place = (rows, pl.ds(0, DIRECT))
            full[(red, core) + place] = (base[(core,) + place] + (rbuf[(red,) + place] + (dbuf[red, 0] + dbuf[red, 1]))).astype(BF16).astype(F32)
        b_copy(red, grp).start()

    def b_wait(red, grp):
        with scope(f"wait_b{red}{grp}"):
            b_copy(red, grp).wait_recv()

    def normed_rows(red, off, size):
        rows = pl.ds(off, size)
        left, right = full[red, 0, rows], full[red, 1, rows]
        total = jnp.sum(left * left, axis=-1, keepdims=True) + jnp.sum(right * right, axis=-1, keepdims=True)
        inv_rms = lax.rsqrt(total * (1.0 / dim) + EPS)
        gain = gain_row(red + 1)
        return jnp.concatenate([(left * inv_rms * gain[:, :cols]).astype(BF16),
                                (right * inv_rms * gain[:, cols:]).astype(BF16)], axis=1)

    def gathered(red, grp):
        b_wait(red, grp)
        return normed_rows(red, offs[grp], SIZES[grp])

    def turn_tiles(ref, rows):
        for k in range(dim // TILE):
            ref[rows, k * TILE:(k + 1) * TILE] = ref[rows, k * TILE:(k + 1) * TILE].T

    def turn(first, last):
        with scope("turn"):
            @pl.loop(first, last)
            def _(blk):
                turn_tiles(wgu, pl.ds(pl.multiple_of(blk * TILE, TILE), TILE))

    def turn_head(step):
        for row in range(0, CHUNK, TILE):
            turn_tiles(wh.at[step], pl.ds(row, TILE))

    def turned_dot(vals, ref, row):
        return functools.reduce(jnp.add, [dot_n(vals[:, k * TILE:(k + 1) * TILE], ref[row:row + TILE, k * TILE:(k + 1) * TILE])
                                          for k in range(dim // TILE)])

    def mlp(grp, b_in):
        rows = rows_of(grp)
        if grp == 0:
            for copy in loads[n_gu:]:
                copy.wait()
        if grp == groups - 1:
            for step in range(AHEAD):
                head_copy(0, step).wait()
                head_copy(1, step).wait()
        with scope(f"mlp{grp}"):
            if grp == groups - 1:
                for step in range(AHEAD):
                    turn_head(step)
            for row in range(0, 2 * ff, TILE):
                gate_up[rows, row:row + TILE] = turned_dot(b_in, wgu, row)
            gate, up = gate_up[rows, 0:ff], gate_up[rows, ff:2 * ff]
            act = (gate * (1.0 / (1.0 + jnp.exp(-gate))) * up).astype(BF16)
            part[1, 0, rows] = dot_n(act, wd[0])
        d_copy(1, grp).start()
        if grp == 0:
            c_copy(1, 0).start()
        if grp + 1 < groups:
            finish(0, grp + 1)
        else:
            finish(1, 0)
        with scope(f"down{grp}"):
            part[1, 1, rows] = dot_n(act, wd[1])
        if grp == 0:
            c_copy(1, 1).start()

    for copy in loads[n_qkv:n_out]:
        copy.wait()
    with scope("oproj"):
        part[0, 0] = dot_n(os_[...], wo[0])
    with scope("entry"):
        pl.semaphore_wait(barrier, 7)
    d_copy(0, 0).start()
    c_copy(0, 0).start()
    for grp in range(1, groups):
        d_copy(0, grp).start()
    with scope("oproj"):
        part[0, 1] = dot_n(os_[...], wo[1])
    c_copy(0, 1).start()
    blocks = 2 * ff // TILE
    early = ff // TILE
    for grp in range(groups):
        chip_sum(0, grp)
    loads[n_out].wait()
    turn(0, early)
    loads[n_out + 1].wait()
    turn(early, blocks - SPARE)
    finish(0, 0)
    turn(blocks - SPARE, blocks)
    for grp in range(groups):
        mlp(grp, gathered(0, grp))
        chip_sum(1, grp)

    for stat in (s_own, s_kl, t_acc):
        stat[...] = jnp.zeros_like(stat)
    m_own[...] = jnp.full_like(m_own, NEG)
    m_kl[...] = jnp.full_like(m_kl, NEG)
    lanes = lax.broadcasted_iota(jnp.int32, (1, CHUNK), 1)
    tiles = CHUNK // 128

    def split(vals):
        return [vals[:, 128 * t:128 * (t + 1)] for t in range(tiles)]

    everyone = pl.ds(0, tokens)

    def z_copy(grp, step, lanes_of=pl.ds(0, CHUNK)):
        place = (step, rows_of(grp), lanes_of)
        return pltpu.make_async_remote_copy(
            zsend.at[place], zrecv.at[place], z_send, z_recv.at[(1 + step) if grp else 0],
            device_id=x_peer, device_id_type=MESH)

    def scaled(z, keep, step):
        _, repeated = chunk_start((1 - send_half) if keep else send_half, step)
        return jnp.where(lanes >= repeated, z * (1.0 / TEMPERATURE), NEG)

    def own_step(step):
        m_old, total, hits = m_own[...], s_own[...], t_acc[...]
        parts = []
        for keep, src in ((0, zsend), (1, zkeep)):
            start, repeated = chunk_start((1 - send_half) if keep else send_half, step)
            z = src[step]
            ids = (lanes + (shard * vocab + start)).astype(F32)
            for hit in split(jnp.where((ids == tgt_col) & (lanes >= repeated), z, 0.0)):
                hits = hits + hit
            parts += split(z)
        m_new = functools.reduce(jnp.maximum, parts, m_old)
        total = total * jnp.exp(m_old - m_new)
        for piece in parts:
            total = total + jnp.exp(piece - m_new)
        m_own[...] = m_new
        s_own[...] = total
        t_acc[...] = hits

    def kl_step(step):
        with scope(f"wait_z{step}"):
            z_copy(groups - 1, step).wait_recv()
        mine, theirs = zkeep[step], zrecv[step]
        policy = half == 0
        tops = split(jnp.where(policy, mine, theirs))
        diffs = split(jnp.where(policy, mine - theirs, theirs - mine))
        m_old = m_kl[...]
        m_new = functools.reduce(jnp.maximum, tops, m_old)
        total = s_kl[...] * jnp.exp(m_old - m_new)
        for top, diff in zip(tops, diffs):
            total = total + jnp.exp(top - m_new) * diff
        m_kl[...] = m_new
        s_kl[...] = total

    for grp in range(groups):
        h_in = gathered(1, grp)
        for step in range(steps):
            late = step + AHEAD - 1 if grp == 0 and 0 < step <= steps - AHEAD else None
            if late is not None:
                with scope("wait_w"):
                    head_copy(0, late).wait()
                    head_copy(1, late).wait()
            rows = range(0, CHUNK, TILE)
            if grp == 0 and step == 0:
                for row in rows:
                    place = pl.ds(row, TILE)
                    with scope("first"):
                        zsend[step, rows_of(grp), place] = turned_dot(h_in, wh.at[step], row) * (1.0 / TEMPERATURE)
                    z_copy(grp, step, place).start()
                continue
            with scope(f"send{grp}"):
                z = jnp.concatenate([turned_dot(h_in, wh.at[step], row) for row in rows], axis=1)
                zsend[step, rows_of(grp)] = scaled(z, 0, step)
                if late is not None:
                    turn_head(late)
            z_copy(grp, step).start()
        if grp + 1 < groups:
            finish(1, grp + 1)
    h_in = normed_rows(1, 0, tokens)
    for step in range(steps):
        with scope("keep"):
            zkeep[step] = scaled(dot_t(h_in, wh[step, CHUNK:2 * CHUNK]), 1, step)
            if step > 0:
                own_step(step - 1)
    own_step(steps - 1)


    def to_row(col):
        return jnp.sum(jnp.where(eye, col, 0.0), axis=0, keepdims=True)

    def stat_rows(m_ref, s_ref):
        m_all = m_ref[...]
        m_col = jnp.max(m_all, axis=1, keepdims=True)
        s_col = jnp.sum(s_ref[...] * jnp.exp(m_all - m_col), axis=1, keepdims=True)
        return to_row(m_col), to_row(s_col)

    packs = (pack, pack_kl)

    def p_copy(which, hop):
        other = (here + hop) % 8
        return pltpu.make_async_remote_copy(
            packs[which].at[here], packs[which].at[here], p_send.at[which], p_recv.at[which],
            device_id={"tp": other % 2, "role": other // 2}, device_id_type=MESH)

    def p_all(which):
        seven = packs[which].at[pl.ds(0, 7)]
        return pltpu.make_async_remote_copy(
            seven, seven, p_send.at[which], p_recv.at[which], device_id=x_peer, device_id_type=MESH)

    pack[here, 0:1, 0:tokens], pack[here, 1:2, 0:tokens] = stat_rows(m_own, s_own)
    pack[here, 2:3, 0:tokens] = to_row(jnp.sum(t_acc[...], axis=1, keepdims=True))
    for hop in range(1, 8):
        p_copy(0, hop).start()
    sent = [(rbuf, d_send), (rbuf, b_send), (dbuf, c_send)]
    sent += [(rbuf.at[pl.ds(0, 2), rows_of(grp), summed(grp)], y_send.at[grp]) for grp in range(groups)]
    for ref, send in sent:
        pltpu.make_async_remote_copy(ref, ref, send, c_recv.at[0], device_id=d_peer, device_id_type=MESH).wait_send()
    early = zrecv.at[pl.ds(0, steps), rows_of(0)]
    pltpu.make_async_remote_copy(early, early, z_send, z_recv.at[0], device_id=x_peer, device_id_type=MESH).wait_recv()
    for step in range(steps):
        kl_step(step)
    pack_kl[here, 0:1, 0:tokens], pack_kl[here, 1:2, 0:tokens] = stat_rows(m_kl, s_kl)
    for hop in range(1, 8):
        p_copy(1, hop).start()
    pltpu.make_async_remote_copy(zsend, zsend, z_send, z_recv.at[0], device_id=x_peer, device_id_type=MESH).wait_send()
    p_all(0).wait_send()
    with scope("wait_p0"):
        p_all(0).wait_recv()
    with scope("wait_p"):
        p_all(1).wait_recv()

    with scope("final"):
        def lse(devices):
            tops = [pack[dev, 0:1, 0:tokens] for dev in devices]
            top = functools.reduce(jnp.maximum, tops)
            total = functools.reduce(jnp.add, [pack[dev, 1:2, 0:tokens] * jnp.exp(t - top) for dev, t in zip(devices, tops)])
            return top + jnp.log(total)

        lse_pol = lse(range(4))
        lse_ref = lse(range(4, 8))
        cross = functools.reduce(jnp.add, [pack_kl[dev, 1:2, 0:tokens] * jnp.exp(pack_kl[dev, 0:1, 0:tokens] - lse_pol) for dev in range(8)])
        tgt_z = functools.reduce(jnp.add, [pack[dev, 2:3, 0:tokens] for dev in range(4)])
        mask_vals = mask_ref[...].astype(F32)
        out_ref[0:1, :] = (cross - lse_pol + lse_ref) * mask_vals
        out_ref[1:2, :] = (tgt_z - lse_pol) * mask_vals
    p_all(1).wait_send()


def solution(mesh):
    by_shard = P(("role", "tp"), None)
    by_role = P("role", None)

    def per_device(hidden, segment_ids, loss_mask, target, norm_gains, w_query, b_query, w_key, b_key, w_value, b_value, w_out, w_gate, w_up, w_down, w_head):
        tokens, dim = hidden.shape[1:]
        q_heads, head_dim = b_query.shape
        ff = w_gate.shape[0]
        vocab = w_head.shape[0]
        groups = len(SIZES)
        cols = dim // 2
        q_rows = q_heads * head_dim
        halves = ((vocab // CHUNK + 2) // 2) * CHUNK
        steps = halves // CHUNK
        wide = 2 * head_dim
        sem = pltpu.SemaphoreType.DMA
        out = pl.pallas_call(
            functools.partial(kernel, (tokens, dim, head_dim, q_heads, vocab)),
            out_shape=pltpu.VMEM((2, tokens), F32),
            in_specs=[pl.BlockSpec(memory_space=pl.ANY)] * 16,
            out_specs=pl.BlockSpec(memory_space=pltpu.VMEM),
            scratch_shapes=[
                pltpu.VMEM((tokens, dim), BF16),
                pltpu.VMEM((3, 2, dim), F32),
                pltpu.VMEM((1, tokens), jnp.int32),
                pltpu.VMEM((1, tokens), jnp.int32),
                pltpu.VMEM((1, tokens), jnp.int32),
                pltpu.VMEM(b_query.shape, BF16),
                pltpu.VMEM(b_key.shape, BF16),
                pltpu.VMEM(b_value.shape, BF16),
                pltpu.VMEM((q_rows + 2 * wide, dim), BF16),
                pltpu.VMEM((2, q_rows, cols), BF16),
                pltpu.VMEM((2 * ff, dim), BF16),
                pltpu.VMEM((2, ff, cols), BF16),
                pltpu.VMEM((steps, 2 * CHUNK, dim), BF16),
                pltpu.VMEM((2, tokens, cols), F32),
                pltpu.VMEM((q_heads * tokens, wide), BF16),
                pltpu.VMEM((tokens, q_rows), BF16),
                pltpu.VMEM((2, 2, tokens, cols), F32),
                pltpu.VMEM((2, tokens, cols), F32),
                pltpu.VMEM((2, tokens, cols), F32),
                pltpu.VMEM((2, 2, SIZES[0], DIRECT), F32),
                pltpu.VMEM((2, 2, tokens, cols), F32),
                pltpu.VMEM((tokens, 2 * ff), F32),
                pltpu.VMEM((steps, tokens, CHUNK), F32),
                pltpu.VMEM((steps, tokens, CHUNK), F32),
                pltpu.VMEM((steps, tokens, CHUNK), F32),
                pltpu.VMEM((tokens, 128), F32),
                pltpu.VMEM((tokens, 128), F32),
                pltpu.VMEM((tokens, 128), F32),
                pltpu.VMEM((tokens, 128), F32),
                pltpu.VMEM((tokens, 128), F32),
                pltpu.VMEM((16, 128), F32),
                pltpu.VMEM((8, 4, 128), F32),
                pltpu.VMEM((8, 2, 128), F32),
                sem((7,)), sem((steps,)),
                sem(()), sem((2, groups)), sem((groups,)), sem((2, groups)), sem(()), sem((2,)), sem(()), sem((2, groups)),
                sem(()), sem((1 + steps,)), sem((2,)), sem((2,)),
            ],
            compiler_params=pltpu.CompilerParams(
                collective_id=0, has_side_effects=True, vmem_limit_bytes=64500000),
            name="layer_head_kl",
        )(hidden, jnp.transpose(norm_gains, (1, 0, 2)), w_query, w_key, w_value, w_out, w_gate, w_up, w_down, w_head,
          segment_ids.reshape(1, tokens), loss_mask.reshape(1, tokens), target.reshape(1, tokens), b_query, b_key, b_value)
        return out[0], out[1]

    in_specs = (P(None, "dp", None), P("dp"), P("dp"), P("dp"), P(None, None, None), by_shard, by_shard, by_role, by_role, by_role, by_role, by_shard, by_shard, by_shard, by_shard, by_shard)
    return jax.shard_map(per_device, mesh=mesh, in_specs=in_specs, out_specs=(P("dp"), P("dp")), check_vma=False)
```

```python
import contextlib
import functools
import math

import jax
import jax.numpy as jnp
from jax import lax
from jax.experimental import pallas as pl
from jax.experimental.pallas import tpu as pltpu
from jax.sharding import PartitionSpec as P

EPS = 1e-6
ROPE_BASE = 1000000.0
TEMPERATURE = 0.7
NEG = -1e30
SIZES = (24, 40)
AHEAD = 4
DIRECT = 256
SPARE = 2
SOON = 3
TILE = 256
CHUNK = 512
F32 = jnp.float32
BF16 = jnp.bfloat16
MESH = pl.DeviceIdType.MESH


def scope(name):
    return contextlib.nullcontext()


def dot_t(rows, weight):
    return lax.dot_general(rows, weight, (((1,), (1,)), ((), ())), preferred_element_type=F32)


def dot_n(rows, weight):
    return lax.dot_general(rows, weight, (((1,), (0,)), ((), ())), preferred_element_type=F32)


def normed(vals, gain):
    inv_rms = lax.rsqrt(jnp.mean(vals * vals, axis=-1, keepdims=True) + EPS)
    return (vals * inv_rms * gain).astype(BF16)


def kernel(cfg, hidden, gains, w_query, w_key, w_value, w_out, w_gate, w_up, w_down, w_head,
           seg_in, mask_in, tgt_in, bq_in, bk_in, bv_in, out_ref,
           xb, gn, seg_ref, mask_ref, tgt_ref, bq_ref, bk_ref, bv_ref, wqkv, wo, wgu, wd, wh, xcol, qs, part, rbuf, ybuf, dbuf, full,
           gate_up, zsend, zkeep, zrecv, m_own, s_own, m_kl, s_kl, t_acc, dup, pack, pack_kl,
           in_sem, head_sem, d_send, d_recv, y_send, y_recv, c_send, c_recv, b_send, b_recv, z_send, z_recv, p_send, p_recv):
    tokens, dim, head_dim, q_heads, vocab = cfg
    offs = [sum(SIZES[:grp]) for grp in range(len(SIZES))]
    groups = len(SIZES)
    cols = dim // 2
    ff = w_gate.shape[0]
    halves = ((vocab // CHUNK + 2) // 2) * CHUNK
    steps = halves // CHUNK
    tp = lax.axis_index("tp")
    role = lax.axis_index("role")
    core = role % 2
    half = role // 2
    here = role * 2 + tp
    shard = core * 2 + tp
    d_peer = {"role": half * 2 + 1 - core}
    y_peer = {"tp": 1 - tp}
    c_peer = {"tp": 1 - tp, "role": half * 2 + 1 - core}
    x_peer = {"role": (1 - half) * 2 + core}
    send_half = 1 - half
    q_rows = q_heads * head_dim
    wide = 2 * head_dim

    kv_rows = pl.ds(pl.multiple_of(tp * head_dim, head_dim), head_dim)
    theirs_cols = pl.ds(pl.multiple_of((1 - core) * cols, cols), cols)
    mine_cols = pl.ds(pl.multiple_of(core * cols, cols), cols)
    kv_two = 2 * head_dim
    moves = [(hidden.at[half], xb), (gains, gn), (seg_in, seg_ref), (mask_in, mask_ref), (tgt_in, tgt_ref),
             (bq_in, bq_ref), (bk_in, bk_ref), (bv_in, bv_ref)]
    n_small = len(moves)
    moves += [(w_key.at[kv_rows], wqkv.at[pl.ds(0, head_dim)]), (w_value.at[kv_rows], wqkv.at[pl.ds(head_dim, head_dim)])]
    n_first = []
    cuts = (0, TILE, 2 * TILE, kv_two + q_rows)
    for begin, end in zip(cuts, cuts[1:]):
        low_row = max(begin - kv_two, 0)
        moves.append((w_query.at[pl.ds(low_row, end - kv_two - low_row)],
                      wqkv.at[pl.ds(kv_two + low_row, end - kv_two - low_row)]))
        n_first.append(len(moves))
    n_qkv = len(moves)
    moves += [(w_out.at[:, theirs_cols], wo.at[0]), (w_out.at[:, mine_cols], wo.at[1])]
    n_out = len(moves)
    moves += [(w_gate, wgu.at[pl.ds(0, ff)]), (w_up, wgu.at[pl.ds(ff, ff)])]
    n_gu = len(moves)
    moves += [(w_down.at[:, theirs_cols], wd.at[0]), (w_down.at[:, mine_cols], wd.at[1])]
    bounds = [n_small] + n_first + [n_out, n_out + 1, n_gu]
    loads = [pltpu.make_async_copy(src, dst, in_sem.at[sum(idx >= bound for bound in bounds)])
             for idx, (src, dst) in enumerate(moves)]
    for copy in loads[:n_out]:
        copy.start()

    barrier = pltpu.get_barrier_semaphore()
    for hop in range(1, 8):
        other = (here + hop) % 8
        pl.semaphore_signal(barrier, inc=1, device_id={"tp": other % 2, "role": other // 2}, device_id_type=MESH)

    def chunk_start(part_half, step):
        nominal = part_half * halves + step * CHUNK
        start = jnp.minimum(nominal, vocab - CHUNK)
        return start, nominal - start

    def head_copy(keep, step):
        start, _ = chunk_start((1 - send_half) if keep else send_half, step)
        return pltpu.make_async_copy(w_head.at[pl.ds(pl.multiple_of(start, 64), CHUNK)],
                                     wh.at[step, pl.ds(keep * CHUNK, CHUNK)], head_sem.at[step])

    ti = lax.broadcasted_iota(jnp.int32, (tokens, tokens), 0)
    tj = lax.broadcasted_iota(jnp.int32, (tokens, tokens), 1)
    eye = ti == tj
    lane = lax.broadcasted_iota(jnp.int32, (1, wide), 1)
    half_dim = head_dim // 2
    freq = jnp.exp((lane % half_dim).astype(F32) * (-2.0 * math.log(ROPE_BASE) / head_dim))
    low = (lane % head_dim) < half_dim
    even = lane < head_dim

    def gain_row(which):
        return jnp.where(half == 0, gn[which, 0:1, :], gn[which, 1:2, :])

    with scope("wait_x"):
        for copy in loads[:n_small]:
            copy.wait()
    with scope("norm_x"):
        seg_row = seg_ref[...].astype(F32)
        seg_col = jnp.sum(jnp.where(eye, seg_row, 0.0), axis=1, keepdims=True)
        same = seg_col == seg_row
        allowed = same & (ti >= tj)
        seg_first = jnp.min(jnp.where(same, tj.astype(F32), 1e9), axis=1, keepdims=True)
        pos = lax.broadcasted_iota(jnp.int32, (tokens, 1), 0).astype(F32) - seg_first
        angles = pos * freq
        cos_t = jnp.cos(angles)
        sin_t = jnp.sin(angles)
        sin_t = jnp.where(low, -sin_t, sin_t)
        tgt_col = jnp.sum(jnp.where(eye, tgt_ref[...].astype(F32), 0.0), axis=1, keepdims=True)
        dup[...] = jnp.zeros_like(dup)
        dup[0:q_heads, 0:head_dim] = bq_ref[...].astype(F32)
        dup[q_heads:q_heads + 2, 0:head_dim] = bk_ref[...].astype(F32)
        dup[q_heads + 2:q_heads + 4, 0:head_dim] = bv_ref[...].astype(F32)
        bias = dup[...]
        bias = bias + pltpu.roll(bias, head_dim, 1)
        bias_k = jnp.where(tp == 0, bias[q_heads:q_heads + 1], bias[q_heads + 1:q_heads + 2])
        bias_v = jnp.where(tp == 0, bias[q_heads + 2:q_heads + 3], bias[q_heads + 3:q_heads + 4])
        xf = xb[...].astype(F32)
        xcol[0] = xf[:, :cols]
        xcol[1] = xf[:, cols:]
        a_in = normed(xf, gain_row(0))

    def rotate(vals):
        turned = jnp.where(low, pltpu.roll(vals, wide - half_dim, 1), pltpu.roll(vals, half_dim, 1))
        return vals * cos_t + turned * sin_t

    def q_store(pair, vals):
        bias_q = jnp.where(even, bias[2 * pair:2 * pair + 1], bias[2 * pair + 1:2 * pair + 2])
        q_rot = rotate(vals + bias_q) * head_dim ** -0.5
        for odd in range(2):
            head = jnp.where(even, 0.0, q_rot) if odd else jnp.where(even, q_rot, 0.0)
            for grp in range(groups):
                off, size = offs[grp], SIZES[grp]
                start = q_heads * off + (2 * pair + odd) * size
                qs[start:start + size, :] = head[off:off + size].astype(BF16)

    with scope("wait_kv"):
        for copy in loads[n_small:n_first[0]]:
            copy.wait()
    for copy in loads[n_out:]:
        copy.start()

    @pl.loop(0, steps)
    def _(step):
        head_copy(0, step).start()
        head_copy(1, step).start()

    with scope("qkv"):
        dots = [dot_t(a_in, wqkv[cuts[0]:cuts[1]])]
        for copy in loads[n_first[0]:n_first[1]]:
            copy.wait()
        dots.append(dot_t(a_in, wqkv[cuts[1]:cuts[2]]))
        kv = dots[0][:, :wide]
        other = pltpu.roll(kv, head_dim, 1)
        k_rot = rotate(jnp.where(even, kv, other) + bias_k).astype(BF16)
        v_two = (jnp.where(even, other, kv) + bias_v).astype(BF16)
        q_store(0, dots[0][:, wide:2 * wide])
        for copy in loads[n_first[1]:n_first[2]]:
            copy.wait()
        dots.append(dot_t(a_in, wqkv[cuts[2]:cuts[3]]))
        q_store(1, dots[1][:, :wide])
        q_store(2, dots[1][:, wide:])
        q_store(3, dots[2])
    def attend(grp):
        off, size = offs[grp], SIZES[grp]
        keys = off + size
        scores = dot_t(qs[q_heads * off:q_heads * keys], k_rot[:keys]).reshape(q_heads, size, keys)
        scores = jnp.where(allowed[None, off:keys, :keys], scores, NEG)
        expd = jnp.exp(scores - jnp.max(scores, axis=-1, keepdims=True))
        probs = (expd / jnp.sum(expd, axis=-1, keepdims=True)).astype(BF16).reshape(q_heads * size, keys)
        heads_out = dot_n(probs, v_two[:keys])
        outs = []
        for pair in range(q_heads // 2):
            lo = heads_out[2 * pair * size:(2 * pair + 1) * size]
            hi = heads_out[(2 * pair + 1) * size:(2 * pair + 2) * size]
            outs.append(jnp.where(even, lo, hi).astype(BF16))
        return jnp.concatenate(outs, axis=1)

    def rows_of(grp):
        return pl.ds(offs[grp], SIZES[grp])

    def d_copy(red, grp):
        return pltpu.make_async_remote_copy(
            part.at[red, 0, rows_of(grp)], rbuf.at[red, rows_of(grp)], d_send, d_recv.at[red, grp],
            device_id=d_peer, device_id_type=MESH)

    def summed(grp):
        return pl.ds(DIRECT, cols - DIRECT) if grp == 0 else pl.ds(0, cols)

    def y_copy(red, grp):
        place = (red, rows_of(grp), summed(grp))
        return pltpu.make_async_remote_copy(
            rbuf.at[place], ybuf.at[place], y_send.at[grp], y_recv.at[red, grp],
            device_id=y_peer, device_id_type=MESH)

    def c_copy(red, mine):
        return pltpu.make_async_remote_copy(
            part.at[red, mine, rows_of(0), pl.ds(0, DIRECT)], dbuf.at[red, 1 - mine], c_send, c_recv.at[red],
            device_id=y_peer if mine else c_peer, device_id_type=MESH)

    def b_copy(red, grp):
        return pltpu.make_async_remote_copy(
            full.at[red, core, rows_of(grp)], full.at[red, core, rows_of(grp)], b_send, b_recv.at[red, grp],
            device_id=d_peer, device_id_type=MESH)

    def chip_sum(red, grp):
        rows = rows_of(grp)
        with scope(f"wait_d{red}{grp}"):
            d_copy(red, grp).wait_recv()
        rbuf[red, rows] = part[red, 1, rows] + rbuf[red, rows]
        y_copy(red, grp).start()

    def finish(red, grp):
        rows = rows_of(grp)
        with scope(f"wait_y{red}{grp}"):
            y_copy(red, grp).wait_recv()
        base = xcol if red == 0 else full.at[0]
        place = (rows, summed(grp))
        full[(red, core) + place] = (base[(core,) + place] + (rbuf[(red,) + place] + ybuf[(red,) + place])).astype(BF16).astype(F32)
        if grp == 0:
            pltpu.make_async_remote_copy(dbuf.at[red], dbuf.at[red], c_send, c_recv.at[red],
                                         device_id=y_peer, device_id_type=MESH).wait_recv()
            place = (rows, pl.ds(0, DIRECT))
            full[(red, core) + place] = (base[(core,) + place] + (rbuf[(red,) + place] + (dbuf[red, 0] + dbuf[red, 1]))).astype(BF16).astype(F32)
        b_copy(red, grp).start()

    def b_wait(red, grp):
        with scope(f"wait_b{red}{grp}"):
            b_copy(red, grp).wait_recv()

    def normed_rows(red, off, size):
        rows = pl.ds(off, size)
        left, right = full[red, 0, rows], full[red, 1, rows]
        total = jnp.sum(left * left, axis=-1, keepdims=True) + jnp.sum(right * right, axis=-1, keepdims=True)
        inv_rms = lax.rsqrt(total * (1.0 / dim) + EPS)
        gain = gain_row(red + 1)
        return jnp.concatenate([(left * inv_rms * gain[:, :cols]).astype(BF16),
                                (right * inv_rms * gain[:, cols:]).astype(BF16)], axis=1)

    def gathered(red, grp):
        b_wait(red, grp)
        return normed_rows(red, offs[grp], SIZES[grp])

    def turn_tiles(ref, rows):
        for k in range(dim // TILE):
            ref[rows, k * TILE:(k + 1) * TILE] = ref[rows, k * TILE:(k + 1) * TILE].T

    def turn(first, last):
        with scope("turn"):
            @pl.loop(first, last)
            def _(blk):
                turn_tiles(wgu, pl.ds(pl.multiple_of(blk * TILE, TILE), TILE))

    def turn_head(step):
        for row in range(0, CHUNK, TILE):
            turn_tiles(wh.at[step], pl.ds(row, TILE))

    def turned_dot(vals, ref, row):
        return functools.reduce(jnp.add, [dot_n(vals[:, k * TILE:(k + 1) * TILE], ref[row:row + TILE, k * TILE:(k + 1) * TILE])
                                          for k in range(dim // TILE)])

    def mlp(grp, b_in):
        rows = rows_of(grp)
        if grp == 0:
            for copy in loads[n_gu:]:
                copy.wait()
        if grp == groups - 1:
            for step in range(AHEAD):
                head_copy(0, step).wait()
                head_copy(1, step).wait()
        with scope(f"mlp{grp}"):
            if grp == groups - 1:
                for step in range(AHEAD):
                    turn_head(step)
            for row in range(0, 2 * ff, TILE):
                gate_up[rows, row:row + TILE] = turned_dot(b_in, wgu, row)
            gate, up = gate_up[rows, 0:ff], gate_up[rows, ff:2 * ff]
            act = (gate * (1.0 / (1.0 + jnp.exp(-gate))) * up).astype(BF16)
            part[1, 0, rows] = dot_n(act, wd[0])
        d_copy(1, grp).start()
        if grp == 0:
            c_copy(1, 0).start()
        if grp + 1 < groups:
            finish(0, grp + 1)
        else:
            finish(1, 0)
        with scope(f"down{grp}"):
            part[1, 1, rows] = dot_n(act, wd[1])
        if grp == 0:
            c_copy(1, 1).start()

    for grp in range(groups):
        with scope(f"attn{grp}"):
            mixed = attend(grp)
        if grp == 0:
            for copy in loads[n_qkv:n_out]:
                copy.wait()
        if grp == 1:
            chip_sum(0, 0)
        with scope("oproj"):
            part[0, 0, rows_of(grp)] = dot_n(mixed, wo[0])
        if grp == 0:
            with scope("entry"):
                pl.semaphore_wait(barrier, 7)
        d_copy(0, grp).start()
        if grp == 0:
            c_copy(0, 0).start()
        with scope("oproj"):
            part[0, 1, rows_of(grp)] = dot_n(mixed, wo[1])
        if grp == 0:
            c_copy(0, 1).start()
    blocks = 2 * ff // TILE
    early = ff // TILE
    loads[n_out].wait()
    turn(0, SOON)
    chip_sum(0, 1)
    turn(SOON, early)
    loads[n_out + 1].wait()
    turn(early, blocks - SPARE)
    finish(0, 0)
    turn(blocks - SPARE, blocks)
    for grp in range(groups):
        mlp(grp, gathered(0, grp))
        chip_sum(1, grp)

    for stat in (s_own, s_kl, t_acc):
        stat[...] = jnp.zeros_like(stat)
    m_own[...] = jnp.full_like(m_own, NEG)
    m_kl[...] = jnp.full_like(m_kl, NEG)
    lanes = lax.broadcasted_iota(jnp.int32, (1, CHUNK), 1)
    tiles = CHUNK // 128

    def split(vals):
        return [vals[:, 128 * t:128 * (t + 1)] for t in range(tiles)]

    everyone = pl.ds(0, tokens)

    def z_copy(grp, step, lanes_of=pl.ds(0, CHUNK)):
        place = (step, rows_of(grp), lanes_of)
        return pltpu.make_async_remote_copy(
            zsend.at[place], zrecv.at[place], z_send, z_recv.at[(1 + step) if grp else 0],
            device_id=x_peer, device_id_type=MESH)

    def scaled(z, keep, step):
        _, repeated = chunk_start((1 - send_half) if keep else send_half, step)
        return jnp.where(lanes >= repeated, z * (1.0 / TEMPERATURE), NEG)

    def own_step(step):
        m_old, total, hits = m_own[...], s_own[...], t_acc[...]
        parts = []
        for keep, src in ((0, zsend), (1, zkeep)):
            start, repeated = chunk_start((1 - send_half) if keep else send_half, step)
            z = src[step]
            ids = (lanes + (shard * vocab + start)).astype(F32)
            for hit in split(jnp.where((ids == tgt_col) & (lanes >= repeated), z, 0.0)):
                hits = hits + hit
            parts += split(z)
        m_new = functools.reduce(jnp.maximum, parts, m_old)
        total = total * jnp.exp(m_old - m_new)
        for piece in parts:
            total = total + jnp.exp(piece - m_new)
        m_own[...] = m_new
        s_own[...] = total
        t_acc[...] = hits

    def kl_step(step):
        with scope(f"wait_z{step}"):
            z_copy(groups - 1, step).wait_recv()
        mine, theirs = zkeep[step], zrecv[step]
        policy = half == 0
        tops = split(jnp.where(policy, mine, theirs))
        diffs = split(jnp.where(policy, mine - theirs, theirs - mine))
        m_old = m_kl[...]
        m_new = functools.reduce(jnp.maximum, tops, m_old)
        total = s_kl[...] * jnp.exp(m_old - m_new)
        for top, diff in zip(tops, diffs):
            total = total + jnp.exp(top - m_new) * diff
        m_kl[...] = m_new
        s_kl[...] = total

    for grp in range(groups):
        h_in = gathered(1, grp)
        for step in range(steps):
            late = step + AHEAD - 1 if grp == 0 and 0 < step <= steps - AHEAD else None
            if late is not None:
                with scope("wait_w"):
                    head_copy(0, late).wait()
                    head_copy(1, late).wait()
            rows = range(0, CHUNK, TILE)
            if grp == 0 and step == 0:
                for row in rows:
                    place = pl.ds(row, TILE)
                    with scope("first"):
                        zsend[step, rows_of(grp), place] = turned_dot(h_in, wh.at[step], row) * (1.0 / TEMPERATURE)
                    z_copy(grp, step, place).start()
                continue
            with scope(f"send{grp}"):
                z = jnp.concatenate([turned_dot(h_in, wh.at[step], row) for row in rows], axis=1)
                zsend[step, rows_of(grp)] = scaled(z, 0, step)
                if late is not None:
                    turn_head(late)
            z_copy(grp, step).start()
        if grp + 1 < groups:
            finish(1, grp + 1)
    h_in = normed_rows(1, 0, tokens)
    for step in range(steps):
        with scope("keep"):
            zkeep[step] = scaled(dot_t(h_in, wh[step, CHUNK:2 * CHUNK]), 1, step)
            if step > 0:
                own_step(step - 1)
    own_step(steps - 1)


    def to_row(col):
        return jnp.sum(jnp.where(eye, col, 0.0), axis=0, keepdims=True)

    def stat_rows(m_ref, s_ref):
        m_all = m_ref[...]
        m_col = jnp.max(m_all, axis=1, keepdims=True)
        s_col = jnp.sum(s_ref[...] * jnp.exp(m_all - m_col), axis=1, keepdims=True)
        return to_row(m_col), to_row(s_col)

    packs = (pack, pack_kl)

    def p_copy(which, hop):
        other = (here + hop) % 8
        return pltpu.make_async_remote_copy(
            packs[which].at[here], packs[which].at[here], p_send.at[which], p_recv.at[which],
            device_id={"tp": other % 2, "role": other // 2}, device_id_type=MESH)

    def p_all(which):
        seven = packs[which].at[pl.ds(0, 7)]
        return pltpu.make_async_remote_copy(
            seven, seven, p_send.at[which], p_recv.at[which], device_id=x_peer, device_id_type=MESH)

    pack[here, 0:1, 0:tokens], pack[here, 1:2, 0:tokens] = stat_rows(m_own, s_own)
    pack[here, 2:3, 0:tokens] = to_row(jnp.sum(t_acc[...], axis=1, keepdims=True))
    for hop in range(1, 8):
        p_copy(0, hop).start()
    sent = [(rbuf, d_send), (rbuf, b_send), (dbuf, c_send)]
    sent += [(rbuf.at[pl.ds(0, 2), rows_of(grp), summed(grp)], y_send.at[grp]) for grp in range(groups)]
    for ref, send in sent:
        pltpu.make_async_remote_copy(ref, ref, send, c_recv.at[0], device_id=d_peer, device_id_type=MESH).wait_send()
    early = zrecv.at[pl.ds(0, steps), rows_of(0)]
    pltpu.make_async_remote_copy(early, early, z_send, z_recv.at[0], device_id=x_peer, device_id_type=MESH).wait_recv()
    for step in range(steps):
        kl_step(step)
    pack_kl[here, 0:1, 0:tokens], pack_kl[here, 1:2, 0:tokens] = stat_rows(m_kl, s_kl)
    for hop in range(1, 8):
        p_copy(1, hop).start()
    pltpu.make_async_remote_copy(zsend, zsend, z_send, z_recv.at[0], device_id=x_peer, device_id_type=MESH).wait_send()
    p_all(0).wait_send()
    with scope("wait_p0"):
        p_all(0).wait_recv()
    with scope("wait_p"):
        p_all(1).wait_recv()

    with scope("final"):
        def lse(devices):
            tops = [pack[dev, 0:1, 0:tokens] for dev in devices]
            top = functools.reduce(jnp.maximum, tops)
            total = functools.reduce(jnp.add, [pack[dev, 1:2, 0:tokens] * jnp.exp(t - top) for dev, t in zip(devices, tops)])
            return top + jnp.log(total)

        lse_pol = lse(range(4))
        lse_ref = lse(range(4, 8))
        cross = functools.reduce(jnp.add, [pack_kl[dev, 1:2, 0:tokens] * jnp.exp(pack_kl[dev, 0:1, 0:tokens] - lse_pol) for dev in range(8)])
        tgt_z = functools.reduce(jnp.add, [pack[dev, 2:3, 0:tokens] for dev in range(4)])
        mask_vals = mask_ref[...].astype(F32)
        out_ref[0:1, :] = (cross - lse_pol + lse_ref) * mask_vals
        out_ref[1:2, :] = (tgt_z - lse_pol) * mask_vals
    p_all(1).wait_send()


def solution(mesh):
    by_shard = P(("role", "tp"), None)
    by_role = P("role", None)

    def per_device(hidden, segment_ids, loss_mask, target, norm_gains, w_query, b_query, w_key, b_key, w_value, b_value, w_out, w_gate, w_up, w_down, w_head):
        tokens, dim = hidden.shape[1:]
        q_heads, head_dim = b_query.shape
        ff = w_gate.shape[0]
        vocab = w_head.shape[0]
        groups = len(SIZES)
        cols = dim // 2
        q_rows = q_heads * head_dim
        halves = ((vocab // CHUNK + 2) // 2) * CHUNK
        steps = halves // CHUNK
        wide = 2 * head_dim
        sem = pltpu.SemaphoreType.DMA
        out = pl.pallas_call(
            functools.partial(kernel, (tokens, dim, head_dim, q_heads, vocab)),
            out_shape=pltpu.VMEM((2, tokens), F32),
            in_specs=[pl.BlockSpec(memory_space=pl.ANY)] * 16,
            out_specs=pl.BlockSpec(memory_space=pltpu.VMEM),
            scratch_shapes=[
                pltpu.VMEM((tokens, dim), BF16),
                pltpu.VMEM((3, 2, dim), F32),
                pltpu.VMEM((1, tokens), jnp.int32),
                pltpu.VMEM((1, tokens), jnp.int32),
                pltpu.VMEM((1, tokens), jnp.int32),
                pltpu.VMEM(b_query.shape, BF16),
                pltpu.VMEM(b_key.shape, BF16),
                pltpu.VMEM(b_value.shape, BF16),
                pltpu.VMEM((q_rows + wide, dim), BF16),
                pltpu.VMEM((2, q_rows, cols), BF16),
                pltpu.VMEM((2 * ff, dim), BF16),
                pltpu.VMEM((2, ff, cols), BF16),
                pltpu.VMEM((steps, 2 * CHUNK, dim), BF16),
                pltpu.VMEM((2, tokens, cols), F32),
                pltpu.VMEM((q_heads * tokens, wide), BF16),
                pltpu.VMEM((2, 2, tokens, cols), F32),
                pltpu.VMEM((2, tokens, cols), F32),
                pltpu.VMEM((2, tokens, cols), F32),
                pltpu.VMEM((2, 2, SIZES[0], DIRECT), F32),
                pltpu.VMEM((2, 2, tokens, cols), F32),
                pltpu.VMEM((tokens, 2 * ff), F32),
                pltpu.VMEM((steps, tokens, CHUNK), F32),
                pltpu.VMEM((steps, tokens, CHUNK), F32),
                pltpu.VMEM((steps, tokens, CHUNK), F32),
                pltpu.VMEM((tokens, 128), F32),
                pltpu.VMEM((tokens, 128), F32),
                pltpu.VMEM((tokens, 128), F32),
                pltpu.VMEM((tokens, 128), F32),
                pltpu.VMEM((tokens, 128), F32),
                pltpu.VMEM((16, 128), F32),
                pltpu.VMEM((8, 4, 128), F32),
                pltpu.VMEM((8, 2, 128), F32),
                sem((8,)), sem((steps,)),
                sem(()), sem((2, groups)), sem((groups,)), sem((2, groups)), sem(()), sem((2,)), sem(()), sem((2, groups)),
                sem(()), sem((1 + steps,)), sem((2,)), sem((2,)),
            ],
            compiler_params=pltpu.CompilerParams(
                collective_id=0, has_side_effects=True, vmem_limit_bytes=64500000),
            name="layer_head_kl",
        )(hidden, jnp.transpose(norm_gains, (1, 0, 2)), w_query, w_key, w_value, w_out, w_gate, w_up, w_down, w_head,
          segment_ids.reshape(1, tokens), loss_mask.reshape(1, tokens), target.reshape(1, tokens), b_query, b_key, b_value)
        return out[0], out[1]

    in_specs = (P(None, "dp", None), P("dp"), P("dp"), P("dp"), P(None, None, None), by_shard, by_shard, by_role, by_role, by_role, by_role, by_shard, by_shard, by_shard, by_shard, by_shard)
    return jax.shard_map(per_device, mesh=mesh, in_specs=in_specs, out_specs=(P("dp"), P("dp")), check_vma=False)
```

```python
import contextlib
import functools
import math

import jax
import jax.numpy as jnp
from jax import lax
from jax.experimental import pallas as pl
from jax.experimental.pallas import tpu as pltpu
from jax.sharding import PartitionSpec as P

EPS = 1e-6
ROPE_BASE = 1000000.0
TEMPERATURE = 0.7
NEG = -1e30
SIZES = (16, 48)
LATER = ((0, 16), (16, 24), (40, 24))
AHEAD = 4
DIRECT = 384
SPARE = 2
SOON = 2
FINISH = (7, 5)
TILE = 256
CHUNK = 512
F32 = jnp.float32
BF16 = jnp.bfloat16
MESH = pl.DeviceIdType.MESH


def scope(name):
    return contextlib.nullcontext()


def dot_t(rows, weight):
    return lax.dot_general(rows, weight, (((1,), (1,)), ((), ())), preferred_element_type=F32)


def dot_n(rows, weight):
    return lax.dot_general(rows, weight, (((1,), (0,)), ((), ())), preferred_element_type=F32)


def normed(vals, gain):
    inv_rms = lax.rsqrt(jnp.mean(vals * vals, axis=-1, keepdims=True) + EPS)
    return (vals * inv_rms * gain).astype(BF16)


def kernel(cfg, hidden, gains, w_query, w_key, w_value, w_out, w_gate, w_up, w_down, w_head,
           seg_in, mask_in, tgt_in, bq_in, bk_in, bv_in, out_ref,
           xb, gn, seg_ref, mask_ref, tgt_ref, bq_ref, bk_ref, bv_ref, wqkv, wo, wgu, wd, wh, xcol, qs, part, rbuf, ybuf, dbuf, full,
           gate_up, zsend, zkeep, zrecv, m_own, s_own, m_kl, s_kl, t_acc, dup, pack, pack_kl,
           in_sem, head_sem, d_send, d_recv, y_send, y_recv, c_send, c_recv, b_send, b_recv, z_send, z_recv, p_send, p_recv):
    tokens, dim, head_dim, q_heads, vocab = cfg
    offs = [sum(SIZES[:grp]) for grp in range(len(SIZES))]
    groups = len(SIZES)
    cols = dim // 2
    ff = w_gate.shape[0]
    halves = ((vocab // CHUNK + 2) // 2) * CHUNK
    steps = halves // CHUNK
    tp = lax.axis_index("tp")
    role = lax.axis_index("role")
    core = role % 2
    half = role // 2
    here = role * 2 + tp
    shard = core * 2 + tp
    d_peer = {"role": half * 2 + 1 - core}
    y_peer = {"tp": 1 - tp}
    c_peer = {"tp": 1 - tp, "role": half * 2 + 1 - core}
    x_peer = {"role": (1 - half) * 2 + core}
    send_half = 1 - half
    q_rows = q_heads * head_dim
    wide = 2 * head_dim

    kv_rows = pl.ds(pl.multiple_of(tp * head_dim, head_dim), head_dim)
    theirs_cols = pl.ds(pl.multiple_of((1 - core) * cols, cols), cols)
    mine_cols = pl.ds(pl.multiple_of(core * cols, cols), cols)
    kv_two = 2 * head_dim
    moves = [(hidden.at[half], xb), (gains, gn), (seg_in, seg_ref), (mask_in, mask_ref), (tgt_in, tgt_ref),
             (bq_in, bq_ref), (bk_in, bk_ref), (bv_in, bv_ref)]
    n_small = len(moves)
    moves += [(w_key.at[kv_rows], wqkv.at[pl.ds(0, head_dim)]), (w_value.at[kv_rows], wqkv.at[pl.ds(head_dim, head_dim)])]
    n_first = []
    cuts = (0, TILE, 2 * TILE, kv_two + q_rows)
    for begin, end in zip(cuts, cuts[1:]):
        low_row = max(begin - kv_two, 0)
        moves.append((w_query.at[pl.ds(low_row, end - kv_two - low_row)],
                      wqkv.at[pl.ds(kv_two + low_row, end - kv_two - low_row)]))
        n_first.append(len(moves))
    n_qkv = len(moves)
    moves += [(w_out.at[:, theirs_cols], wo.at[0]), (w_out.at[:, mine_cols], wo.at[1])]
    n_out = len(moves)
    moves += [(w_gate, wgu.at[pl.ds(0, ff)]), (w_up, wgu.at[pl.ds(ff, ff)])]
    n_gu = len(moves)
    moves += [(w_down.at[:, theirs_cols], wd.at[0]), (w_down.at[:, mine_cols], wd.at[1])]
    bounds = [n_small] + n_first + [n_out, n_out + 1, n_gu]
    loads = [pltpu.make_async_copy(src, dst, in_sem.at[sum(idx >= bound for bound in bounds)])
             for idx, (src, dst) in enumerate(moves)]
    for copy in loads[:n_out]:
        copy.start()

    barrier = pltpu.get_barrier_semaphore()
    for hop in range(1, 8):
        other = (here + hop) % 8
        pl.semaphore_signal(barrier, inc=1, device_id={"tp": other % 2, "role": other // 2}, device_id_type=MESH)

    def chunk_start(part_half, step):
        nominal = part_half * halves + step * CHUNK
        start = jnp.minimum(nominal, vocab - CHUNK)
        return start, nominal - start

    def head_copy(keep, step):
        start, _ = chunk_start((1 - send_half) if keep else send_half, step)
        return pltpu.make_async_copy(w_head.at[pl.ds(pl.multiple_of(start, 64), CHUNK)],
                                     wh.at[step, pl.ds(keep * CHUNK, CHUNK)], head_sem.at[step])

    ti = lax.broadcasted_iota(jnp.int32, (tokens, tokens), 0)
    tj = lax.broadcasted_iota(jnp.int32, (tokens, tokens), 1)
    eye = ti == tj
    lane = lax.broadcasted_iota(jnp.int32, (1, wide), 1)
    half_dim = head_dim // 2
    freq = jnp.exp((lane % half_dim).astype(F32) * (-2.0 * math.log(ROPE_BASE) / head_dim))
    low = (lane % head_dim) < half_dim
    even = lane < head_dim

    def gain_row(which):
        return jnp.where(half == 0, gn[which, 0:1, :], gn[which, 1:2, :])

    with scope("wait_x"):
        for copy in loads[:n_small]:
            copy.wait()
    with scope("norm_x"):
        seg_row = seg_ref[...].astype(F32)
        seg_col = jnp.sum(jnp.where(eye, seg_row, 0.0), axis=1, keepdims=True)
        same = seg_col == seg_row
        allowed = same & (ti >= tj)
        seg_first = jnp.min(jnp.where(same, tj.astype(F32), 1e9), axis=1, keepdims=True)
        pos = lax.broadcasted_iota(jnp.int32, (tokens, 1), 0).astype(F32) - seg_first
        angles = pos * freq
        cos_t = jnp.cos(angles)
        sin_t = jnp.sin(angles)
        sin_t = jnp.where(low, -sin_t, sin_t)
        tgt_col = jnp.sum(jnp.where(eye, tgt_ref[...].astype(F32), 0.0), axis=1, keepdims=True)
        dup[...] = jnp.zeros_like(dup)
        dup[0:q_heads, 0:head_dim] = bq_ref[...].astype(F32)
        dup[q_heads:q_heads + 2, 0:head_dim] = bk_ref[...].astype(F32)
        dup[q_heads + 2:q_heads + 4, 0:head_dim] = bv_ref[...].astype(F32)
        bias = dup[...]
        bias = bias + pltpu.roll(bias, head_dim, 1)
        bias_k = jnp.where(tp == 0, bias[q_heads:q_heads + 1], bias[q_heads + 1:q_heads + 2])
        bias_v = jnp.where(tp == 0, bias[q_heads + 2:q_heads + 3], bias[q_heads + 3:q_heads + 4])
        xf = xb[...].astype(F32)
        xcol[0] = xf[:, :cols]
        xcol[1] = xf[:, cols:]
        a_in = normed(xf, gain_row(0))

    def rotate(vals):
        turned = jnp.where(low, pltpu.roll(vals, wide - half_dim, 1), pltpu.roll(vals, half_dim, 1))
        return vals * cos_t + turned * sin_t

    def q_store(pair, vals):
        bias_q = jnp.where(even, bias[2 * pair:2 * pair + 1], bias[2 * pair + 1:2 * pair + 2])
        q_rot = rotate(vals + bias_q) * head_dim ** -0.5
        for odd in range(2):
            head = jnp.where(even, 0.0, q_rot) if odd else jnp.where(even, q_rot, 0.0)
            for grp in range(groups):
                off, size = offs[grp], SIZES[grp]
                start = q_heads * off + (2 * pair + odd) * size
                qs[start:start + size, :] = head[off:off + size].astype(BF16)

    with scope("wait_kv"):
        for copy in loads[n_small:n_first[0]]:
            copy.wait()
    for copy in loads[n_out:]:
        copy.start()

    @pl.loop(0, steps)
    def _(step):
        head_copy(0, step).start()
        head_copy(1, step).start()

    with scope("qkv"):
        dots = [dot_t(a_in, wqkv[cuts[0]:cuts[1]])]
        for copy in loads[n_first[0]:n_first[1]]:
            copy.wait()
        dots.append(dot_t(a_in, wqkv[cuts[1]:cuts[2]]))
        kv = dots[0][:, :wide]
        other = pltpu.roll(kv, head_dim, 1)
        k_rot = rotate(jnp.where(even, kv, other) + bias_k).astype(BF16)
        v_two = (jnp.where(even, other, kv) + bias_v).astype(BF16)
        q_store(0, dots[0][:, wide:2 * wide])
        for copy in loads[n_first[1]:n_first[2]]:
            copy.wait()
        dots.append(dot_t(a_in, wqkv[cuts[2]:cuts[3]]))
        q_store(1, dots[1][:, :wide])
        q_store(2, dots[1][:, wide:])
        q_store(3, dots[2])
    def attend(grp):
        off, size = offs[grp], SIZES[grp]
        keys = off + size
        scores = dot_t(qs[q_heads * off:q_heads * keys], k_rot[:keys]).reshape(q_heads, size, keys)
        scores = jnp.where(allowed[None, off:keys, :keys], scores, NEG)
        expd = jnp.exp(scores - jnp.max(scores, axis=-1, keepdims=True))
        probs = (expd / jnp.sum(expd, axis=-1, keepdims=True)).astype(BF16).reshape(q_heads * size, keys)
        heads_out = dot_n(probs, v_two[:keys])
        outs = []
        for pair in range(q_heads // 2):
            lo = heads_out[2 * pair * size:(2 * pair + 1) * size]
            hi = heads_out[(2 * pair + 1) * size:(2 * pair + 2) * size]
            outs.append(jnp.where(even, lo, hi).astype(BF16))
        return jnp.concatenate(outs, axis=1)

    ranges = (tuple(zip(offs, SIZES)), LATER)
    later_of = ((0,), (1, 2))

    def rows_of(grp, red=0):
        return pl.ds(*ranges[red][grp])

    def d_copy(red, grp):
        return pltpu.make_async_remote_copy(
            part.at[red, 0, rows_of(grp, red)], rbuf.at[red, rows_of(grp, red)], d_send, d_recv.at[red, grp],
            device_id=d_peer, device_id_type=MESH)

    def summed(grp):
        return pl.ds(DIRECT, cols - DIRECT) if grp == 0 else pl.ds(0, cols)

    def y_copy(red, grp):
        place = (red, rows_of(grp, red), summed(grp))
        return pltpu.make_async_remote_copy(
            rbuf.at[place], ybuf.at[place], y_send.at[min(grp, 1)], y_recv.at[red, grp],
            device_id=y_peer, device_id_type=MESH)

    def c_copy(red, mine):
        return pltpu.make_async_remote_copy(
            part.at[red, mine, rows_of(0), pl.ds(0, DIRECT)], dbuf.at[red, 1 - mine], c_send, c_recv.at[red],
            device_id=y_peer if mine else c_peer, device_id_type=MESH)

    def b_copy(red, grp):
        return pltpu.make_async_remote_copy(
            full.at[red, core, rows_of(grp, red)], full.at[red, core, rows_of(grp, red)], b_send, b_recv.at[red, grp],
            device_id=d_peer, device_id_type=MESH)

    def chip_sum(red, grp):
        rows = rows_of(grp, red)
        with scope(f"wait_d{red}{grp}"):
            d_copy(red, grp).wait_recv()
        rbuf[red, rows] = part[red, 1, rows] + rbuf[red, rows]
        y_copy(red, grp).start()

    def finish(red, grp):
        rows = rows_of(grp, red)
        with scope(f"wait_y{red}{grp}"):
            y_copy(red, grp).wait_recv()
        base = xcol if red == 0 else full.at[0]
        place = (rows, summed(grp))
        full[(red, core) + place] = (base[(core,) + place] + (rbuf[(red,) + place] + ybuf[(red,) + place])).astype(BF16).astype(F32)
        if grp == 0:
            pltpu.make_async_remote_copy(dbuf.at[red], dbuf.at[red], c_send, c_recv.at[red],
                                         device_id=y_peer, device_id_type=MESH).wait_recv()
            place = (rows, pl.ds(0, DIRECT))
            full[(red, core) + place] = (base[(core,) + place] + (rbuf[(red,) + place] + (dbuf[red, 0] + dbuf[red, 1]))).astype(BF16).astype(F32)
        b_copy(red, grp).start()

    def b_wait(red, grp):
        with scope(f"wait_b{red}{grp}"):
            b_copy(red, grp).wait_recv()

    def normed_rows(red, off, size):
        rows = pl.ds(off, size)
        left, right = full[red, 0, rows], full[red, 1, rows]
        total = jnp.sum(left * left, axis=-1, keepdims=True) + jnp.sum(right * right, axis=-1, keepdims=True)
        inv_rms = lax.rsqrt(total * (1.0 / dim) + EPS)
        gain = gain_row(red + 1)
        return jnp.concatenate([(left * inv_rms * gain[:, :cols]).astype(BF16),
                                (right * inv_rms * gain[:, cols:]).astype(BF16)], axis=1)

    def gathered(red, grp):
        b_wait(red, grp)
        return normed_rows(red, *ranges[red][grp])

    def turn_tiles(ref, rows):
        for k in range(dim // TILE):
            ref[rows, k * TILE:(k + 1) * TILE] = ref[rows, k * TILE:(k + 1) * TILE].T

    def turn(first, end):
        with scope("turn"):
            for blk in range(first, end):
                turn_tiles(wgu, pl.ds(blk * TILE, TILE))

    def turn_head(step):
        for row in range(0, CHUNK, TILE):
            turn_tiles(wh.at[step], pl.ds(row, TILE))

    def turned_dot(vals, ref, row):
        return functools.reduce(jnp.add, [dot_n(vals[:, k * TILE:(k + 1) * TILE], ref[row:row + TILE, k * TILE:(k + 1) * TILE])
                                          for k in range(dim // TILE)])

    def mlp(grp, b_in):
        rows = rows_of(grp)
        if grp == 0:
            for copy in loads[n_gu:]:
                copy.wait()
        if grp == groups - 1:
            for step in range(AHEAD):
                head_copy(0, step).wait()
                head_copy(1, step).wait()
        with scope(f"mlp{grp}"):
            if grp == groups - 1:
                for step in range(AHEAD):
                    turn_head(step)
            for row in range(0, 2 * ff, TILE):
                gate_up[rows, row:row + TILE] = turned_dot(b_in, wgu, row)
            gate, up = gate_up[rows, 0:ff], gate_up[rows, ff:2 * ff]
            act = (gate * (1.0 / (1.0 + jnp.exp(-gate))) * up).astype(BF16)
            part[1, 0, rows] = dot_n(act, wd[0])
        for late in later_of[grp]:
            d_copy(1, late).start()
        if grp == 0:
            c_copy(1, 0).start()
        if grp + 1 < groups:
            finish(0, grp + 1)
        else:
            finish(1, 0)
        with scope(f"down{grp}"):
            part[1, 1, rows] = dot_n(act, wd[1])
        if grp == 0:
            c_copy(1, 1).start()

    for grp in range(groups):
        with scope(f"attn{grp}"):
            mixed = attend(grp)
        if grp == 0:
            for copy in loads[n_qkv:n_out]:
                copy.wait()
        if grp == 1:
            chip_sum(0, 0)
        with scope("oproj"):
            part[0, 0, rows_of(grp)] = dot_n(mixed, wo[0])
        if grp == 0:
            with scope("entry"):
                pl.semaphore_wait(barrier, 7)
        d_copy(0, grp).start()
        if grp == 0:
            c_copy(0, 0).start()
        with scope("oproj"):
            part[0, 1, rows_of(grp)] = dot_n(mixed, wo[1])
        if grp == 0:
            c_copy(0, 1).start()
    blocks = 2 * ff // TILE
    early = ff // TILE
    loads[n_out].wait()
    turn(0, SOON)
    chip_sum(0, 1)
    turn(SOON, early)
    loads[n_out + 1].wait()
    turn(early, blocks - SPARE)
    finish(0, 0)
    turn(blocks - SPARE, blocks)
    for grp in range(groups):
        mlp(grp, gathered(0, grp))
        for late in later_of[grp]:
            chip_sum(1, late)

    for stat in (s_own, s_kl, t_acc):
        stat[...] = jnp.zeros_like(stat)
    m_own[...] = jnp.full_like(m_own, NEG)
    m_kl[...] = jnp.full_like(m_kl, NEG)
    lanes = lax.broadcasted_iota(jnp.int32, (1, CHUNK), 1)
    tiles = CHUNK // 128

    def split(vals):
        return [vals[:, 128 * t:128 * (t + 1)] for t in range(tiles)]

    last = len(LATER) - 1

    def z_copy(grp, step, lanes_of=pl.ds(0, CHUNK)):
        place = (step, rows_of(grp, 1), lanes_of)
        return pltpu.make_async_remote_copy(
            zsend.at[place], zrecv.at[place], z_send, z_recv.at[grp + (step if grp == last else 0)],
            device_id=x_peer, device_id_type=MESH)

    def scaled(z, keep, step):
        _, repeated = chunk_start((1 - send_half) if keep else send_half, step)
        return jnp.where(lanes >= repeated, z * (1.0 / TEMPERATURE), NEG)

    def own_step(step):
        m_old, total, hits = m_own[...], s_own[...], t_acc[...]
        parts = []
        for keep, src in ((0, zsend), (1, zkeep)):
            start, repeated = chunk_start((1 - send_half) if keep else send_half, step)
            z = src[step]
            ids = (lanes + (shard * vocab + start)).astype(F32)
            for hit in split(jnp.where((ids == tgt_col) & (lanes >= repeated), z, 0.0)):
                hits = hits + hit
            parts += split(z)
        m_new = functools.reduce(jnp.maximum, parts, m_old)
        total = total * jnp.exp(m_old - m_new)
        for piece in parts:
            total = total + jnp.exp(piece - m_new)
        m_own[...] = m_new
        s_own[...] = total
        t_acc[...] = hits

    def kl_step(step):
        with scope(f"wait_z{step}"):
            z_copy(last, step).wait_recv()
        mine, theirs = zkeep[step], zrecv[step]
        policy = half == 0
        tops = split(jnp.where(policy, mine, theirs))
        diffs = split(jnp.where(policy, mine - theirs, theirs - mine))
        m_old = m_kl[...]
        m_new = functools.reduce(jnp.maximum, tops, m_old)
        total = s_kl[...] * jnp.exp(m_old - m_new)
        for top, diff in zip(tops, diffs):
            total = total + jnp.exp(top - m_new) * diff
        m_kl[...] = m_new
        s_kl[...] = total

    for grp in range(last + 1):
        h_in = gathered(1, grp)
        for step in range(steps):
            if grp < last and step == FINISH[grp]:
                finish(1, grp + 1)
            late = step + AHEAD - 1 if grp == 0 and 0 < step <= steps - AHEAD else None
            if late is not None:
                with scope("wait_w"):
                    head_copy(0, late).wait()
                    head_copy(1, late).wait()
            rows = range(0, CHUNK, TILE)
            if grp == 0 and step == 0:
                for row in rows:
                    place = pl.ds(row, TILE)
                    with scope("first"):
                        zsend[step, rows_of(grp, 1), place] = turned_dot(h_in, wh.at[step], row) * (1.0 / TEMPERATURE)
                    z_copy(grp, step, place).start()
                continue
            with scope(f"send{grp}"):
                z = jnp.concatenate([turned_dot(h_in, wh.at[step], row) for row in rows], axis=1)
                zsend[step, rows_of(grp, 1)] = scaled(z, 0, step)
                if late is not None:
                    turn_head(late)
            z_copy(grp, step).start()
    h_in = normed_rows(1, 0, tokens)
    for step in range(steps):
        with scope("keep"):
            zkeep[step] = scaled(dot_t(h_in, wh[step, CHUNK:2 * CHUNK]), 1, step)
            if step > 0:
                own_step(step - 1)
    own_step(steps - 1)


    def to_row(col):
        return jnp.sum(jnp.where(eye, col, 0.0), axis=0, keepdims=True)

    def stat_rows(m_ref, s_ref):
        m_all = m_ref[...]
        m_col = jnp.max(m_all, axis=1, keepdims=True)
        s_col = jnp.sum(s_ref[...] * jnp.exp(m_all - m_col), axis=1, keepdims=True)
        return to_row(m_col), to_row(s_col)

    packs = (pack, pack_kl)

    def p_copy(which, hop):
        other = (here + hop) % 8
        return pltpu.make_async_remote_copy(
            packs[which].at[here], packs[which].at[here], p_send.at[which], p_recv.at[which],
            device_id={"tp": other % 2, "role": other // 2}, device_id_type=MESH)

    def p_all(which):
        seven = packs[which].at[pl.ds(0, 7)]
        return pltpu.make_async_remote_copy(
            seven, seven, p_send.at[which], p_recv.at[which], device_id=x_peer, device_id_type=MESH)

    pack[here, 0:1, 0:tokens], pack[here, 1:2, 0:tokens] = stat_rows(m_own, s_own)
    pack[here, 2:3, 0:tokens] = to_row(jnp.sum(t_acc[...], axis=1, keepdims=True))
    for hop in range(1, 8):
        p_copy(0, hop).start()
    sent = [(rbuf, d_send), (rbuf, b_send), (dbuf, c_send)]
    sent += [(rbuf.at[pl.ds(0, 2), rows_of(grp), summed(grp)], y_send.at[grp]) for grp in range(groups)]
    for ref, send in sent:
        pltpu.make_async_remote_copy(ref, ref, send, c_recv.at[0], device_id=d_peer, device_id_type=MESH).wait_send()
    for grp in range(last):
        whole = zrecv.at[pl.ds(0, steps), rows_of(grp, 1)]
        pltpu.make_async_remote_copy(whole, whole, z_send, z_recv.at[grp], device_id=x_peer, device_id_type=MESH).wait_recv()
    for step in range(steps):
        kl_step(step)
    pack_kl[here, 0:1, 0:tokens], pack_kl[here, 1:2, 0:tokens] = stat_rows(m_kl, s_kl)
    for hop in range(1, 8):
        p_copy(1, hop).start()
    pltpu.make_async_remote_copy(zsend, zsend, z_send, z_recv.at[0], device_id=x_peer, device_id_type=MESH).wait_send()
    p_all(0).wait_send()
    with scope("wait_p0"):
        p_all(0).wait_recv()
    with scope("wait_p"):
        p_all(1).wait_recv()

    with scope("final"):
        def lse(devices):
            tops = [pack[dev, 0:1, 0:tokens] for dev in devices]
            top = functools.reduce(jnp.maximum, tops)
            total = functools.reduce(jnp.add, [pack[dev, 1:2, 0:tokens] * jnp.exp(t - top) for dev, t in zip(devices, tops)])
            return top + jnp.log(total)

        lse_pol = lse(range(4))
        lse_ref = lse(range(4, 8))
        cross = functools.reduce(jnp.add, [pack_kl[dev, 1:2, 0:tokens] * jnp.exp(pack_kl[dev, 0:1, 0:tokens] - lse_pol) for dev in range(8)])
        tgt_z = functools.reduce(jnp.add, [pack[dev, 2:3, 0:tokens] for dev in range(4)])
        mask_vals = mask_ref[...].astype(F32)
        out_ref[0:1, :] = (cross - lse_pol + lse_ref) * mask_vals
        out_ref[1:2, :] = (tgt_z - lse_pol) * mask_vals
    p_all(1).wait_send()


def solution(mesh):
    by_shard = P(("role", "tp"), None)
    by_role = P("role", None)

    def per_device(hidden, segment_ids, loss_mask, target, norm_gains, w_query, b_query, w_key, b_key, w_value, b_value, w_out, w_gate, w_up, w_down, w_head):
        tokens, dim = hidden.shape[1:]
        q_heads, head_dim = b_query.shape
        ff = w_gate.shape[0]
        vocab = w_head.shape[0]
        groups = len(SIZES)
        cols = dim // 2
        q_rows = q_heads * head_dim
        halves = ((vocab // CHUNK + 2) // 2) * CHUNK
        steps = halves // CHUNK
        wide = 2 * head_dim
        sem = pltpu.SemaphoreType.DMA
        out = pl.pallas_call(
            functools.partial(kernel, (tokens, dim, head_dim, q_heads, vocab)),
            out_shape=pltpu.VMEM((2, tokens), F32),
            in_specs=[pl.BlockSpec(memory_space=pl.ANY)] * 16,
            out_specs=pl.BlockSpec(memory_space=pltpu.VMEM),
            scratch_shapes=[
                pltpu.VMEM((tokens, dim), BF16),
                pltpu.VMEM((3, 2, dim), F32),
                pltpu.VMEM((1, tokens), jnp.int32),
                pltpu.VMEM((1, tokens), jnp.int32),
                pltpu.VMEM((1, tokens), jnp.int32),
                pltpu.VMEM(b_query.shape, BF16),
                pltpu.VMEM(b_key.shape, BF16),
                pltpu.VMEM(b_value.shape, BF16),
                pltpu.VMEM((q_rows + wide, dim), BF16),
                pltpu.VMEM((2, q_rows, cols), BF16),
                pltpu.VMEM((2 * ff, dim), BF16),
                pltpu.VMEM((2, ff, cols), BF16),
                pltpu.VMEM((steps, 2 * CHUNK, dim), BF16),
                pltpu.VMEM((2, tokens, cols), F32),
                pltpu.VMEM((q_heads * tokens, wide), BF16),
                pltpu.VMEM((2, 2, tokens, cols), F32),
                pltpu.VMEM((2, tokens, cols), F32),
                pltpu.VMEM((2, tokens, cols), F32),
                pltpu.VMEM((2, 2, SIZES[0], DIRECT), F32),
                pltpu.VMEM((2, 2, tokens, cols), F32),
                pltpu.VMEM((tokens, 2 * ff), F32),
                pltpu.VMEM((steps, tokens, CHUNK), F32),
                pltpu.VMEM((steps, tokens, CHUNK), F32),
                pltpu.VMEM((steps, tokens, CHUNK), F32),
                pltpu.VMEM((tokens, 128), F32),
                pltpu.VMEM((tokens, 128), F32),
                pltpu.VMEM((tokens, 128), F32),
                pltpu.VMEM((tokens, 128), F32),
                pltpu.VMEM((tokens, 128), F32),
                pltpu.VMEM((16, 128), F32),
                pltpu.VMEM((8, 4, 128), F32),
                pltpu.VMEM((8, 2, 128), F32),
                sem((8,)), sem((steps,)),
                sem(()), sem((2, 3)), sem((groups,)), sem((2, 3)), sem(()), sem((2,)), sem(()), sem((2, 3)),
                sem(()), sem((2 + steps,)), sem((2,)), sem((2,)),
            ],
            compiler_params=pltpu.CompilerParams(
                collective_id=0, has_side_effects=True, vmem_limit_bytes=64500000),
            name="layer_head_kl",
        )(hidden, jnp.transpose(norm_gains, (1, 0, 2)), w_query, w_key, w_value, w_out, w_gate, w_up, w_down, w_head,
          segment_ids.reshape(1, tokens), loss_mask.reshape(1, tokens), target.reshape(1, tokens), b_query, b_key, b_value)
        return out[0], out[1]

    in_specs = (P(None, "dp", None), P("dp"), P("dp"), P("dp"), P(None, None, None), by_shard, by_shard, by_role, by_role, by_role, by_role, by_shard, by_shard, by_shard, by_shard, by_shard)
    return jax.shard_map(per_device, mesh=mesh, in_specs=in_specs, out_specs=(P("dp"), P("dp")), check_vma=False)
```

```python
import contextlib
import functools
import math

import jax
import jax.numpy as jnp
from jax import lax
from jax.experimental import pallas as pl
from jax.experimental.pallas import tpu as pltpu
from jax.sharding import PartitionSpec as P

EPS = 1e-6
ROPE_BASE = 1000000.0
TEMPERATURE = 0.7
NEG = -1e30
SIZES = (16, 48)
LATER = ((0, 16), (16, 24), (40, 24))
AHEAD = 4
DIRECT = 384
SPARE = 2
SOON = 2
FINISH = (7, 5)
TILE = 256
CHUNK = 512
F32 = jnp.float32
BF16 = jnp.bfloat16
MESH = pl.DeviceIdType.MESH


def scope(name):
    return contextlib.nullcontext()


def dot_t(rows, weight):
    return lax.dot_general(rows, weight, (((1,), (1,)), ((), ())), preferred_element_type=F32)


def dot_n(rows, weight):
    return lax.dot_general(rows, weight, (((1,), (0,)), ((), ())), preferred_element_type=F32)


def normed(vals, gain):
    inv_rms = lax.rsqrt(jnp.mean(vals * vals, axis=-1, keepdims=True) + EPS)
    return (vals * inv_rms * gain).astype(BF16)


def kernel(cfg, hidden, gains, w_query, w_key, w_value, w_out, w_gate, w_up, w_down, w_head,
           seg_in, mask_in, tgt_in, bq_in, bk_in, bv_in, out_ref,
           xb, gn, seg_ref, mask_ref, tgt_ref, bq_ref, bk_ref, bv_ref, wqkv, wo, wgu, wd, wh, xcol, qs, part, rbuf, ybuf, dbuf, full,
           gate_up, zsend, zkeep, zrecv, m_own, s_own, m_kl, s_kl, t_acc, dup, pack, pack_kl,
           in_sem, head_sem, d_send, d_recv, y_send, y_recv, c_send, c_recv, b_send, b_recv, z_send, z_recv, p_send, p_recv):
    tokens, dim, head_dim, q_heads, vocab = cfg
    offs = [sum(SIZES[:grp]) for grp in range(len(SIZES))]
    groups = len(SIZES)
    cols = dim // 2
    ff = w_gate.shape[0]
    halves = ((vocab // CHUNK + 2) // 2) * CHUNK
    steps = halves // CHUNK
    tp = lax.axis_index("tp")
    role = lax.axis_index("role")
    core = role % 2
    half = role // 2
    here = role * 2 + tp
    shard = core * 2 + tp
    d_peer = {"role": half * 2 + 1 - core}
    y_peer = {"tp": 1 - tp}
    c_peer = {"tp": 1 - tp, "role": half * 2 + 1 - core}
    x_peer = {"role": (1 - half) * 2 + core}
    send_half = 1 - half
    q_rows = q_heads * head_dim
    wide = 2 * head_dim

    kv_rows = pl.ds(pl.multiple_of(tp * head_dim, head_dim), head_dim)
    theirs_cols = pl.ds(pl.multiple_of((1 - core) * cols, cols), cols)
    mine_cols = pl.ds(pl.multiple_of(core * cols, cols), cols)
    kv_two = 2 * head_dim
    moves = [(hidden.at[half], xb), (gains, gn), (seg_in, seg_ref), (mask_in, mask_ref), (tgt_in, tgt_ref),
             (bq_in, bq_ref), (bk_in, bk_ref), (bv_in, bv_ref)]
    n_small = len(moves)
    moves += [(w_key.at[kv_rows], wqkv.at[pl.ds(0, head_dim)]), (w_value.at[kv_rows], wqkv.at[pl.ds(head_dim, head_dim)])]
    n_first = []
    cuts = (0, TILE, 2 * TILE, kv_two + q_rows)
    for begin, end in zip(cuts, cuts[1:]):
        low_row = max(begin - kv_two, 0)
        moves.append((w_query.at[pl.ds(low_row, end - kv_two - low_row)],
                      wqkv.at[pl.ds(kv_two + low_row, end - kv_two - low_row)]))
        n_first.append(len(moves))
    n_qkv = len(moves)
    moves += [(w_out.at[:, theirs_cols], wo.at[0]), (w_out.at[:, mine_cols], wo.at[1])]
    n_out = len(moves)
    moves += [(w_gate, wgu.at[pl.ds(0, ff)]), (w_up, wgu.at[pl.ds(ff, ff)])]
    n_gu = len(moves)
    moves += [(w_down.at[:, theirs_cols], wd.at[0]), (w_down.at[:, mine_cols], wd.at[1])]
    bounds = [n_small] + n_first + [n_out, n_out + 1, n_gu]
    loads = [pltpu.make_async_copy(src, dst, in_sem.at[sum(idx >= bound for bound in bounds)])
             for idx, (src, dst) in enumerate(moves)]
    for copy in loads[:n_out]:
        copy.start()

    barrier = pltpu.get_barrier_semaphore()
    for hop in range(1, 8):
        other = (here + hop) % 8
        pl.semaphore_signal(barrier, inc=1, device_id={"tp": other % 2, "role": other // 2}, device_id_type=MESH)

    def chunk_start(part_half, step):
        nominal = part_half * halves + step * CHUNK
        start = jnp.minimum(nominal, vocab - CHUNK)
        return start, nominal - start

    def head_copy(keep, step):
        start, _ = chunk_start((1 - send_half) if keep else send_half, step)
        return pltpu.make_async_copy(w_head.at[pl.ds(pl.multiple_of(start, 64), CHUNK)],
                                     wh.at[step, pl.ds(keep * CHUNK, CHUNK)], head_sem.at[step])

    ti = lax.broadcasted_iota(jnp.int32, (tokens, tokens), 0)
    tj = lax.broadcasted_iota(jnp.int32, (tokens, tokens), 1)
    eye = ti == tj
    lane = lax.broadcasted_iota(jnp.int32, (1, wide), 1)
    half_dim = head_dim // 2
    freq = jnp.exp((lane % half_dim).astype(F32) * (-2.0 * math.log(ROPE_BASE) / head_dim))
    low = (lane % head_dim) < half_dim
    even = lane < head_dim

    def gain_row(which):
        return jnp.where(half == 0, gn[which, 0:1, :], gn[which, 1:2, :])

    with scope("wait_x"):
        for copy in loads[:n_small]:
            copy.wait()
    with scope("norm_x"):
        seg_row = seg_ref[...].astype(F32)
        seg_col = jnp.sum(jnp.where(eye, seg_row, 0.0), axis=1, keepdims=True)
        same = seg_col == seg_row
        allowed = same & (ti >= tj)
        seg_first = jnp.min(jnp.where(same, tj.astype(F32), 1e9), axis=1, keepdims=True)
        pos = lax.broadcasted_iota(jnp.int32, (tokens, 1), 0).astype(F32) - seg_first
        angles = pos * freq
        cos_t = jnp.cos(angles)
        sin_t = jnp.sin(angles)
        sin_t = jnp.where(low, -sin_t, sin_t)
        tgt_col = jnp.sum(jnp.where(eye, tgt_ref[...].astype(F32), 0.0), axis=1, keepdims=True)
        dup[...] = jnp.zeros_like(dup)
        dup[0:q_heads, 0:head_dim] = bq_ref[...].astype(F32)
        dup[q_heads:q_heads + 2, 0:head_dim] = bk_ref[...].astype(F32)
        dup[q_heads + 2:q_heads + 4, 0:head_dim] = bv_ref[...].astype(F32)
        bias = dup[...]
        bias = bias + pltpu.roll(bias, head_dim, 1)
        bias_k = jnp.where(tp == 0, bias[q_heads:q_heads + 1], bias[q_heads + 1:q_heads + 2])
        bias_v = jnp.where(tp == 0, bias[q_heads + 2:q_heads + 3], bias[q_heads + 3:q_heads + 4])
        xf = xb[...].astype(F32)
        xcol[0] = xf[:, :cols]
        xcol[1] = xf[:, cols:]
        a_in = normed(xf, gain_row(0))

    def rotate(vals):
        turned = jnp.where(low, pltpu.roll(vals, wide - half_dim, 1), pltpu.roll(vals, half_dim, 1))
        return vals * cos_t + turned * sin_t

    def q_store(pair, vals):
        bias_q = jnp.where(even, bias[2 * pair:2 * pair + 1], bias[2 * pair + 1:2 * pair + 2])
        q_rot = rotate(vals + bias_q) * head_dim ** -0.5
        for odd in range(2):
            head = jnp.where(even, 0.0, q_rot) if odd else jnp.where(even, q_rot, 0.0)
            for grp in range(groups):
                off, size = offs[grp], SIZES[grp]
                start = q_heads * off + (2 * pair + odd) * size
                qs[start:start + size, :] = head[off:off + size].astype(BF16)

    with scope("wait_kv"):
        for copy in loads[n_small:n_first[0]]:
            copy.wait()
    for copy in loads[n_out:]:
        copy.start()

    @pl.loop(0, steps)
    def _(step):
        head_copy(0, step).start()
        head_copy(1, step).start()

    with scope("qkv"):
        dots = [dot_t(a_in, wqkv[cuts[0]:cuts[1]])]
        for copy in loads[n_first[0]:n_first[1]]:
            copy.wait()
        dots.append(dot_t(a_in, wqkv[cuts[1]:cuts[2]]))
        kv = dots[0][:, :wide]
        other = pltpu.roll(kv, head_dim, 1)
        k_rot = rotate(jnp.where(even, kv, other) + bias_k).astype(BF16)
        v_two = (jnp.where(even, other, kv) + bias_v).astype(BF16)
        q_store(0, dots[0][:, wide:2 * wide])
        for copy in loads[n_first[1]:n_first[2]]:
            copy.wait()
        dots.append(dot_t(a_in, wqkv[cuts[2]:cuts[3]]))
        q_store(1, dots[1][:, :wide])
        q_store(2, dots[1][:, wide:])
        q_store(3, dots[2])
    def attend(grp):
        off, size = offs[grp], SIZES[grp]
        keys = off + size
        scores = dot_t(qs[q_heads * off:q_heads * keys], k_rot[:keys]).reshape(q_heads, size, keys)
        scores = jnp.where(allowed[None, off:keys, :keys], scores, NEG)
        expd = jnp.exp(scores - jnp.max(scores, axis=-1, keepdims=True))
        probs = (expd / jnp.sum(expd, axis=-1, keepdims=True)).astype(BF16).reshape(q_heads * size, keys)
        heads_out = dot_n(probs, v_two[:keys])
        outs = []
        for pair in range(q_heads // 2):
            lo = heads_out[2 * pair * size:(2 * pair + 1) * size]
            hi = heads_out[(2 * pair + 1) * size:(2 * pair + 2) * size]
            outs.append(jnp.where(even, lo, hi).astype(BF16))
        return jnp.concatenate(outs, axis=1)

    ranges = (tuple(zip(offs, SIZES)), LATER)
    later_of = ((0,), (1, 2))

    def rows_of(grp, red=0):
        return pl.ds(*ranges[red][grp])

    def d_copy(red, grp):
        return pltpu.make_async_remote_copy(
            part.at[red, 0, rows_of(grp, red)], rbuf.at[red, rows_of(grp, red)], d_send, d_recv.at[red, grp],
            device_id=d_peer, device_id_type=MESH)

    def summed(grp):
        return pl.ds(DIRECT, cols - DIRECT) if grp == 0 else pl.ds(0, cols)

    def y_copy(red, grp):
        place = (red, rows_of(grp, red), summed(grp))
        return pltpu.make_async_remote_copy(
            rbuf.at[place], ybuf.at[place], y_send.at[min(grp, 1)], y_recv.at[red, grp],
            device_id=y_peer, device_id_type=MESH)

    def c_copy(red, mine):
        return pltpu.make_async_remote_copy(
            part.at[red, mine, rows_of(0), pl.ds(0, DIRECT)], dbuf.at[red, 1 - mine], c_send, c_recv.at[red],
            device_id=y_peer if mine else c_peer, device_id_type=MESH)

    def b_copy(red, grp):
        return pltpu.make_async_remote_copy(
            full.at[red, core, rows_of(grp, red)], full.at[red, core, rows_of(grp, red)], b_send, b_recv.at[red, grp],
            device_id=d_peer, device_id_type=MESH)

    def chip_sum(red, grp):
        rows = rows_of(grp, red)
        with scope(f"wait_d{red}{grp}"):
            d_copy(red, grp).wait_recv()
        rbuf[red, rows] = part[red, 1, rows] + rbuf[red, rows]
        y_copy(red, grp).start()

    def finish(red, grp):
        rows = rows_of(grp, red)
        with scope(f"wait_y{red}{grp}"):
            y_copy(red, grp).wait_recv()
        base = xcol if red == 0 else full.at[0]
        place = (rows, summed(grp))
        full[(red, core) + place] = (base[(core,) + place] + (rbuf[(red,) + place] + ybuf[(red,) + place])).astype(BF16).astype(F32)
        if grp == 0:
            pltpu.make_async_remote_copy(dbuf.at[red], dbuf.at[red], c_send, c_recv.at[red],
                                         device_id=y_peer, device_id_type=MESH).wait_recv()
            place = (rows, pl.ds(0, DIRECT))
            full[(red, core) + place] = (base[(core,) + place] + (rbuf[(red,) + place] + (dbuf[red, 0] + dbuf[red, 1]))).astype(BF16).astype(F32)
        b_copy(red, grp).start()

    def b_wait(red, grp):
        with scope(f"wait_b{red}{grp}"):
            b_copy(red, grp).wait_recv()

    def normed_rows(red, off, size):
        rows = pl.ds(off, size)
        left, right = full[red, 0, rows], full[red, 1, rows]
        total = jnp.sum(left * left, axis=-1, keepdims=True) + jnp.sum(right * right, axis=-1, keepdims=True)
        inv_rms = lax.rsqrt(total * (1.0 / dim) + EPS)
        gain = gain_row(red + 1)
        return jnp.concatenate([(left * inv_rms * gain[:, :cols]).astype(BF16),
                                (right * inv_rms * gain[:, cols:]).astype(BF16)], axis=1)

    def gathered(red, grp):
        b_wait(red, grp)
        return normed_rows(red, *ranges[red][grp])

    def turn_tiles(ref, rows):
        for k in range(dim // TILE):
            ref[rows, k * TILE:(k + 1) * TILE] = ref[rows, k * TILE:(k + 1) * TILE].T

    def turn(first, end):
        with scope("turn"):
            for blk in range(first, end):
                turn_tiles(wgu, pl.ds(blk * TILE, TILE))

    def turn_head(step):
        for row in range(0, CHUNK, TILE):
            turn_tiles(wh.at[step], pl.ds(row, TILE))

    def turned_dot(vals, ref, row):
        return functools.reduce(jnp.add, [dot_n(vals[:, k * TILE:(k + 1) * TILE], ref[row:row + TILE, k * TILE:(k + 1) * TILE])
                                          for k in range(dim // TILE)])

    def mlp(grp, b_in):
        rows = rows_of(grp)
        if grp == 0:
            for copy in loads[n_gu:]:
                copy.wait()
        if grp == groups - 1:
            for step in range(AHEAD):
                head_copy(0, step).wait()
                head_copy(1, step).wait()
        with scope(f"mlp{grp}"):
            if grp == groups - 1:
                for step in range(AHEAD):
                    turn_head(step)
            for row in range(0, 2 * ff, TILE):
                gate_up[rows, row:row + TILE] = turned_dot(b_in, wgu, row)
            gate, up = gate_up[rows, 0:ff], gate_up[rows, ff:2 * ff]
            act = (gate * (1.0 / (1.0 + jnp.exp(-gate))) * up).astype(BF16)
            part[1, 0, rows] = dot_n(act, wd[0])
        for late in later_of[grp]:
            d_copy(1, late).start()
        if grp == 0:
            c_copy(1, 0).start()
        if grp + 1 < groups:
            finish(0, grp + 1)
        else:
            finish(1, 0)
        with scope(f"down{grp}"):
            part[1, 1, rows] = dot_n(act, wd[1])
        if grp == 0:
            c_copy(1, 1).start()

    for grp in range(groups):
        with scope(f"attn{grp}"):
            mixed = attend(grp)
        if grp == 0:
            for copy in loads[n_qkv:n_out]:
                copy.wait()
        if grp == 1:
            chip_sum(0, 0)
        with scope("oproj"):
            part[0, 0, rows_of(grp)] = dot_n(mixed, wo[0])
        if grp == 0:
            with scope("entry"):
                pl.semaphore_wait(barrier, 7)
        d_copy(0, grp).start()
        if grp == 0:
            c_copy(0, 0).start()
        with scope("oproj"):
            part[0, 1, rows_of(grp)] = dot_n(mixed, wo[1])
        if grp == 0:
            c_copy(0, 1).start()
    blocks = 2 * ff // TILE
    early = ff // TILE
    loads[n_out].wait()
    turn(0, SOON)
    chip_sum(0, 1)
    turn(SOON, early)
    loads[n_out + 1].wait()
    turn(early, blocks - SPARE)
    finish(0, 0)
    turn(blocks - SPARE, blocks)
    for grp in range(groups):
        mlp(grp, gathered(0, grp))
        for late in later_of[grp]:
            chip_sum(1, late)

    for stat in (s_own, s_kl, t_acc):
        stat[...] = jnp.zeros_like(stat)
    m_own[...] = jnp.full_like(m_own, NEG)
    m_kl[...] = jnp.full_like(m_kl, NEG)
    lanes = lax.broadcasted_iota(jnp.int32, (1, CHUNK), 1)
    tiles = CHUNK // 128

    def split(vals):
        return [vals[:, 128 * t:128 * (t + 1)] for t in range(tiles)]

    last = len(LATER) - 1

    def z_copy(grp, step, lanes_of=pl.ds(0, CHUNK)):
        place = (step, rows_of(grp, 1), lanes_of)
        return pltpu.make_async_remote_copy(
            zsend.at[place], zrecv.at[place], z_send, z_recv.at[grp + (step if grp == last else 0)],
            device_id=x_peer, device_id_type=MESH)

    def scaled(z, keep, step):
        _, repeated = chunk_start((1 - send_half) if keep else send_half, step)
        return jnp.where(lanes >= repeated, z * (1.0 / TEMPERATURE), NEG)

    def own_step(step):
        m_old, total, hits = m_own[...], s_own[...], t_acc[...]
        parts = []
        for keep, src in ((0, zsend), (1, zkeep)):
            start, repeated = chunk_start((1 - send_half) if keep else send_half, step)
            z = src[step]
            ids = (lanes + (shard * vocab + start)).astype(F32)
            for hit in split(jnp.where((ids == tgt_col) & (lanes >= repeated), z, 0.0)):
                hits = hits + hit
            parts += split(z)
        m_new = functools.reduce(jnp.maximum, parts, m_old)
        total = total * jnp.exp(m_old - m_new)
        for piece in parts:
            total = total + jnp.exp(piece - m_new)
        m_own[...] = m_new
        s_own[...] = total
        t_acc[...] = hits

    def kl_step(step):
        with scope(f"wait_z{step}"):
            z_copy(last, step).wait_recv()
        mine, theirs = zkeep[step], zrecv[step]
        policy = half == 0
        tops = split(jnp.where(policy, mine, theirs))
        diffs = split(jnp.where(policy, mine - theirs, theirs - mine))
        m_old = m_kl[...]
        m_new = functools.reduce(jnp.maximum, tops, m_old)
        total = s_kl[...] * jnp.exp(m_old - m_new)
        for top, diff in zip(tops, diffs):
            total = total + jnp.exp(top - m_new) * diff
        m_kl[...] = m_new
        s_kl[...] = total

    for grp in range(last + 1):
        h_in = gathered(1, grp)
        for step in range(steps):
            if grp < last and step == FINISH[grp]:
                finish(1, grp + 1)
            late = step + AHEAD - 1 if grp == 0 and 0 < step <= steps - AHEAD else None
            if late is not None:
                with scope("wait_w"):
                    head_copy(0, late).wait()
                    head_copy(1, late).wait()
            rows = range(0, CHUNK, TILE)
            if grp == 0 and step == 0:
                for row in rows:
                    place = pl.ds(row, TILE)
                    with scope("first"):
                        zsend[step, rows_of(grp, 1), place] = turned_dot(h_in, wh.at[step], row) * (1.0 / TEMPERATURE)
                    z_copy(grp, step, place).start()
                continue
            with scope(f"send{grp}"):
                z = jnp.concatenate([turned_dot(h_in, wh.at[step], row) for row in rows], axis=1)
                zsend[step, rows_of(grp, 1)] = scaled(z, 0, step)
                if late is not None:
                    turn_head(late)
            z_copy(grp, step).start()
    h_in = normed_rows(1, 0, tokens)
    for step in range(steps):
        with scope("keep"):
            zkeep[step] = scaled(dot_t(h_in, wh[step, CHUNK:2 * CHUNK]), 1, step)
            if step > 0:
                own_step(step - 1)
    own_step(steps - 1)


    def to_row(col):
        return jnp.sum(jnp.where(eye, col, 0.0), axis=0, keepdims=True)

    def stat_rows(m_ref, s_ref):
        m_all = m_ref[...]
        m_col = jnp.max(m_all, axis=1, keepdims=True)
        s_col = jnp.sum(s_ref[...] * jnp.exp(m_all - m_col), axis=1, keepdims=True)
        return to_row(m_col), to_row(s_col)

    packs = (pack, pack_kl)

    flips = ((1, 0, 1), (1, 1, 1), (1, 0, 0), (1, 1, 0), (0, 0, 1), (0, 1, 1), (0, 1, 0))
    pairs = ((tp, 1 - tp), (core, 1 - core), (half, 1 - half))

    def p_copy(which, hop):
        to_half, to_core, to_tp = flips[hop - 1]
        target = {"tp": pairs[0][to_tp], "role": pairs[2][to_half] * 2 + pairs[1][to_core]}
        return pltpu.make_async_remote_copy(
            packs[which].at[here], packs[which].at[here], p_send.at[which], p_recv.at[which],
            device_id=target, device_id_type=MESH)

    def p_all(which):
        seven = packs[which].at[pl.ds(0, 7)]
        return pltpu.make_async_remote_copy(
            seven, seven, p_send.at[which], p_recv.at[which], device_id=x_peer, device_id_type=MESH)

    pack[here, 0:1, 0:tokens], pack[here, 1:2, 0:tokens] = stat_rows(m_own, s_own)
    pack[here, 2:3, 0:tokens] = to_row(jnp.sum(t_acc[...], axis=1, keepdims=True))
    for hop in range(1, 8):
        p_copy(0, hop).start()
    sent = [(rbuf, d_send), (rbuf, b_send), (dbuf, c_send)]
    sent += [(rbuf.at[pl.ds(0, 2), rows_of(grp), summed(grp)], y_send.at[grp]) for grp in range(groups)]
    for ref, send in sent:
        pltpu.make_async_remote_copy(ref, ref, send, c_recv.at[0], device_id=d_peer, device_id_type=MESH).wait_send()
    for grp in range(last):
        whole = zrecv.at[pl.ds(0, steps), rows_of(grp, 1)]
        pltpu.make_async_remote_copy(whole, whole, z_send, z_recv.at[grp], device_id=x_peer, device_id_type=MESH).wait_recv()
    for step in range(steps):
        kl_step(step)
    pack_kl[here, 0:1, 0:tokens], pack_kl[here, 1:2, 0:tokens] = stat_rows(m_kl, s_kl)
    for hop in range(1, 8):
        p_copy(1, hop).start()
    pltpu.make_async_remote_copy(zsend, zsend, z_send, z_recv.at[0], device_id=x_peer, device_id_type=MESH).wait_send()
    p_all(0).wait_send()
    with scope("wait_p0"):
        p_all(0).wait_recv()
    with scope("wait_p"):
        p_all(1).wait_recv()

    with scope("final"):
        def lse(devices):
            tops = [pack[dev, 0:1, 0:tokens] for dev in devices]
            top = functools.reduce(jnp.maximum, tops)
            total = functools.reduce(jnp.add, [pack[dev, 1:2, 0:tokens] * jnp.exp(t - top) for dev, t in zip(devices, tops)])
            return top + jnp.log(total)

        lse_pol = lse(range(4))
        lse_ref = lse(range(4, 8))
        cross = functools.reduce(jnp.add, [pack_kl[dev, 1:2, 0:tokens] * jnp.exp(pack_kl[dev, 0:1, 0:tokens] - lse_pol) for dev in range(8)])
        tgt_z = functools.reduce(jnp.add, [pack[dev, 2:3, 0:tokens] for dev in range(4)])
        mask_vals = mask_ref[...].astype(F32)
        out_ref[0:1, :] = (cross - lse_pol + lse_ref) * mask_vals
        out_ref[1:2, :] = (tgt_z - lse_pol) * mask_vals
    p_all(1).wait_send()


def solution(mesh):
    by_shard = P(("role", "tp"), None)
    by_role = P("role", None)

    def per_device(hidden, segment_ids, loss_mask, target, norm_gains, w_query, b_query, w_key, b_key, w_value, b_value, w_out, w_gate, w_up, w_down, w_head):
        tokens, dim = hidden.shape[1:]
        q_heads, head_dim = b_query.shape
        ff = w_gate.shape[0]
        vocab = w_head.shape[0]
        groups = len(SIZES)
        cols = dim // 2
        q_rows = q_heads * head_dim
        halves = ((vocab // CHUNK + 2) // 2) * CHUNK
        steps = halves // CHUNK
        wide = 2 * head_dim
        sem = pltpu.SemaphoreType.DMA
        out = pl.pallas_call(
            functools.partial(kernel, (tokens, dim, head_dim, q_heads, vocab)),
            out_shape=pltpu.VMEM((2, tokens), F32),
            in_specs=[pl.BlockSpec(memory_space=pl.ANY)] * 16,
            out_specs=pl.BlockSpec(memory_space=pltpu.VMEM),
            scratch_shapes=[
                pltpu.VMEM((tokens, dim), BF16),
                pltpu.VMEM((3, 2, dim), F32),
                pltpu.VMEM((1, tokens), jnp.int32),
                pltpu.VMEM((1, tokens), jnp.int32),
                pltpu.VMEM((1, tokens), jnp.int32),
                pltpu.VMEM(b_query.shape, BF16),
                pltpu.VMEM(b_key.shape, BF16),
                pltpu.VMEM(b_value.shape, BF16),
                pltpu.VMEM((q_rows + wide, dim), BF16),
                pltpu.VMEM((2, q_rows, cols), BF16),
                pltpu.VMEM((2 * ff, dim), BF16),
                pltpu.VMEM((2, ff, cols), BF16),
                pltpu.VMEM((steps, 2 * CHUNK, dim), BF16),
                pltpu.VMEM((2, tokens, cols), F32),
                pltpu.VMEM((q_heads * tokens, wide), BF16),
                pltpu.VMEM((2, 2, tokens, cols), F32),
                pltpu.VMEM((2, tokens, cols), F32),
                pltpu.VMEM((2, tokens, cols), F32),
                pltpu.VMEM((2, 2, SIZES[0], DIRECT), F32),
                pltpu.VMEM((2, 2, tokens, cols), F32),
                pltpu.VMEM((tokens, 2 * ff), F32),
                pltpu.VMEM((steps, tokens, CHUNK), F32),
                pltpu.VMEM((steps, tokens, CHUNK), F32),
                pltpu.VMEM((steps, tokens, CHUNK), F32),
                pltpu.VMEM((tokens, 128), F32),
                pltpu.VMEM((tokens, 128), F32),
                pltpu.VMEM((tokens, 128), F32),
                pltpu.VMEM((tokens, 128), F32),
                pltpu.VMEM((tokens, 128), F32),
                pltpu.VMEM((16, 128), F32),
                pltpu.VMEM((8, 4, 128), F32),
                pltpu.VMEM((8, 2, 128), F32),
                sem((8,)), sem((steps,)),
                sem(()), sem((2, 3)), sem((groups,)), sem((2, 3)), sem(()), sem((2,)), sem(()), sem((2, 3)),
                sem(()), sem((2 + steps,)), sem((2,)), sem((2,)),
            ],
            compiler_params=pltpu.CompilerParams(
                collective_id=0, has_side_effects=True, vmem_limit_bytes=64500000),
            name="layer_head_kl",
        )(hidden, jnp.transpose(norm_gains, (1, 0, 2)), w_query, w_key, w_value, w_out, w_gate, w_up, w_down, w_head,
          segment_ids.reshape(1, tokens), loss_mask.reshape(1, tokens), target.reshape(1, tokens), b_query, b_key, b_value)
        return out[0], out[1]

    in_specs = (P(None, "dp", None), P("dp"), P("dp"), P("dp"), P(None, None, None), by_shard, by_shard, by_role, by_role, by_role, by_role, by_shard, by_shard, by_shard, by_shard, by_shard)
    return jax.shard_map(per_device, mesh=mesh, in_specs=in_specs, out_specs=(P("dp"), P("dp")), check_vma=False)
```
